32 devices in a mesh: agg: 2 (over y), gx: 4 (over x, core), gy: 4 (over z).
Axes of the slice: x: 2, y: 2, z: 4, core: 2. Of those that a mesh axis runs over, the one named last changes fastest.
Arguments:
- velocity_prev: float32 [3, 32, 64, 256], P(None, 'gx', 'gy', 'agg'), may hold values from -6 to 6
- forcing: float32 [3, 32, 64, 256], P(None, 'gx', 'gy', 'agg'), may hold values from -6 to 6
- reaction: float32 [32, 64, 256], P('gx', 'gy', 'agg'), may hold values from 0.1 to 4
Outputs:
- velocity: float32 [3, 32, 64, 256], P(None, 'gx', 'gy', 'agg')
- compressed: float32 [3, 64, 256, 16], P(None, 'gy', ('agg', 'gx'))
The draws below stay inside these ranges and needn't reach their ends.
All inputs are finite; a program needn't handle non-finite values.
Results may differ from the reference program's by a relative error of at most 0.00002.
Values sent between devices are 32-bit elements; how exact they have to be, the bound alone decides.
A program may use at most 64 MiB of HBM per device.

```python
import math
import jax
import jax.numpy as jnp
from jax import lax

SWEEPS = 2
COARSE_SWEEPS = 4
LX = 5
NX = 32
NY = 64
NZ = 256


def shard_levels(rng, dims, cuts, low, top_value):
    loudness, own = 1.0, jax.random.fold_in(rng, 6)
    for axis_at, blocks in cuts:
        heights = jnp.exp(jax.random.uniform(jax.random.fold_in(own, axis_at), (blocks,), jnp.float32, low / len(cuts), top_value / len(cuts)))
        loudness = loudness * jnp.repeat(heights, dims[axis_at] // blocks).reshape([-1 if axis == axis_at else 1 for axis in range(len(dims))])
    return loudness


def normal_values(key, shape, scale, limit, split=(), kind=jnp.bfloat16):
    result = jax.random.normal(key, shape, jnp.float32) * scale
    if len(split) > 0:
        result = shard_levels(key, shape, split, -0.22, 0.18) * result
    return jnp.clip(result, min=-limit, max=limit).astype(kind)


def setup_inputs(seed: int = 0) -> dict:
    key_list = jax.random.split(jax.random.key(seed), 4)
    velocity_prev = normal_values(key_list[0], (3, NX, NY, NZ), 1.0, 6.0, ((1, 4), (2, 4), (3, 2)), jnp.float32)
    forcing = normal_values(key_list[1], (3, NX, NY, NZ), 1.0, 6.0, ((1, 4), (2, 4), (3, 2)), jnp.float32)
    reaction = jnp.clip(jnp.exp(math.log(4.0) - 3.6888794 * jax.random.uniform(key_list[2], (NX, NY, NZ), jnp.float32) ** shard_levels(key_list[2], (NX, NY, NZ), ((0, 4), (1, 4), (2, 2)), -0.2, 0.2)), 0.1, 4.0)
    return dict(velocity_prev=velocity_prev, forcing=forcing, reaction=reaction)


damping = 0.8
root_half = 0.7071067811865476


def neighbours(field):
    padded = jnp.pad(field, 1)
    summed = padded[2:, 1:-1, 1:-1] + padded[:-2, 1:-1, 1:-1]
    summed = summed + padded[1:-1, 2:, 1:-1] + padded[1:-1, :-2, 1:-1]
    summed = summed + padded[1:-1, 1:-1, 2:] + padded[1:-1, 1:-1, :-2]
    return summed


def fine_residual(current, forcing_part, diagonal):
    return forcing_part - (diagonal * current - neighbours(current))


def block_mean(field):
    size_x, size_y, size_z = field.shape
    return field.reshape(size_x // 2, 2, size_y // 2, 2, size_z // 2, 2).mean(axis=(1, 3, 5))


def prolong(coarse):
    size_x, size_y, size_z = coarse.shape
    expanded = jnp.broadcast_to(coarse[:, None, :, None, :, None], (size_x, 2, size_y, 2, size_z, 2))
    return expanded.reshape(2 * size_x, 2 * size_y, 2 * size_z)


def halve_last(values):
    paired = values.reshape(values.shape[:-1] + (values.shape[-1] // 2, 2))
    even_cells = paired[..., 0]
    odd_cells = paired[..., 1]
    return (even_cells + odd_cells) * root_half, (even_cells - odd_cells) * root_half


def x_levels(approx):
    details = []
    for level_index in range(LX - 1):
        approx, detail = halve_last(approx)
        details.append(detail)
    return jnp.concatenate([approx] + details[::-1], axis=-1)


def pair_pass(values, which_dim):
    layout = values.shape
    paired = values.reshape(layout[:which_dim] + (layout[which_dim] // 2, 2) + layout[which_dim + 1:])
    even_cells = lax.index_in_dim(paired, 0, which_dim + 1, keepdims=False)
    odd_cells = lax.index_in_dim(paired, 1, which_dim + 1, keepdims=False)
    stacked = jnp.stack([(even_cells + odd_cells) * root_half, (even_cells - odd_cells) * root_half], axis=which_dim + 1)
    return stacked.reshape(layout)


def reference(velocity_prev, forcing, reaction):
    diagonal = 6.0 + reaction
    coarse_diag = (6.0 + 4.0 * block_mean(reaction)) * 0.25

    def solve_component(inputs):
        previous, forcing_part = inputs
        current = previous
        for sweep_index in range(SWEEPS):
            current = current + damping * fine_residual(current, forcing_part, diagonal) / diagonal
        coarse_rhs = block_mean(fine_residual(current, forcing_part, diagonal))
        correction = damping * coarse_rhs / coarse_diag
        for sweep_index in range(COARSE_SWEEPS - 1):
            correction = correction + damping * (coarse_rhs - (coarse_diag * correction - 0.25 * neighbours(correction))) / coarse_diag
        current = current + prolong(correction)
        current = current + damping * fine_residual(current, forcing_part, diagonal) / diagonal
        x_lines = jnp.transpose(previous, (1, 2, 0))
        coeffs = x_levels(halve_last(x_lines)[0])
        coeffs = pair_pass(pair_pass(coeffs, 0), 1)
        return current, coeffs

    velocity, compressed = lax.map(solve_component, (velocity_prev, forcing))
    return velocity, compressed
```

```python
import functools

import jax
import jax.numpy as jnp
import numpy as np
from jax import lax
from jax.experimental import pallas as pl
from jax.experimental.pallas import tpu as pltpu
from jax.sharding import PartitionSpec as P

SWEEPS = 2
COARSE_SWEEPS = 4
LX = 5
MESH = pl.DeviceIdType.MESH

damping = 0.8
keep = 1.0 - damping
root_half = 0.7071067811865476


def local_levels(cells_x):
    return min(LX, cells_x.bit_length() - 1)


def finish_matrix(cells_x, blocks, rows):
    levels = local_levels(cells_x)
    kept = cells_x // 2
    eye = np.eye(blocks * kept).reshape(blocks, kept, blocks * kept)
    width = cells_x >> levels
    approx = eye[:, :width].reshape(blocks * width, -1)
    details, at = [], width
    for level in range(levels, 1, -1):
        width = cells_x >> level
        details.append(eye[:, at : at + width].reshape(blocks * width, -1))
        at += width
    for level in range(levels, LX):
        low, high = approx[0::2], approx[1::2]
        approx, detail = (low + high) * root_half, (low - high) * root_half
        details.insert(0, detail)
    along_x = np.concatenate([approx] + details, axis=0)
    along_y = np.zeros((rows, rows))
    for row in range(0, rows, 2):
        along_y[row, row : row + 2] = root_half
        along_y[row + 1, row : row + 2] = root_half, -root_half
    return np.einsum("qk,yr->yqkr", along_x, along_y).reshape(-1, blocks * kept * rows).astype(np.float32)


def neighbour_sides():
    return [(axis, high) for axis in ("gx", "gy", "agg") for high in (False, True)]


def edge_sides():
    pairs = (("gx", "gy"), ("gx", "agg"), ("gy", "agg"))
    return [((a, p), (b, q)) for a, b in pairs for p in (False, True) for q in (False, True)]


def around():
    axes = ("gx", "gy", "agg")
    found = []
    for number in range(1, 27):
        turn = [(number // 3**i) % 3 for i in range(3)]
        found.append(tuple((axis, way == 1) for axis, way in zip(axes, turn) if way))
    return sorted(found, key=lambda sides: (-len(sides), sides))


def kernel(
    sizes, v_hbm, f_hbm, r_hbm, m_hbm, vel_ref, comp_ref, v_ref, f_ref, r_ref, m_ref,
    xs_fine, xr_fine, ys_fine, yr_fine, zs_fine, zr_fine,
    q_ext, h_ext, zs_coarse,
    xs_deep, xr_deep, ys_deep, yr_deep, zs_deep, zr_deep, exy, exz, eyz,
c_send, c_recv, w_buf, send_sem, recv_sem, deep_send_sem, deep_recv_sem, q_send_sem, q_recv_sem,
    c_send_sem, c_recv_sem, in_sem,
):
    counts = sizes
    C, X, Y, Z = v_ref.shape
    Xc = X // 2
    half = Z // 2
    me = {axis: lax.axis_index(axis) for axis in counts}
    blocks = counts["gx"]
    chunk = Z // blocks

    def exists(axis, high):
        return me[axis] < counts[axis] - 1 if high else me[axis] > 0

    loads = [
        pltpu.make_async_copy(src, dst, in_sem.at[i])
        for i, (src, dst) in enumerate(
            ((v_hbm, v_ref), (f_hbm, f_ref), (r_hbm, r_ref), (m_hbm, m_ref))
        )
    ]
    for load in loads:
        load.start()
    def beside(*sides):
        return {axis: me[axis] + (1 if high else -1) for axis, high in sides}

    barrier = pltpu.get_barrier_semaphore()
    expected = blocks - 1
    for step in range(1, blocks):
        pl.semaphore_signal(
            barrier, inc=1, device_id={"gx": lax.rem(me["gx"] + step, blocks)}, device_id_type=MESH
        )
    def all_exist(sides, flip):
        there = None
        for axis, high in sides:
            one = exists(axis, high != flip)
            there = one if there is None else there & one
        return there

    for sides in around():
        if len(sides) > 1 or sides[0][0] != "gx":
            there = all_exist(sides, False)
            expected = expected + there.astype(jnp.int32)

            @pl.when(there)
            def _():
                pl.semaphore_signal(barrier, inc=1, device_id=beside(*sides), device_id_type=MESH)

    def coarse_message(sides):
        at = {axis: 1 if high else -1 for axis, high in sides}
        block = 1 - at.get("gx", 0)
        here, there = {
            0: (slice(0, Y), slice(0, Y)),
            1: (slice(Y - 8, Y), slice(Y + 8, Y + 16)),
            -1: (slice(0, 8), slice(Y, Y + 8)),
        }[at.get("gy", 0)]
        if "agg" in at:
            return zs_coarse.at[here], h_ext.at[0 if at["agg"] > 0 else 1, block, there]
        return q_ext.at[1, :, here], q_ext.at[block, :, there]

    def coarse_copies():
        return [
            (
                sides,
                pltpu.make_async_remote_copy(
                    src_ref=coarse_message(sides)[0],
                    dst_ref=coarse_message(sides)[1],
                    send_sem=q_send_sem.at[slot],
                    recv_sem=q_recv_sem.at[slot],
                    device_id=beside(*sides),
                    device_id_type=MESH,
                ),
            )
            for slot, sides in enumerate(around())
        ]

    for sides in around():
        @pl.when(jnp.logical_not(all_exist(sides, True)))
        def _():
            target = coarse_message(sides)[1]
            target[...] = jnp.zeros(target.shape, jnp.float32)

    received = {
        "gx": (xr_fine, xr_deep),
        "gy": (yr_fine, yr_deep),
        "agg": (zr_fine, zr_deep),
    }
    edges = {("gx", "gy"): exy, ("gx", "agg"): exz, ("gy", "agg"): eyz}
    for (axis_a, high_a), (axis_b, high_b) in edge_sides():
        @pl.when(jnp.logical_not(exists(axis_a, high_a) & exists(axis_b, high_b)))
        def _():
            buffer = edges[axis_a, axis_b]
            for phase in range(buffer.shape[0]):
                buffer[phase, 2 * int(high_a) + int(high_b)] = jnp.zeros(buffer.shape[2:], buffer.dtype)

    ys_deep[...] = jnp.zeros(ys_deep.shape, ys_deep.dtype)
    for axis, high in neighbour_sides():
        @pl.when(jnp.logical_not(exists(axis, high)))
        def _():
            for buffer in received[axis]:
                for phase in range(buffer.shape[0]):
                    buffer[phase, int(high)] = jnp.zeros(buffer.shape[2:], buffer.dtype)

    row = lax.broadcasted_iota(jnp.int32, (Y, Z), 0)
    lane = lax.broadcasted_iota(jnp.int32, (Y, Z), 1)
    zero = jnp.zeros((Y, Z), jnp.float32)

    def pack(fields, width, phase, xs, ys, zs):
        packed = zero
        for c in range(C):
            for x in range(width):
                k = c * width + x
                field = fields[c][x]
                ys[phase, 0, k : k + 1] = field[0:1]
                ys[phase, 1, k : k + 1] = field[Y - 1 : Y]
                packed = jnp.where(lane == k, field[:, 0:1], packed)
                packed = jnp.where(lane == half + k, field[:, Z - 1 : Z], packed)
        zs[phase] = packed

    def copies(fine, phase):
        number = phase
        xs, xr, ys, yr, zs, zr = xs_fine, xr_fine, ys_fine, yr_fine, zs_fine, zr_fine
        made = []
        for slot, (axis, high) in enumerate(neighbour_sides()):
            side = int(high)
            if axis == "gx":
                if fine and phase == 0:
                    src = v_ref.at[:, X - 1 if high else 0]
                else:
                    src = xs.at[phase, side]
                dst = xr.at[phase, 1 - side]
            elif axis == "gy":
                src, dst = ys.at[phase, side], yr.at[phase, 1 - side]
            else:
                src, dst = zs.at[phase], zr.at[phase, 1 - side]
            made.append((
                axis,
                high,
                pltpu.make_async_remote_copy(
                    src_ref=src,
                    dst_ref=dst,
                    send_sem=send_sem.at[number, slot],
                    recv_sem=recv_sem.at[number, slot],
                    device_id={axis: me[axis] + (1 if high else -1)},
                    device_id_type=MESH,
                ),
            ))
        return made

    def start(fine, phase, axes=("gx", "gy", "agg")):
        for axis, high, copy in copies(fine, phase):
            if axis in axes:
                pl.when(exists(axis, high))(copy.start)

    def send(fine, phase, fields, width):
        xs, ys, zs = fine_send
        for c in range(C):
            xs[phase, 0, c] = fields[c][0]
            xs[phase, 1, c] = fields[c][width - 1]
        start(fine, phase, ("gx",))
        pack(fields, width, phase, xs, ys, zs)
        start(fine, phase, ("gy", "agg"))

    def arrive(fine, phase):
        for axis, high, copy in copies(fine, phase):
            pl.when(exists(axis, not high))(copy.wait_recv)

    def sent(fine, phase):
        for axis, high, copy in copies(fine, phase):
            pl.when(exists(axis, high))(copy.wait_send)

    def inner_sum(fields, width, stride):
        sums = []
        for c in range(C):
            line = []
            for x in range(width):
                field = fields[c][x]
                total = jnp.where(row < stride, zero, pltpu.roll(field, stride, 0))
                total = total + jnp.where(row >= Y - stride, zero, pltpu.roll(field, Y - stride, 0))
                total = total + jnp.where(lane < stride, zero, pltpu.roll(field, stride, 1))
                total = total + jnp.where(lane >= Z - stride, zero, pltpu.roll(field, Z - stride, 1))
                if x > 0:
                    total = total + fields[c][x - 1]
                if x < width - 1:
                    total = total + fields[c][x + 1]
                line.append(total)
            sums.append(line)
        return sums

    def outer_sum(sums, width, stride, faces, repeat=1):
        along_x, along_y, along_z = faces
        result = []
        for c in range(C):
            line = []
            for x in range(width):
                k = c * (width // repeat) + x // repeat
                total = sums[c][x]
                total = total + jnp.where(row < stride, along_y[0][k : k + 1], 0.0)
                total = total + jnp.where(row >= Y - stride, along_y[1][k : k + 1], 0.0)
                total = total + jnp.where(lane < stride, along_z[0][:, k : k + 1], 0.0)
                total = total + jnp.where(lane >= Z - stride, along_z[1][:, k : k + 1], 0.0)
                if x == 0:
                    total = total + along_x[0][c]
                if x == width - 1:
                    total = total + along_x[1][c]
                line.append(total)
            result.append(line)
        return result

    def faces_of(xr, yr, zr, phase):
        return (
            [[xr[phase, side, c] for c in range(C)] for side in range(2)],
            [yr[phase, side] for side in range(2)],
            [pltpu.roll(zr[phase, 0], half, 1), zr[phase, 1]],
        )

    group = Z // 4
    far = {0: 2, 1: 0}

    def rows_of(width):
        return -(-C * width // 8) * 8

    def deep_copies(phase):
        made = []
        rows = pl.ds(0, rows_of(X if phase == 0 else Xc))
        for slot, (first, second) in enumerate(edge_sides()):
            number = 2 * int(first[1]) + int(second[1])
            back = 3 - number
            if second[0] == "gy":
                src, dst = ys_deep.at[phase, int(second[1]), 0, rows], exy.at[phase, back, rows]
            else:
                src, dst = zs_deep.at[phase], (exz if first[0] == "gx" else eyz).at[phase, back]
            made.append(((first, second), src, dst, 6 + slot))
        for slot, (axis, high) in enumerate(neighbour_sides()):
            side = int(high)
            if axis == "gx":
                src, dst = xs_deep.at[phase, side], xr_deep.at[phase, 1 - side]
            elif axis == "gy":
                src, dst = ys_deep.at[phase, side, :, rows], yr_deep.at[phase, 1 - side, :, rows]
            else:
                src, dst = zs_deep.at[phase], zr_deep.at[phase, 1 - side]
            made.append((((axis, high),), src, dst, slot))
        return [
            (
                sides,
                pltpu.make_async_remote_copy(
                    src_ref=src,
                    dst_ref=dst,
                    send_sem=deep_send_sem.at[phase, slot],
                    recv_sem=deep_recv_sem.at[phase, slot],
                    device_id=beside(*sides),
                    device_id_type=MESH,
                ),
            )
            for sides, src, dst, slot in made
        ]

    def deep_send(phase, fields, width, stride):
        for c in range(C):
            for depth in range(2):
                xs_deep[phase, 0, depth, c] = fields[c][depth]
                xs_deep[phase, 1, depth, c] = fields[c][width - 1 - depth]
        ready = deep_copies(phase)
        packed = zero
        for c in range(C):
            for x in range(width):
                k = c * width + x
                field = fields[c][x]
                for depth in range(2):
                    at = depth * stride
                    ys_deep[phase, 0, depth, k : k + 1] = field[at : at + 1]
                    ys_deep[phase, 1, depth, k : k + 1] = field[Y - 1 - at : Y - at]
                    packed = jnp.where(lane == depth * group + k, field[:, at : at + 1], packed)
                    packed = jnp.where(
                        lane == (2 + depth) * group + k, field[:, Z - 1 - at : Z - at], packed
                    )
        zs_deep[phase] = packed
        for sides, copy in ready:
            pl.when(all_exist(sides, False))(copy.start)

    def deep_arrive(phase):
        for sides, copy in deep_copies(phase):
            pl.when(all_exist(sides, True))(copy.wait_recv)

    def deep_sent(phase):
        for sides, copy in deep_copies(phase):
            pl.when(all_exist(sides, False))(copy.wait_send)

    def lanes_from(packed, number, shift=0):
        turn = (shift - number * group) % Z
        return pltpu.roll(packed, turn, 1) if turn else packed

    def deep_faces(phase):
        return (
            [[xr_deep[phase, side, 0, c] for c in range(C)] for side in range(2)],
            [yr_deep[phase, side, 0, : rows_of(X if phase == 0 else Xc)] for side in range(2)],
            [lanes_from(zr_deep[phase, side], far[side]) for side in range(2)],
        )

    def advance_faces(phase, fields, width, stride, faces, added, weight):
        along_x, along_y, along_z = [], [], []
        rows = rows_of(width)
        k_row = lax.broadcasted_iota(jnp.int32, (rows, Z), 0)
        k_lane = lax.broadcasted_iota(jnp.int32, (rows, Z), 1)
        for side in range(2):
            near = width - 1 if side == 0 else 0
            planes = []
            for c in range(C):
                plane = faces[0][side][c]
                k = c * width + near
                total = xr_deep[phase, side, 1, c] + fields[c][0 if side == 0 else width - 1]
                total = total + jnp.where(
                    row < stride, exy[phase, 2 * side, k : k + 1], pltpu.roll(plane, stride, 0)
                )
                total = total + jnp.where(
                    row >= Y - stride, exy[phase, 2 * side + 1, k : k + 1], pltpu.roll(plane, Y - stride, 0)
                )
                low = exz[phase, 2 * side][:, far[0] * group + k : far[0] * group + k + 1]
                high = exz[phase, 2 * side + 1][:, far[1] * group + k : far[1] * group + k + 1]
                total = total + jnp.where(lane < stride, low, pltpu.roll(plane, stride, 1))
                total = total + jnp.where(lane >= Z - stride, high, pltpu.roll(plane, Z - stride, 1))
                planes.append(keep * plane + added[0][side][c] + weight[0][side][c] * total)
            along_x.append(planes)

            layer = faces[1][side]
            total = yr_deep[phase, side, 1, :rows] + ys_deep[phase, side, 0, :rows]
            spot = k_row % width
            total = total + jnp.where(
                spot == 0, pltpu.roll(exy[phase, side, :rows], rows - (width - 1), 0), pltpu.roll(layer, 1, 0)
            )
            total = total + jnp.where(
                spot == width - 1, pltpu.roll(exy[phase, 2 + side, :rows], width - 1, 0), pltpu.roll(layer, rows - 1, 0)
            )
            at = Y - 1 if side == 0 else 0
            ends = []
            for z_side in range(2):
                line = eyz[phase, 2 * side + z_side, at : at + 1]
                chosen = jnp.where(k_lane == far[z_side] * group + k_row, line, 0.0)
                ends.append(jnp.sum(chosen, axis=1, keepdims=True))
            total = total + jnp.where(k_lane < stride, ends[0], pltpu.roll(layer, stride, 1))
            total = total + jnp.where(k_lane >= Z - stride, ends[1], pltpu.roll(layer, Z - stride, 1))
            along_y.append(keep * layer + added[1][side] + weight[1][side] * total)

            layer = faces[2][side]
            total = lanes_from(zr_deep[phase, side], far[side] + 1)
            total = total + lanes_from(zs_deep[phase], 2 - far[side])
            low = lanes_from(eyz[phase, side], far[side])[Y - 1 : Y]
            high = lanes_from(eyz[phase, 2 + side], far[side])[0:1]
            total = total + jnp.where(row < stride, low, pltpu.roll(layer, stride, 0))
            total = total + jnp.where(row >= Y - stride, high, pltpu.roll(layer, Y - stride, 0))
            spot = lane % width
            total = total + jnp.where(
                spot == 0, lanes_from(exz[phase, side], far[side], 1 - width), pltpu.roll(layer, 1, 1)
            )
            total = total + jnp.where(
                spot == width - 1, lanes_from(exz[phase, 2 + side], far[side], width - 1), pltpu.roll(layer, Z - 1, 1)
            )
            along_z.append(keep * layer + added[2][side] + weight[2][side] * total)
        return along_x, along_y, along_z

    fine_recv = (xr_fine, yr_fine, zr_fine)
    fine_send = (xs_fine, ys_fine, zs_fine)

    loads[0].wait()
    previous = [[v_ref[c, x] for x in range(X)] for c in range(C)]
    pack(previous, X, 0, *fine_send)
    pl.semaphore_wait(barrier, expected)
    start(True, 0)

    loads[1].wait()
    loads[2].wait()
    for x in range(X):
        w_buf[x] = damping / (6.0 + r_ref[x])
    scaled = [[w_buf[x] * f_ref[c, x] for x in range(X)] for c in range(C)]
    send(True, 1, scaled, X)
    send(True, 2, [[w_buf[x] for x in range(X)]] * C, X)

    kept = X // 2
    parts = Y // 8
    even_row = row % 2 == 0
    even_lane = lane % 2 == 0
    combos_per_tile = Z // chunk
    def c_copy(j, source):
        return pltpu.make_async_remote_copy(
            src_ref=c_send.at[j],
            dst_ref=c_recv.at[source],
            send_sem=c_send_sem.at[j],
            recv_sem=c_recv_sem.at[source],
            device_id={"gx": j},
            device_id_type=MESH,
        )

    def finish_compressed(tiles):
        coefs = blocks * kept
        for tile in tiles:
            gathered = c_recv[:, tile].reshape(coefs * 8, Z)
            done = lax.dot_general(
                m_ref[...], gathered, (((1,), (0,)), ((), ())),
                precision=lax.Precision.HIGHEST, preferred_element_type=jnp.float32,
            )
            for place in range(combos_per_tile):
                c, part = divmod(tile * combos_per_tile + place, parts)
                if c < C:
                    for y in range(8):
                        comp_ref[c, part * 8 + y] = done[
                            y * coefs : (y + 1) * coefs, place * chunk : (place + 1) * chunk
                        ]

    tiles_y = Y // 8
    lane8 = lax.broadcasted_iota(jnp.int32, (8, Z), 1)
    row_in = lax.broadcasted_iota(jnp.int32, (8, Z), 0)
    even_l = lane8 % 2 == 0
    even_r = row_in % 2 == 0
    slot_at = lane8 % 16
    lane_roll = lambda t, shift: pltpu.roll(t, shift % Z, 1) if shift % Z else t
    row_roll = lambda t, shift: pltpu.roll(t, shift % 8, 0)
    lane_swap = lambda t: jnp.where(even_l, lane_roll(t, -1), lane_roll(t, 1))
    row_swap = lambda t: jnp.where(even_r, row_roll(t, -1), row_roll(t, 1))
    corner_of = ((0, 0), (0, 1), (1, 1), (1, 0))

    def pooled(planes):
        pairs = [planes[x] + planes[x + 1] for x in range(0, X, 2)]
        out = []
        for t in range(tiles_y):
            t0, t1, t2, t3 = (pair[t * 8 : t * 8 + 8] for pair in pairs)
            left = jnp.where(even_r, t0, t3) + row_swap(jnp.where(even_r, t3, t0))
            right = jnp.where(even_r, t1, t2) + row_swap(jnp.where(even_r, t2, t1))
            out.append(jnp.where(even_l, left, right) + lane_swap(jnp.where(even_l, right, left)))
        return out

    def edge_lanes(fields, t):
        packed = jnp.zeros((8, Z), jnp.float32)
        for start, field in fields:
            for depth in range(1, 5):
                high = (lane8 >= start + 8 - 2 * depth) & (lane8 < start + 10 - 2 * depth)
                packed = jnp.where(high, lane_roll(field[t], start + 10 - 4 * depth), packed)
                low = (lane8 >= start + 6 + 2 * depth) & (lane8 < start + 8 + 2 * depth)
                packed = jnp.where(low, lane_roll(field[t], start + 6 + 4 * depth), packed)
        return packed

    coarse_weight = [
        damping / ((6.0 + 0.5 * total) * 0.25) for total in pooled([r_ref[x] for x in range(X)])
    ]
    coarse_step = [0.25 * weight for weight in coarse_weight]
    step_edges = [edge_lanes([(64 + 16 * c, coarse_step) for c in range(C)], t) for t in range(tiles_y)]
    for t in range(tiles_y):
        q_ext[1, C, t * 8 : t * 8 + 8] = coarse_step[t]

    def fine_sums(current):
        inner = inner_sum(current, X, 1)
        return [[inner[c][x] + f_ref[c, x] for x in range(X)] for c in range(C)]

    def fine_sweep(current, total):
        return [[keep * current[c][x] + w_buf[x] * total[c][x] for x in range(X)] for c in range(C)]

    sums = fine_sums(previous)
    arrive(True, 0)
    field = fine_sweep(previous, outer_sum(sums, X, 1, faces_of(*fine_recv, 0)))
    deep_send(0, field, X, 1)

    levels = local_levels(X)
    coefficients = []
    for c in range(C):
        approx, details = previous[c], []
        for level in range(levels):
            low, high = approx[0::2], approx[1::2]
            approx = [(a + b) * root_half for a, b in zip(low, high)]
            if level > 0:
                details = [(a - b) * root_half for a, b in zip(low, high)] + details
        line = []
        for values in approx + details:
            swapped = jnp.where(even_lane, pltpu.roll(values, Z - 1, 1), pltpu.roll(values, 1, 1))
            line.append((jnp.where(even_lane, values, -values) + swapped) * root_half)
        coefficients.append(line)
    row8 = lax.broadcasted_iota(jnp.int32, (8, Z), 1)
    for j in range(blocks):
        for k in range(kept):
            tiles = {}
            for c in range(C):
                for part in range(parts):
                    tile, place = divmod(c * parts + part, combos_per_tile)
                    values = coefficients[c][k][part * 8 : part * 8 + 8]
                    shift = (place * chunk - j * chunk) % Z
                    moved = pltpu.roll(values, shift, 1) if shift else values
                    if tile in tiles:
                        moved = jnp.where((row8 >= place * chunk) & (row8 < (place + 1) * chunk), moved, tiles[tile])
                    tiles[tile] = moved
            for tile, value in tiles.items():
                c_send[j, tile, k] = value

    for j in range(blocks):
        pl.when(me["gx"] != j)(c_copy(j, me["gx"]).start)

        @pl.when(me["gx"] == j)
        def _():
            c_recv[j] = c_send[j]

    sums = fine_sums(field)
    arrive(True, 1)
    arrive(True, 2)
    deep_arrive(0)
    faces = deep_faces(0)
    later_faces = advance_faces(
        0, field, X, 1, faces, faces_of(*fine_recv, 1), faces_of(*fine_recv, 2)
    )
    field = fine_sweep(field, outer_sum(sums, X, 1, faces))
    sums = outer_sum(fine_sums(field), X, 1, later_faces)
    correction = []
    for c in range(C):
        rhs = pooled([sums[c][x] - (6.0 + r_ref[x]) * field[c][x] for x in range(X)])
        correction.append([weight * (0.125 * total) for weight, total in zip(coarse_weight, rhs)])
    for c in range(C):
        for t in range(tiles_y):
            q_ext[1, c, t * 8 : t * 8 + 8] = correction[c][t]
    for t in range(tiles_y):
        edges_t = edge_lanes([(16 * c, correction[c]) for c in range(C)], t)
        zs_coarse[t * 8 : t * 8 + 8] = jnp.where(lane8 < 64, edges_t, step_edges[t])
    for sides, copy in coarse_copies():
        pl.when(all_exist(sides, False))(copy.start)

    for j in range(blocks):
        pl.when(me["gx"] != j)(c_copy(j, j).wait_recv)
    loads[3].wait()
    finish_compressed(range(c_send.shape[1]))

    for sides, copy in coarse_copies():
        pl.when(all_exist(sides, True))(copy.wait_recv)

    near, ring = range(tiles_y), range(tiles_y + 2)
    after = lambda t: (t + 1) % len(ring)
    before = lambda t: (t - 1) % len(ring)
    tile_of = lambda t: slice(t * 8, t * 8 + 8)
    main = {(b, c, t): q_ext[b, c, tile_of(t)] for b in range(3) for c in range(C) for t in ring}
    step_main = {(b, t): q_ext[b, C, tile_of(t)] for b in range(3) for t in ring}
    edge = {
        (b, t): jnp.where(slot_at < 8, h_ext[1, b, tile_of(t)], h_ext[0, b, tile_of(t)])
        for b in range(3) for t in ring
    }
    step_edge = {key: lane_roll(value, -64) for key, value in edge.items()}
    first_main, first_edge = dict(main), dict(edge)

    def above(get, t):
        return jnp.where(row_in < 6, row_roll(get(t), -2), row_roll(get(after(t)), -2))

    def below(get, t):
        return jnp.where(row_in >= 2, row_roll(get(t), 2), row_roll(get(before(t)), 2))

    def along(get, b, t):
        low, high = get(max(b - 1, 0), t), get(min(b + 1, 2), t)
        across = jnp.where(even_l, jnp.where(even_r, high, low), get(b, t))
        return lane_swap(get(b, t)) + row_swap(across)

    def inject(edge, b, c, t):
        return lane_roll(edge[b, t], -(16 * c + 8))

    def left_of(main, edge, b, c, t):
        return jnp.where(lane8 < 2, inject(edge, b, c, t), lane_roll(main[b, c, t], 2))

    def right_of(main, edge, b, c, t):
        return jnp.where(lane8 >= Z - 2, inject(edge, b, c, t), lane_roll(main[b, c, t], -2))

    def coarse_sweep(main, edge, main_at, edge_at):
        new_main, new_edge = dict(main), dict(edge)
        for b, t in main_at:
            for c in range(C):
                get = lambda b, t, c=c: main[b, c, t]
                row_get = lambda t, b=b, c=c: main[b, c, t]
                total = along(get, b, t) + (above(row_get, t) + below(row_get, t))
                total = total + (left_of(main, edge, b, c, t) + right_of(main, edge, b, c, t))
                new_main[b, c, t] = keep * main[b, c, t] + first_main[b, c, t] + step_main[b, t] * total
        for b, t in edge_at:
            get = lambda b, t: edge[b, t]
            row_get = lambda t, b=b: edge[b, t]
            own = lane_roll(main[b, 0, t], 8)
            for c in range(1, C):
                own = jnp.where(lane8 < 16 * c, own, lane_roll(main[b, c, t], 16 * c + 8))
            total = along(get, b, t) + (above(row_get, t) + below(row_get, t))
            total = total + jnp.where((slot_at == 8) | (slot_at == 9), own, lane_roll(edge[b, t], 2))
            total = total + jnp.where((slot_at == 6) | (slot_at == 7), own, lane_roll(edge[b, t], -2))
            new_edge[b, t] = keep * edge[b, t] + first_edge[b, t] + step_edge[b, t] * total
        return new_main, new_edge

    everywhere = [(b, t) for b in range(3) for t in ring]
    centre = [(1, t) for t in ring]
    sides_near = [(b, t) for b in (0, 2) for t in near]
    main, edge = coarse_sweep(main, edge, everywhere, everywhere)
    main, edge = coarse_sweep(main, edge, everywhere, centre + sides_near)
    main, edge = coarse_sweep(main, edge, centre + sides_near, [(1, t) for t in near])

    def spread_rows(even, odd, pa):
        if pa == 0:
            return jnp.where(even_r, even, row_roll(odd, 1))
        return jnp.where(even_r, row_roll(even, -1), odd)

    def spread_lanes(even, odd, pb):
        if pb == 0:
            return jnp.where(even_l, even, lane_roll(odd, 1))
        return jnp.where(even_l, lane_roll(even, -1), odd)

    for c in range(C):
        for t in near:
            at = tile_of(t)
            row_get = lambda t, c=c: main[1, c, t]
            own = main[1, c, t]
            rows_near = (below(row_get, t), above(row_get, t))
            lanes_near = (left_of(main, edge, 1, c, t), right_of(main, edge, 1, c, t))
            alone = [spread_lanes(own, own, pb) for pb in range(2)]
            spread = [spread_rows(alone[pb], alone[pb], pa) for pa, pb in corner_of]
            low, high = (spread_lanes(main[b, c, t], main[b, c, t], 0) for b in (0, 2))
            spread = [spread_rows(low, low, 1)] + spread + [spread_rows(high, high, 0)]
            based = [3.0 * own + rows_near[a] for a in range(2)]
            wide = [
                [spread_lanes(based[a] + lanes_near[0], based[a] + lanes_near[1], pb) for pb in range(2)]
                for a in range(2)
            ]
            for x in range(X):
                p = x // 2
                pa, pb = corner_of[p]
                added = spread_rows(wide[0][pb], wide[1][pb], pa) + spread[p + 2 * (x % 2)]
                total = sums[c][x][at] + added
                vel_ref[c, x, at] = keep * (field[c][x][at] + spread[p + 1]) + w_buf[x, at] * total

    for phase in range(SWEEPS + 1):
        sent(True, phase)
    deep_sent(0)
    for sides, copy in coarse_copies():
        pl.when(all_exist(sides, False))(copy.wait_send)
    for j in range(blocks):
        pl.when(me["gx"] != j)(c_copy(j, me["gx"]).wait_send)


def on_device(counts, velocity_prev, forcing, reaction):
    C, X, Y, Z = velocity_prev.shape
    blocks = counts["gx"]
    kept = X // 2
    chunk = Z // blocks
    tiles = -(-(C * (Y // 8)) // (Z // chunk))
    matrix = jnp.asarray(finish_matrix(X, blocks, 8))
    vmem = pl.BlockSpec(memory_space=pltpu.VMEM)

    def buffers(phases, width):
        return [
            pltpu.VMEM((phases, 2, C, Y, Z), jnp.float32),
            pltpu.VMEM((phases, 2, C, Y, Z), jnp.float32),
            pltpu.VMEM((phases, 2, -(-C * width // 8) * 8, Z), jnp.float32),
            pltpu.VMEM((phases, 2, -(-C * width // 8) * 8, Z), jnp.float32),
            pltpu.VMEM((phases, Y, Z), jnp.float32),
            pltpu.VMEM((phases, 2, Y, Z), jnp.float32),
        ]

    def deep_buffers(phases, width):
        rows = -(-C * width // 8) * 8
        return [
            pltpu.VMEM((phases, 2, 2, C, Y, Z), jnp.float32),
            pltpu.VMEM((phases, 2, 2, C, Y, Z), jnp.float32),
            pltpu.VMEM((phases, 2, 2, rows, Z), jnp.float32),
            pltpu.VMEM((phases, 2, 2, rows, Z), jnp.float32),
            pltpu.VMEM((phases, Y, Z), jnp.float32),
            pltpu.VMEM((phases, 2, Y, Z), jnp.float32),
            pltpu.VMEM((phases, 4, rows, Z), jnp.float32),
            pltpu.VMEM((phases, 4, Y, Z), jnp.float32),
            pltpu.VMEM((phases, 4, Y, Z), jnp.float32),
        ]

    phases = SWEEPS + 1
    velocity, compressed = pl.pallas_call(
        functools.partial(kernel, counts),
        out_shape=(
            jax.ShapeDtypeStruct((C, X, Y, Z), jnp.float32),
            jax.ShapeDtypeStruct((C, Y, kept * blocks, chunk), jnp.float32),
        ),
        in_specs=[pl.BlockSpec(memory_space=pltpu.HBM)] * 4,
        out_specs=(vmem, vmem),
        scratch_shapes=[
            pltpu.VMEM((C, X, Y, Z), jnp.float32),
            pltpu.VMEM((C, X, Y, Z), jnp.float32),
            pltpu.VMEM((X, Y, Z), jnp.float32),
            pltpu.VMEM(matrix.shape, jnp.float32),
        ] + buffers(SWEEPS + 1, X) + [
            pltpu.VMEM((3, C + 1, Y + 16, Z), jnp.float32),
            pltpu.VMEM((2, 3, Y + 16, Z), jnp.float32),
            pltpu.VMEM((Y, Z), jnp.float32),
        ] + deep_buffers(1, X) + [
            pltpu.VMEM((blocks, tiles, kept, 8, Z), jnp.float32),
            pltpu.VMEM((blocks, tiles, kept, 8, Z), jnp.float32),
            pltpu.VMEM((X, Y, Z), jnp.float32),
            pltpu.SemaphoreType.DMA((phases, 6)),
            pltpu.SemaphoreType.DMA((phases, 6)),
            pltpu.SemaphoreType.DMA((1, 18)),
            pltpu.SemaphoreType.DMA((1, 18)),
            pltpu.SemaphoreType.DMA((26,)),
            pltpu.SemaphoreType.DMA((26,)),
            pltpu.SemaphoreType.DMA((blocks,)),
            pltpu.SemaphoreType.DMA((blocks,)),
            pltpu.SemaphoreType.DMA((4,)),
        ],
        compiler_params=pltpu.CompilerParams(collective_id=0, has_side_effects=True, vmem_limit_bytes=40000000),
    )(*(pltpu.with_memory_space_constraint(a, pltpu.HBM) for a in (velocity_prev, forcing, reaction, matrix)))
    return velocity, jnp.swapaxes(compressed, 2, 3)


def solution(mesh):
    counts = {axis: mesh.shape[axis] for axis in ("agg", "gx", "gy")}
    placed = (P(None, "gx", "gy", "agg"), P(None, "gx", "gy", "agg"), P("gx", "gy", "agg"))
    return jax.shard_map(
        functools.partial(on_device, counts),
        mesh=mesh,
        in_specs=placed,
        out_specs=(P(None, "gx", "gy", "agg"), P(None, "gy", ("agg", "gx"), None)),
        check_vma=False,
    )
```

```python
import functools

import jax
import jax.numpy as jnp
import numpy as np
from jax import lax
from jax.experimental import pallas as pl
from jax.experimental.pallas import tpu as pltpu
from jax.sharding import PartitionSpec as P

SWEEPS = 2
COARSE_SWEEPS = 4
LX = 5
MESH = pl.DeviceIdType.MESH

damping = 0.8
keep = 1.0 - damping
root_half = 0.7071067811865476


def local_levels(cells_x):
    return min(LX, cells_x.bit_length() - 1)


def finish_matrix(cells_x, blocks, rows):
    levels = local_levels(cells_x)
    kept = cells_x // 2
    eye = np.eye(blocks * kept).reshape(blocks, kept, blocks * kept)
    width = cells_x >> levels
    approx = eye[:, :width].reshape(blocks * width, -1)
    details, at = [], width
    for level in range(levels, 1, -1):
        width = cells_x >> level
        details.append(eye[:, at : at + width].reshape(blocks * width, -1))
        at += width
    for level in range(levels, LX):
        low, high = approx[0::2], approx[1::2]
        approx, detail = (low + high) * root_half, (low - high) * root_half
        details.insert(0, detail)
    along_x = np.concatenate([approx] + details, axis=0)
    along_y = np.zeros((rows, rows))
    for row in range(0, rows, 2):
        along_y[row, row : row + 2] = root_half
        along_y[row + 1, row : row + 2] = root_half, -root_half
    return np.einsum("qk,yr->yqkr", along_x, along_y).reshape(-1, blocks * kept * rows).astype(np.float32)


def around():
    axes = ("gx", "gy", "agg")
    found = []
    for number in range(1, 27):
        turn = [(number // 3**i) % 3 for i in range(3)]
        found.append(tuple((axis, way == 1) for axis, way in zip(axes, turn) if way))
    return sorted(found, key=lambda sides: (-len(sides), sides))


far = 1e30


def kernel(
    sizes, v_hbm, f_hbm, r_hbm, m_hbm, vel_ref, comp_ref, v_ext, f_ext, r_ext, m_ref, w_ext, u1_ext, u2_ext,
    y_send, y_recv, xy_send, xy_recv, z_send, z_recv, yz_send, yz_recv, xz_send, xz_recv, corner_recv,
    q_ext, h_ext, zs_coarse, c_send, c_recv,
    a_send_sem, a_recv_sem, q_send_sem, q_recv_sem, c_send_sem, c_recv_sem, in_sem,
):
    counts = sizes
    C, X, Y, Z = vel_ref.shape
    me = {axis: lax.axis_index(axis) for axis in counts}
    blocks = counts["gx"]
    chunk = Z // blocks
    rows_ext = Y + 8
    f32 = jnp.float32

    loads = [
        pltpu.make_async_copy(src, dst, in_sem.at[i])
        for i, (src, dst) in enumerate((
            (v_hbm, v_ext.at[:, 3 : 3 + X, :Y]),
            (f_hbm, f_ext.at[:, 2 : 2 + X, :Y]),
            (r_hbm, r_ext.at[2 : 2 + X, :Y]),
            (m_hbm, m_ref),
        ))
    ]
    for load in loads:
        load.start()

    def exists(axis, high):
        return me[axis] < counts[axis] - 1 if high else me[axis] > 0

    def all_exist(sides, flip):
        there = None
        for axis, high in sides:
            one = exists(axis, high != flip)
            there = one if there is None else there & one
        return there

    def beside(*sides):
        return {axis: me[axis] + (1 if high else -1) for axis, high in sides}

    barrier = pltpu.get_barrier_semaphore()
    expected = blocks - 1
    for step in range(1, blocks):
        pl.semaphore_signal(
            barrier, inc=1, device_id={"gx": lax.rem(me["gx"] + step, blocks)}, device_id_type=MESH
        )
    for sides in around():
        if len(sides) > 1 or sides[0][0] != "gx":
            there = all_exist(sides, False)
            expected = expected + there.astype(jnp.int32)

            @pl.when(there)
            def _():
                pl.semaphore_signal(barrier, inc=1, device_id=beside(*sides), device_id_type=MESH)

    lane = lax.broadcasted_iota(jnp.int32, (8, Z), 1)
    row = lax.broadcasted_iota(jnp.int32, (8, Z), 0)
    place = lane % 8
    group = lane // 8
    low_half = (lane < 32) | (lane >= 96)
    near_groups = (group % 8 == 2) | (group % 8 == 3) | (group % 8 == 4) | (group % 8 == 5)

    def fine_messages(sides):
        at = {axis: high for axis, high in sides}
        x, y, z = at.get("gx"), at.get("gy"), at.get("agg")
        from_x, from_y, from_z = 0 if x else 1, 0 if y else 1, 0 if z else 1
        if z is None and y is None:
            made = []
            for ref, depth, fill in ((v_ext, 3, 0.0), (f_ext, 2, 0.0), (r_ext, 2, far)):
                here = pl.ds(X if x else depth, depth)
                there = pl.ds(0 if x else depth + X, depth)
                index = (slice(None),) if ref is not r_ext else ()
                made.append((ref.at[index + (here, pl.ds(0, Y))], ref.at[index + (there, pl.ds(0, Y))], fill))
            return made
        if z is None and x is None:
            return [(y_send.at[int(y)], y_recv.at[from_y], None)]
        if z is None:
            return [(xy_send.at[2 * int(x) + int(y)], xy_recv.at[2 * from_x + from_y], None)]
        if x is None and y is None:
            return [(z_send, z_recv.at[from_z, :, pl.ds(0, Y)], None)]
        if x is None:
            return [(yz_send.at[int(y)], yz_recv.at[from_z, from_y], None)]
        if y is None:
            return [(xz_send, xz_recv.at[from_z, from_x], None)]
        return [(xz_send.at[0, pl.ds(Y - 8 if y else 0, 8)], corner_recv.at[from_z, from_x, from_y], 0.0)]

    def remote(src, dst, send_sem, recv_sem, sides):
        return pltpu.make_async_remote_copy(
            src_ref=src, dst_ref=dst, send_sem=send_sem, recv_sem=recv_sem,
            device_id=beside(*sides), device_id_type=MESH,
        )

    def fine_copies():
        made, slot = [], 0
        for sides in around():
            for src, dst, _ in fine_messages(sides):
                made.append((sides, remote(src, dst, a_send_sem.at[slot], a_recv_sem.at[slot], sides)))
                slot += 1
        return made

    def start_fine(chosen):
        for sides, copy in fine_copies():
            if chosen(tuple(axis for axis, _ in sides)):
                pl.when(all_exist(sides, False))(copy.start)

    def coarse_message(sides):
        at = {axis: 1 if high else -1 for axis, high in sides}
        block = 1 - at.get("gx", 0)
        here, there = {
            0: (slice(0, Y), slice(0, Y)),
            1: (slice(Y - 8, Y), slice(Y + 8, Y + 16)),
            -1: (slice(0, 8), slice(Y, Y + 8)),
        }[at.get("gy", 0)]
        if "agg" in at:
            return zs_coarse.at[here], h_ext.at[0 if at["agg"] > 0 else 1, block, there]
        return q_ext.at[1, :, here], q_ext.at[block, :, there]

    def coarse_copies():
        return [
            (sides, remote(*coarse_message(sides), q_send_sem.at[slot], q_recv_sem.at[slot], sides))
            for slot, sides in enumerate(around())
        ]

    far_high = jnp.where(low_half, far, 0.0).astype(f32)
    for sides in around():
        @pl.when(jnp.logical_not(all_exist(sides, True)))
        def _():
            axes = tuple(axis for axis, _ in sides)
            for _, target, fill in fine_messages(sides):
                if fill is not None:
                    target[...] = jnp.full(target.shape, fill, f32)
                elif axes == ("gy",):
                    target[: 5 * C] = jnp.zeros((5 * C, 8, Z), f32)
                    target[5 * C :] = jnp.full((2, 8, Z), far, f32)
                elif axes == ("gx", "gy"):
                    target[0:8] = jnp.zeros((8, Z), f32)
                    target[8:16] = jnp.where(row == 4 * C - 8, far, 0.0)
                elif axes == ("agg",):
                    target[:3] = jnp.zeros((3, Y, Z), f32)
                    for t in range(Y // 8):
                        target[3, t * 8 : t * 8 + 8] = far_high
                elif axes == ("gy", "agg"):
                    target[...] = jnp.where(row >= 6, far_high, 0.0)
                else:
                    target[0] = jnp.zeros((Y, Z), f32)
                    for t in range(Y // 8):
                        target[1, t * 8 : t * 8 + 8] = jnp.where(
                            (group == 0) | (group == 1) | (group == 6) | (group == 7), far, 0.0
                        )
            target = coarse_message(sides)[1]
            target[...] = jnp.zeros(target.shape, f32)

    tiles_y = Y // 8
    near, ring = range(tiles_y), range(tiles_y + 1)
    tile_of = lambda t: slice(t * 8, t * 8 + 8)
    even_l = lane % 2 == 0
    even_r = row % 2 == 0
    lane_roll = lambda t, shift: pltpu.roll(t, shift % Z, 1) if shift % Z else t
    row_roll = lambda t, shift: pltpu.roll(t, shift % 8, 0)
    v_flat = v_ext.reshape(C * (X + 6) * rows_ext, Z)
    f_flat = f_ext.reshape(C * (X + 4) * rows_ext, Z)
    r_flat = r_ext.reshape((X + 4) * rows_ext, Z)

    def x_line(number, y):
        if number < 3 * C:
            c, ref, extra = number // 3, v_flat, 3
        elif number < 5 * C:
            c, ref, extra = (number - 3 * C) // 2, f_flat, 2
        else:
            c, ref, extra = 0, r_flat, 2
        return ref, pl.ds((c * (X + 2 * extra) + extra) * rows_ext + y, X, stride=rows_ext)

    depth_of = lambda number: number % 3 if number < 3 * C else (number - 3 * C) % 2

    loads[0].wait()
    loads[1].wait()
    loads[2].wait()
    for number in range(5 * C + 2):
        for side in range(2):
            depth = depth_of(number)
            ref, at = x_line(number, Y - 1 - depth if side else depth)
            y_send[side, number] = ref[at, :]
    for high_x in range(2):
        for high_y in range(2):
            xs = [X - 1 - d if high_x else d for d in range(2)]
            ys = [Y - 1 - d if high_y else d for d in range(2)]
            target = xy_send.at[2 * high_x + high_y]
            for c in range(C):
                for i, (x, y) in enumerate(((xs[0], ys[0]), (xs[1], ys[0]), (xs[0], ys[1]))):
                    target[3 * c + i : 3 * c + i + 1] = v_ext[c, 3 + x, y : y + 1]
                target[3 * C + c : 3 * C + c + 1] = f_ext[c, 2 + xs[0], ys[0] : ys[0] + 1]
            target[4 * C : 4 * C + 1] = r_ext[2 + xs[0], ys[0] : ys[0] + 1]
    pl.semaphore_wait(barrier, expected)
    start_fine(lambda axes: axes == ("gx", "gy"))
    start_fine(lambda axes: axes in (("gx",), ("gy",)))

    v_at = lambda c, x, t: v_ext[c, 3 + x, tile_of(t)]
    f_at = lambda c, x, t: f_ext[c, 2 + x, tile_of(t)]
    held = (
        (lambda x, t: v_at(0, x, t), lambda x, t: v_at(1, x, t)),
        (lambda x, t: v_at(2, x, t), None),
        (lambda x, t: f_at(0, x, t), lambda x, t: f_at(1, x, t)),
        (lambda x, t: f_at(2, x, t), lambda x, t: r_ext[2 + x, tile_of(t)]),
    )
    for t in near:
        turned = []
        for pair in held:
            packed = jnp.zeros((8, Z), f32)
            for half, get in enumerate(pair):
                if get is not None:
                    for x in range(X):
                        at = (x + 4 + 8 * half) % 16
                        packed = jnp.where(group == at, lane_roll(get(x, t), 8 * at + 3), packed)
            out = jnp.where(place == 3, packed, lane_roll(packed, 6))
            for spot, shift in ((2, -2), (1, -4), (4, 2), (5, 4)):
                out = jnp.where(place == spot, lane_roll(packed, shift), out)
            turned.append(out)
        for i in range(4):
            z_send[i, tile_of(t)] = turned[i]
            for side in range(2):
                if t == (tiles_y - 1 if side else 0):
                    first = 6 if side else 0
                    yz_send[side, 2 * i : 2 * i + 2] = turned[i][first : first + 2]
        for i in range(2):
            xz_send[i, tile_of(t)] = jnp.where(near_groups, turned[2 * i], lane_roll(turned[2 * i + 1], 32))
    start_fine(lambda axes: axes == ("gx", "gy", "agg"))
    start_fine(lambda axes: axes in (("gx", "agg"), ("gy", "agg")))
    start_fine(lambda axes: axes == ("agg",))

    kept = X // 2
    parts = Y // 8
    combos_per_tile = Z // chunk

    def c_copy(j, source):
        return pltpu.make_async_remote_copy(
            src_ref=c_send.at[j],
            dst_ref=c_recv.at[source],
            send_sem=c_send_sem.at[j],
            recv_sem=c_recv_sem.at[source],
            device_id={"gx": j},
            device_id_type=MESH,
        )

    def finish_compressed(tiles):
        coefs = blocks * kept
        for tile in tiles:
            gathered = c_recv[:, tile].reshape(coefs * 8, Z)
            done = lax.dot_general(
                m_ref[...], gathered, (((1,), (0,)), ((), ())),
                precision=lax.Precision.HIGHEST, preferred_element_type=jnp.float32,
            )
            for place in range(combos_per_tile):
                c, part = divmod(tile * combos_per_tile + place, parts)
                if c < C:
                    for y in range(8):
                        comp_ref[c, part * 8 + y] = done[
                            y * coefs : (y + 1) * coefs, place * chunk : (place + 1) * chunk
                        ]

    lane_swap = lambda t: jnp.where(even_l, lane_roll(t, -1), lane_roll(t, 1))
    row_swap = lambda t: jnp.where(even_r, row_roll(t, -1), row_roll(t, 1))
    slot_at = lane % 16
    corner_of = ((0, 0), (0, 1), (1, 1), (1, 0))

    def pooled(planes):
        pairs = [[planes[x][t] + planes[x + 1][t] for t in near] for x in range(0, X, 2)]
        out = []
        for t in near:
            t0, t1, t2, t3 = (pair[t] for pair in pairs)
            left = jnp.where(even_r, t0, t3) + row_swap(jnp.where(even_r, t3, t0))
            right = jnp.where(even_r, t1, t2) + row_swap(jnp.where(even_r, t2, t1))
            out.append(jnp.where(even_l, left, right) + lane_swap(jnp.where(even_l, right, left)))
        return out

    def edge_lanes(fields, t):
        packed = jnp.zeros((8, Z), f32)
        for start, field in fields:
            for depth in range(1, 5):
                high = (lane >= start + 8 - 2 * depth) & (lane < start + 10 - 2 * depth)
                packed = jnp.where(high, lane_roll(field[t], start + 10 - 4 * depth), packed)
                low = (lane >= start + 6 + 2 * depth) & (lane < start + 8 + 2 * depth)
                packed = jnp.where(low, lane_roll(field[t], start + 6 + 4 * depth), packed)
        return packed

    coarse_weight = [
        damping / ((6.0 + 0.5 * total) * 0.25)
        for total in pooled([[r_ext[2 + x, tile_of(t)] for t in near] for x in range(X)])
    ]
    coarse_step = [0.25 * weight for weight in coarse_weight]
    step_edges = [edge_lanes([(64 + 16 * c, coarse_step) for c in range(C)], t) for t in near]
    for t in near:
        q_ext[1, C, tile_of(t)] = coarse_step[t]
        zs_coarse[tile_of(t)] = step_edges[t]
    for x in range(X):
        for t in near:
            w_ext[2 + x, tile_of(t)] = damping / (6.0 + r_ext[2 + x, tile_of(t)])

    levels = local_levels(X)
    for c in range(C):
        for t in near:
            approx, details = [v_at(c, x, t) for x in range(X)], []
            for level in range(levels):
                low, high = approx[0::2], approx[1::2]
                approx = [(a + b) * root_half for a, b in zip(low, high)]
                if level > 0:
                    details = [(a - b) * root_half for a, b in zip(low, high)] + details
            tile, spot = divmod(c * parts + t, combos_per_tile)
            inside = (lane >= spot * chunk) & (lane < (spot + 1) * chunk)
            for k, values in enumerate(approx + details):
                done = (jnp.where(even_l, values, -values) + lane_swap(values)) * root_half
                for j in range(blocks):
                    moved = lane_roll(done, spot * chunk - j * chunk)
                    if spot:
                        moved = jnp.where(inside, moved, c_send[j, tile, k])
                    c_send[j, tile, k] = moved

    for sides, copy in fine_copies():
        pl.when(all_exist(sides, True))(copy.wait_recv)

    for j in range(blocks):
        pl.when(me["gx"] != j)(c_copy(j, me["gx"]).start)

    for number in range(5 * C + 2):
        for side in range(2):
            depth = depth_of(number)
            ref, at = x_line(number, Y + depth if side else rows_ext - 1 - depth)
            ref[at, :] = y_recv[side, number]
    for high_x in range(2):
        for high_y in range(2):
            xs = [X + d if high_x else -1 - d for d in range(2)]
            ys = [Y + d if high_y else rows_ext - 1 - d for d in range(2)]
            source = xy_recv.at[2 * high_x + high_y]
            for c in range(C):
                for i, (x, y) in enumerate(((xs[0], ys[0]), (xs[1], ys[0]), (xs[0], ys[1]))):
                    v_ext[c, 3 + x, y : y + 1] = source[3 * c + i : 3 * c + i + 1]
                f_ext[c, 2 + xs[0], ys[0] : ys[0] + 1] = source[3 * C + c : 3 * C + c + 1]
            r_ext[2 + xs[0], ys[0] : ys[0] + 1] = source[4 * C : 4 * C + 1]
    for side in range(2):
        for i in range(4):
            z_recv[side, i, Y : Y + 2] = yz_recv[side, 1, 2 * i : 2 * i + 2]
            z_recv[side, i, Y + 6 : Y + 8] = yz_recv[side, 0, 2 * i : 2 * i + 2]

    def weight_of(reaction):
        return jnp.where(reaction < 0.1 * far, damping / (6.0 + reaction), 0.0)

    for x in range(-2, X + 2):
        outside = max(-x, x - X + 1)
        for t in ring:
            if (outside > 0 and t < tiles_y) or (t == tiles_y and outside < 2):
                w_ext[2 + x, tile_of(t)] = weight_of(r_ext[2 + x, tile_of(t)])

    mixed = {}
    for i in range(4):
        for t in ring:
            mixed[i, t] = jnp.where(place < 4, z_recv[1, i, tile_of(t)], z_recv[0, i, tile_of(t)])
    beyond = {}
    for side in range(2):
        for i in range(2):
            for t in near:
                beyond[side, i, t] = jnp.where(
                    place < 4, xz_recv[1, side, i, tile_of(t)], xz_recv[0, side, i, tile_of(t)]
                )
        ends = [
            jnp.where(place < 4, corner_recv[1, side, high], corner_recv[0, side, high]) for high in range(2)
        ]
        beyond[side, 0, tiles_y] = jnp.where(row < 4, ends[1], ends[0])

    def edge_field(number, t):
        i, half = divmod(number, 2)
        value = lane_roll(mixed[i, t], 64 * half)
        if t < tiles_y or number < 4:
            shift = (64, 0, 32, -32)[number % 4]
            low, high = (lane_roll(beyond[side, i // 2, t], shift) for side in range(2))
            value = jnp.where(group < 4, low, jnp.where(group >= 12, high, value))
        return value

    edge_v = {(c, t): edge_field(c, t) for c in range(C) for t in ring}
    edge_f = {(c, t): edge_field(4 + c, t) for c in range(C) for t in ring}
    edge_w = {t: weight_of(edge_field(7, t)) for t in ring}

    def around_rows(get, t, tiles, by):
        after, before = (t + 1) % tiles, (t - 1) % tiles
        own = get(t)
        above = jnp.where(row < 8 - by, row_roll(own, -by), row_roll(get(after), -by))
        below = jnp.where(row >= by, row_roll(own, by), row_roll(get(before), by))
        return below, above

    def main_total(get, edge, c, x, t):
        below, above = around_rows(lambda t: get(c, x, t), t, tiles_y + 1, 1)
        total = (get(c, x - 1, t) + get(c, x + 1, t)) + (below + above)
        beside_z = lane_roll(edge[c, t], -(8 * (x + 4) + 4))
        own = get(c, x, t)
        total = total + jnp.where(lane == 0, beside_z, lane_roll(own, 1))
        return total + jnp.where(lane == Z - 1, beside_z, lane_roll(own, -1))

    def edge_total(get, edge, c, xs, t):
        own = edge[c, t]
        line = own
        for x in xs:
            line = jnp.where(group == x + 4, lane_roll(get(c, x, t), 8 * (x + 4) + 4), line)
        below, above = around_rows(lambda t: edge[c, t], t, tiles_y + 1, 1)
        total = (lane_roll(own, 8) + lane_roll(own, -8)) + (below + above)
        total = total + jnp.where(place == 4, line, lane_roll(own, 1))
        return total + jnp.where(place == 3, line, lane_roll(own, -1))

    u1_at = lambda c, x, t: u1_ext[c, 2 + x, tile_of(t)]
    u2_at = lambda c, x, t: u2_ext[c, 1 + x, tile_of(t)]
    w_at = lambda x, t: w_ext[2 + x, tile_of(t)]

    edge_1, edge_2 = {}, {}
    for c in range(C):
        for t in ring:
            total = edge_total(v_at, edge_v, c, range(-1, X + 1), t)
            edge_1[c, t] = keep * edge_v[c, t] + edge_w[t] * (edge_f[c, t] + total)
        for x in range(-2, X + 2):
            for t in near if x in (-2, X + 1) else ring:
                total = main_total(v_at, edge_v, c, x, t)
                u1_ext[c, 2 + x, tile_of(t)] = keep * v_at(c, x, t) + w_at(x, t) * (f_at(c, x, t) + total)
    for c in range(C):
        for t in near:
            total = edge_total(u1_at, edge_1, c, range(X), t)
            edge_2[c, t] = keep * edge_1[c, t] + edge_w[t] * (edge_f[c, t] + total)
        for x in range(-1, X + 1):
            for t in near if x in (-1, X) else ring:
                total = main_total(u1_at, edge_1, c, x, t)
                u2_ext[c, 1 + x, tile_of(t)] = keep * u1_at(c, x, t) + w_at(x, t) * (f_at(c, x, t) + total)
    sums = [
        [[main_total(u2_at, edge_2, c, x, t) + f_at(c, x, t) for t in near] for x in range(X)] for c in range(C)
    ]

    correction = []
    for c in range(C):
        rhs = pooled([
            [sums[c][x][t] - (6.0 + r_ext[2 + x, tile_of(t)]) * u2_at(c, x, t) for t in near] for x in range(X)
        ])
        correction.append([weight * (0.125 * total) for weight, total in zip(coarse_weight, rhs)])
    for c in range(C):
        for t in near:
            q_ext[1, c, tile_of(t)] = correction[c][t]
    for t in near:
        edges_t = edge_lanes([(16 * c, correction[c]) for c in range(C)], t)
        zs_coarse[tile_of(t)] = jnp.where(lane < 64, edges_t, zs_coarse[tile_of(t)])
    for sides, copy in coarse_copies():
        pl.when(all_exist(sides, False))(copy.start)

    for j in range(blocks):
        @pl.when(me["gx"] == j)
        def _():
            c_recv[j] = c_send[j]

    for j in range(blocks):
        pl.when(me["gx"] != j)(c_copy(j, j).wait_recv)
    loads[3].wait()
    finish_compressed(range(c_send.shape[1]))

    for sides, copy in coarse_copies():
        pl.when(all_exist(sides, True))(copy.wait_recv)

    ring = range(tiles_y + 2)
    after = lambda t: (t + 1) % len(ring)
    before = lambda t: (t - 1) % len(ring)
    main = {(b, c, t): q_ext[b, c, tile_of(t)] for b in range(3) for c in range(C) for t in ring}
    step_main = {(b, t): q_ext[b, C, tile_of(t)] for b in range(3) for t in ring}
    edge = {
        (b, t): jnp.where(slot_at < 8, h_ext[1, b, tile_of(t)], h_ext[0, b, tile_of(t)])
        for b in range(3) for t in ring
    }
    step_edge = {key: lane_roll(value, -64) for key, value in edge.items()}
    first_main, first_edge = dict(main), dict(edge)

    def above(get, t):
        return jnp.where(row < 6, row_roll(get(t), -2), row_roll(get(after(t)), -2))

    def below(get, t):
        return jnp.where(row >= 2, row_roll(get(t), 2), row_roll(get(before(t)), 2))

    def along(get, b, t):
        low, high = get(max(b - 1, 0), t), get(min(b + 1, 2), t)
        across = jnp.where(even_l, jnp.where(even_r, high, low), get(b, t))
        return lane_swap(get(b, t)) + row_swap(across)

    def inject(edge, b, c, t):
        return lane_roll(edge[b, t], -(16 * c + 8))

    def left_of(main, edge, b, c, t):
        return jnp.where(lane < 2, inject(edge, b, c, t), lane_roll(main[b, c, t], 2))

    def right_of(main, edge, b, c, t):
        return jnp.where(lane >= Z - 2, inject(edge, b, c, t), lane_roll(main[b, c, t], -2))

    def coarse_sweep(main, edge, main_at, edge_at):
        new_main, new_edge = dict(main), dict(edge)
        for b, t in main_at:
            for c in range(C):
                get = lambda b, t, c=c: main[b, c, t]
                row_get = lambda t, b=b, c=c: main[b, c, t]
                total = along(get, b, t) + (above(row_get, t) + below(row_get, t))
                total = total + (left_of(main, edge, b, c, t) + right_of(main, edge, b, c, t))
                new_main[b, c, t] = keep * main[b, c, t] + first_main[b, c, t] + step_main[b, t] * total
        for b, t in edge_at:
            get = lambda b, t: edge[b, t]
            row_get = lambda t, b=b: edge[b, t]
            own = lane_roll(main[b, 0, t], 8)
            for c in range(1, C):
                own = jnp.where(lane < 16 * c, own, lane_roll(main[b, c, t], 16 * c + 8))
            total = along(get, b, t) + (above(row_get, t) + below(row_get, t))
            total = total + jnp.where((slot_at == 8) | (slot_at == 9), own, lane_roll(edge[b, t], 2))
            total = total + jnp.where((slot_at == 6) | (slot_at == 7), own, lane_roll(edge[b, t], -2))
            new_edge[b, t] = keep * edge[b, t] + first_edge[b, t] + step_edge[b, t] * total
        return new_main, new_edge

    everywhere = [(b, t) for b in range(3) for t in ring]
    centre = [(1, t) for t in ring]
    sides_near = [(b, t) for b in (0, 2) for t in near]
    main, edge = coarse_sweep(main, edge, everywhere, everywhere)
    main, edge = coarse_sweep(main, edge, everywhere, centre + sides_near)
    main, edge = coarse_sweep(main, edge, centre + sides_near, [(1, t) for t in near])

    def spread_rows(even, odd, pa):
        if pa == 0:
            return jnp.where(even_r, even, row_roll(odd, 1))
        return jnp.where(even_r, row_roll(even, -1), odd)

    def spread_lanes(even, odd, pb):
        if pb == 0:
            return jnp.where(even_l, even, lane_roll(odd, 1))
        return jnp.where(even_l, lane_roll(even, -1), odd)

    for c in range(C):
        for t in near:
            at = tile_of(t)
            row_get = lambda t, c=c: main[1, c, t]
            own = main[1, c, t]
            rows_near = (below(row_get, t), above(row_get, t))
            lanes_near = (left_of(main, edge, 1, c, t), right_of(main, edge, 1, c, t))
            alone = [spread_lanes(own, own, pb) for pb in range(2)]
            spread = [spread_rows(alone[pb], alone[pb], pa) for pa, pb in corner_of]
            low, high = (spread_lanes(main[b, c, t], main[b, c, t], 0) for b in (0, 2))
            spread = [spread_rows(low, low, 1)] + spread + [spread_rows(high, high, 0)]
            based = [3.0 * own + rows_near[a] for a in range(2)]
            wide = [
                [spread_lanes(based[a] + lanes_near[0], based[a] + lanes_near[1], pb) for pb in range(2)]
                for a in range(2)
            ]
            for x in range(X):
                p = x // 2
                pa, pb = corner_of[p]
                added = spread_rows(wide[0][pb], wide[1][pb], pa) + spread[p + 2 * (x % 2)]
                total = sums[c][x][t] + added
                vel_ref[c, x, at] = keep * (u2_at(c, x, t) + spread[p + 1]) + w_at(x, t) * total

    for sides, copy in fine_copies():
        pl.when(all_exist(sides, False))(copy.wait_send)
    for sides, copy in coarse_copies():
        pl.when(all_exist(sides, False))(copy.wait_send)
    for j in range(blocks):
        pl.when(me["gx"] != j)(c_copy(j, me["gx"]).wait_send)


def on_device(counts, velocity_prev, forcing, reaction):
    C, X, Y, Z = velocity_prev.shape
    blocks = counts["gx"]
    kept = X // 2
    chunk = Z // blocks
    tiles = -(-(C * (Y // 8)) // (Z // chunk))
    matrix = jnp.asarray(finish_matrix(X, blocks, 8))
    vmem = pl.BlockSpec(memory_space=pltpu.VMEM)
    space = lambda *shape: pltpu.VMEM(shape, jnp.float32)

    velocity, compressed = pl.pallas_call(
        functools.partial(kernel, counts),
        out_shape=(
            jax.ShapeDtypeStruct((C, X, Y, Z), jnp.float32),
            jax.ShapeDtypeStruct((C, Y, kept * blocks, chunk), jnp.float32),
        ),
        in_specs=[pl.BlockSpec(memory_space=pltpu.HBM)] * 4,
        out_specs=(vmem, vmem),
        scratch_shapes=[
            space(C, X + 6, Y + 8, Z),
            space(C, X + 4, Y + 8, Z),
            space(X + 4, Y + 8, Z),
            space(*matrix.shape),
            space(X + 4, Y + 8, Z),
            space(C, X + 4, Y + 8, Z),
            space(C, X + 2, Y + 8, Z),
            space(2, 5 * C + 2, X, Z),
            space(2, 5 * C + 2, X, Z),
            space(4, 16, Z),
            space(4, 16, Z),
            space(4, Y, Z),
            space(2, 4, Y + 8, Z),
            space(2, 8, Z),
            space(2, 2, 8, Z),
            space(2, Y, Z),
            space(2, 2, 2, Y, Z),
            space(2, 2, 2, 8, Z),
            space(3, C + 1, Y + 16, Z),
            space(2, 3, Y + 16, Z),
            space(Y, Z),
            space(blocks, tiles, kept, 8, Z),
            space(blocks, tiles, kept, 8, Z),
            pltpu.SemaphoreType.DMA((30,)),
            pltpu.SemaphoreType.DMA((30,)),
            pltpu.SemaphoreType.DMA((26,)),
            pltpu.SemaphoreType.DMA((26,)),
            pltpu.SemaphoreType.DMA((blocks,)),
            pltpu.SemaphoreType.DMA((blocks,)),
            pltpu.SemaphoreType.DMA((4,)),
        ],
        compiler_params=pltpu.CompilerParams(collective_id=0, has_side_effects=True, vmem_limit_bytes=40000000),
    )(*(pltpu.with_memory_space_constraint(a, pltpu.HBM) for a in (velocity_prev, forcing, reaction, matrix)))
    return velocity, jnp.swapaxes(compressed, 2, 3)


def solution(mesh):
    counts = {axis: mesh.shape[axis] for axis in ("agg", "gx", "gy")}
    placed = (P(None, "gx", "gy", "agg"), P(None, "gx", "gy", "agg"), P("gx", "gy", "agg"))
    return jax.shard_map(
        functools.partial(on_device, counts),
        mesh=mesh,
        in_specs=placed,
        out_specs=(P(None, "gx", "gy", "agg"), P(None, "gy", ("agg", "gx"), None)),
        check_vma=False,
    )
```

```python
import functools
import itertools
import math

import jax
import jax.numpy as jnp
import numpy as np
from jax import lax
from jax.experimental import pallas as pl
from jax.experimental.pallas import tpu as pltpu
from jax.sharding import PartitionSpec as P

SWEEPS = 2
COARSE_SWEEPS = 4
LX = 5
MESH = pl.DeviceIdType.MESH

damping = 0.8
keep = 1.0 - damping
root_half = 0.7071067811865476


def local_levels(cells_x):
    return min(LX, cells_x.bit_length() - 1)


def finish_matrix(cells_x, blocks, rows):
    levels = local_levels(cells_x)
    kept = cells_x // 2
    eye = np.eye(blocks * kept).reshape(blocks, kept, blocks * kept)
    width = cells_x >> levels
    approx = eye[:, :width].reshape(blocks * width, -1)
    details, at = [], width
    for level in range(levels, 1, -1):
        width = cells_x >> level
        details.append(eye[:, at : at + width].reshape(blocks * width, -1))
        at += width
    for level in range(levels, LX):
        low, high = approx[0::2], approx[1::2]
        approx, detail = (low + high) * root_half, (low - high) * root_half
        details.insert(0, detail)
    along_x = np.concatenate([approx] + details, axis=0)
    along_y = np.zeros((rows, rows))
    for row in range(0, rows, 2):
        along_y[row, row : row + 2] = root_half
        along_y[row + 1, row : row + 2] = root_half, -root_half
    return np.einsum("qk,yr->yqkr", along_x, along_y).reshape(-1, blocks * kept * rows).astype(np.float32)


def around():
    axes = ("gx", "gy", "agg")
    found = []
    for number in range(1, 27):
        turn = [(number // 3**i) % 3 for i in range(3)]
        found.append(tuple((axis, way == 1) for axis, way in zip(axes, turn) if way))
    return sorted(found, key=lambda sides: (-len(sides), sides))


far = 1e30


def kernel(
    sizes, v_hbm, f_hbm, r_hbm, m_hbm, vel_ref, comp_ref, v_ext, f_ext, r_ext, m_ref, w_ext, u1_ext, u2_ext,
    y_send, y_recv, xy_send, xy_recv, z_send, z_recv, yz_send, yz_recv, xz_send, xz_recv, corner_recv,
    q_ext, h_ext, zs_coarse, c_send, c_recv, measure,
    a_send_sem, a_recv_sem, q_send_sem, q_recv_sem, c_send_sem, c_recv_sem, in_sem,
):
    counts = sizes
    C, X, Y, Z = vel_ref.shape
    me = {axis: lax.axis_index(axis) for axis in counts}
    blocks = counts["gx"]
    chunk = Z // blocks
    rows_ext = Y + 8
    f32 = jnp.float32

    loads = [
        pltpu.make_async_copy(src, dst, in_sem.at[i])
        for i, (src, dst) in enumerate((
            (v_hbm, v_ext.at[:, 3 : 3 + X, :Y]),
            (f_hbm, f_ext.at[:, 2 : 2 + X, :Y]),
            (r_hbm, r_ext.at[2 : 2 + X, :Y]),
            (m_hbm, m_ref),
        ))
    ]
    for load in loads:
        load.start()

    def exists(axis, high):
        return me[axis] < counts[axis] - 1 if high else me[axis] > 0

    def all_exist(sides, flip):
        there = None
        for axis, high in sides:
            one = exists(axis, high != flip)
            there = one if there is None else there & one
        return there

    def beside(*sides):
        return {axis: me[axis] + (1 if high else -1) for axis, high in sides}

    barrier = pltpu.get_barrier_semaphore()
    expected = blocks - 1
    for sides in around():
        if len(sides) > 1 or sides[0][0] != "gx":
            there = all_exist(sides, False)
            expected = expected + there.astype(jnp.int32)

            @pl.when(there)
            def _():
                pl.semaphore_signal(barrier, inc=1, device_id=beside(*sides), device_id_type=MESH)

    for step in range(1, blocks):
        pl.semaphore_signal(
            barrier, inc=1, device_id={"gx": lax.rem(me["gx"] + step, blocks)}, device_id_type=MESH
        )

    lane = lax.broadcasted_iota(jnp.int32, (8, Z), 1)
    row = lax.broadcasted_iota(jnp.int32, (8, Z), 0)
    place = lane % 8
    group = lane // 8
    low_half = (lane < 32) | (lane >= 96)
    near_groups = (group % 8 == 2) | (group % 8 == 3) | (group % 8 == 4) | (group % 8 == 5)

    def fine_messages(sides):
        at = {axis: high for axis, high in sides}
        x, y, z = at.get("gx"), at.get("gy"), at.get("agg")
        from_x, from_y, from_z = 0 if x else 1, 0 if y else 1, 0 if z else 1
        if z is None and y is None:
            made = []
            for ref, depth, fill in ((v_ext, 3, 0.0), (f_ext, 2, 0.0), (r_ext, 2, far)):
                here = pl.ds(X if x else depth, depth)
                there = pl.ds(0 if x else depth + X, depth)
                index = (slice(None),) if ref is not r_ext else ()
                made.append((ref.at[index + (here, pl.ds(0, Y))], ref.at[index + (there, pl.ds(0, Y))], fill))
            return made
        if z is None and x is None:
            return [(y_send.at[int(y)], y_recv.at[from_y], None)]
        if z is None:
            return [(xy_send.at[2 * int(x) + int(y)], xy_recv.at[2 * from_x + from_y], None)]
        if x is None and y is None:
            return [(z_send, z_recv.at[from_z, :, pl.ds(0, Y)], None)]
        if x is None:
            return [(yz_send.at[int(y)], yz_recv.at[from_z, from_y], None)]
        if y is None:
            return [(xz_send, xz_recv.at[from_z, from_x], None)]
        return [(xz_send.at[0, pl.ds(Y - 8 if y else 0, 8)], corner_recv.at[from_z, from_x, from_y], 0.0)]

    def remote(src, dst, send_sem, recv_sem, sides):
        return pltpu.make_async_remote_copy(
            src_ref=src, dst_ref=dst, send_sem=send_sem, recv_sem=recv_sem,
            device_id=beside(*sides), device_id_type=MESH,
        )

    def fine_copies():
        return [
            (sides, remote(src, dst, a_send_sem.at[0], a_recv_sem.at[0], sides))
            for sides in around()
            for src, dst, _ in fine_messages(sides)
        ]

    def rows_of(copies):
        found = {}
        for sides, copy in copies:
            axes = tuple(axis for axis, _ in sides)
            if all(high for _, high in sides):
                found[axes] = found.get(axes, 0) + math.prod(copy.src_ref.shape[:-1])
        return found

    def settle(copies, sem):
        sizes = rows_of(copies)
        neighbours = {
            axis: exists(axis, False).astype(jnp.int32) + exists(axis, True).astype(jnp.int32) for axis in counts
        }
        options = {axis: {1: (0,), 2: (1,)}.get(count, (1, 2)) for axis, count in counts.items()}
        for numbers in itertools.product(*options.values()):
            number = dict(zip(options, numbers))
            rows = sum(size * math.prod(number[axis] for axis in axes) for axes, size in sizes.items())
            there = None
            for axis, value in number.items():
                one = neighbours[axis] == value
                there = one if there is None else there & one
            if rows:
                part = measure.at[pl.ds(0, rows)]
                pl.when(there)(pltpu.make_async_copy(part, part, sem).wait)

    def coarse_message(sides, first=0, fields=C):
        at = {axis: 1 if high else -1 for axis, high in sides}
        block = 1 - at.get("gx", 0)
        here, there = {
            0: (slice(0, Y), slice(0, Y)),
            1: (slice(Y - 8, Y), slice(Y + 8, Y + 16)),
            -1: (slice(0, 8), slice(Y, Y + 8)),
        }[at.get("gy", 0)]
        if "agg" in at:
            return zs_coarse.at[here], h_ext.at[0 if at["agg"] > 0 else 1, block, there]
        which = pl.ds(first, fields)
        return q_ext.at[1, which, here], q_ext.at[block, which, there]

    def coarse_copies():
        return [
            (sides, remote(*coarse_message(sides), q_send_sem.at[0], q_recv_sem.at[0], sides))
            for sides in around()
        ]

    def step_copies():
        return [
            (sides, remote(*coarse_message(sides, C, 1), q_send_sem.at[1], q_recv_sem.at[1], sides))
            for sides in around()
            if "agg" not in dict(sides)
        ]

    far_high = jnp.where(low_half, far, 0.0).astype(f32)
    for sides in around():
        @pl.when(jnp.logical_not(all_exist(sides, True)))
        def _():
            axes = tuple(axis for axis, _ in sides)
            for _, target, fill in fine_messages(sides):
                if fill is not None:
                    target[...] = jnp.full(target.shape, fill, f32)
                elif axes == ("gy",):
                    target[: 5 * C] = jnp.zeros((5 * C, 8, Z), f32)
                    target[5 * C :] = jnp.full((2, 8, Z), far, f32)
                elif axes == ("gx", "gy"):
                    target[0:8] = jnp.zeros((8, Z), f32)
                    target[8:16] = jnp.where(row == 4 * C - 8, far, 0.0)
                elif axes == ("agg",):
                    target[:3] = jnp.zeros((3, Y, Z), f32)
                    for t in range(Y // 8):
                        target[3, t * 8 : t * 8 + 8] = far_high
                elif axes == ("gy", "agg"):
                    target[...] = jnp.where(row >= 6, far_high, 0.0)
                else:
                    target[0] = jnp.zeros((Y, Z), f32)
                    for t in range(Y // 8):
                        target[1, t * 8 : t * 8 + 8] = jnp.where(
                            (group == 0) | (group == 1) | (group == 6) | (group == 7), far, 0.0
                        )
            for target in [coarse_message(sides)[1], coarse_message(sides, C, 1)[1]][: 1 + ("agg" not in axes)]:
                target[...] = jnp.zeros(target.shape, f32)

    tiles_y = Y // 8
    near, ring = range(tiles_y), range(tiles_y + 1)
    tile_of = lambda t: slice(t * 8, t * 8 + 8)
    even_l = lane % 2 == 0
    even_r = row % 2 == 0
    lane_roll = lambda t, shift: pltpu.roll(t, shift % Z, 1) if shift % Z else t
    row_roll = lambda t, shift: pltpu.roll(t, shift % 8, 0)
    v_flat = v_ext.reshape(C * (X + 6) * rows_ext, Z)
    f_flat = f_ext.reshape(C * (X + 4) * rows_ext, Z)
    r_flat = r_ext.reshape((X + 4) * rows_ext, Z)

    def x_line(number, y):
        if number < 3 * C:
            c, ref, extra = number // 3, v_flat, 3
        elif number < 5 * C:
            c, ref, extra = (number - 3 * C) // 2, f_flat, 2
        else:
            c, ref, extra = 0, r_flat, 2
        return ref, pl.ds((c * (X + 2 * extra) + extra) * rows_ext + y, X, stride=rows_ext)

    depth_of = lambda number: number % 3 if number < 3 * C else (number - 3 * C) % 2

    loads[0].wait()
    loads[1].wait()
    loads[2].wait()
    for number in range(5 * C + 2):
        for side in range(2):
            depth = depth_of(number)
            ref, at = x_line(number, Y - 1 - depth if side else depth)
            y_send[side, number] = ref[at, :]
    for high_x in range(2):
        for high_y in range(2):
            xs = [X - 1 - d if high_x else d for d in range(2)]
            ys = [Y - 1 - d if high_y else d for d in range(2)]
            target = xy_send.at[2 * high_x + high_y]
            for c in range(C):
                for i, (x, y) in enumerate(((xs[0], ys[0]), (xs[1], ys[0]), (xs[0], ys[1]))):
                    target[3 * c + i : 3 * c + i + 1] = v_ext[c, 3 + x, y : y + 1]
                target[3 * C + c : 3 * C + c + 1] = f_ext[c, 2 + xs[0], ys[0] : ys[0] + 1]
            target[4 * C : 4 * C + 1] = r_ext[2 + xs[0], ys[0] : ys[0] + 1]
    v_at = lambda c, x, t: v_ext[c, 3 + x, tile_of(t)]
    f_at = lambda c, x, t: f_ext[c, 2 + x, tile_of(t)]
    held = (
        (lambda x, t: v_at(0, x, t), lambda x, t: v_at(1, x, t)),
        (lambda x, t: v_at(2, x, t), None),
        (lambda x, t: f_at(0, x, t), lambda x, t: f_at(1, x, t)),
        (lambda x, t: f_at(2, x, t), lambda x, t: r_ext[2 + x, tile_of(t)]),
    )
    for t in near:
        turned = []
        for pair in held:
            packed = jnp.zeros((8, Z), f32)
            for half, get in enumerate(pair):
                if get is not None:
                    for x in range(X):
                        at = (x + 4 + 8 * half) % 16
                        packed = jnp.where(group == at, lane_roll(get(x, t), 8 * at + 3), packed)
            out = jnp.where(place == 3, packed, lane_roll(packed, 6))
            for spot, shift in ((2, -2), (1, -4), (4, 2), (5, 4)):
                out = jnp.where(place == spot, lane_roll(packed, shift), out)
            turned.append(out)
        for i in range(4):
            z_send[i, tile_of(t)] = turned[i]
            for side in range(2):
                if t == (tiles_y - 1 if side else 0):
                    first = 6 if side else 0
                    yz_send[side, 2 * i : 2 * i + 2] = turned[i][first : first + 2]
        for i in range(2):
            xz_send[i, tile_of(t)] = jnp.where(near_groups, turned[2 * i], lane_roll(turned[2 * i + 1], 32))
    pl.semaphore_wait(barrier, expected)
    for sides, copy in fine_copies():
        pl.when(all_exist(sides, False))(copy.start)

    kept = X // 2
    parts = Y // 8
    combos_per_tile = Z // chunk

    def c_copy(j, source):
        return pltpu.make_async_remote_copy(
            src_ref=c_send.at[j],
            dst_ref=c_recv.at[source],
            send_sem=c_send_sem.at[0],
            recv_sem=c_recv_sem.at[0],
            device_id={"gx": j},
            device_id_type=MESH,
        )

    def settle_parts(sem):
        rows = (blocks - 1) * math.prod(c_send.shape[1:-1])
        if rows:
            part = measure.at[pl.ds(0, rows)]
            pltpu.make_async_copy(part, part, sem).wait()

    def finish_compressed(tiles):
        coefs = blocks * kept
        for tile in tiles:
            gathered = c_recv[:, tile].reshape(coefs * 8, Z)
            done = lax.dot_general(
                m_ref[...], gathered, (((1,), (0,)), ((), ())),
                precision=lax.Precision.HIGHEST, preferred_element_type=jnp.float32,
            )
            for place in range(combos_per_tile):
                c, part = divmod(tile * combos_per_tile + place, parts)
                if c < C:
                    for y in range(8):
                        comp_ref[c, part * 8 + y] = done[
                            y * coefs : (y + 1) * coefs, place * chunk : (place + 1) * chunk
                        ]

    lane_swap = lambda t: jnp.where(even_l, lane_roll(t, -1), lane_roll(t, 1))
    row_swap = lambda t: jnp.where(even_r, row_roll(t, -1), row_roll(t, 1))
    slot_at = lane % 16
    corner_of = ((0, 0), (0, 1), (1, 1), (1, 0))

    def pooled(planes):
        pairs = [[planes[x][t] + planes[x + 1][t] for t in near] for x in range(0, X, 2)]
        out = []
        for t in near:
            t0, t1, t2, t3 = (pair[t] for pair in pairs)
            left = jnp.where(even_r, t0, t3) + row_swap(jnp.where(even_r, t3, t0))
            right = jnp.where(even_r, t1, t2) + row_swap(jnp.where(even_r, t2, t1))
            out.append(jnp.where(even_l, left, right) + lane_swap(jnp.where(even_l, right, left)))
        return out

    def edge_lanes(fields, t):
        packed = jnp.zeros((8, Z), f32)
        for start, field in fields:
            for depth in range(1, 5):
                high = (lane >= start + 8 - 2 * depth) & (lane < start + 10 - 2 * depth)
                packed = jnp.where(high, lane_roll(field[t], start + 10 - 4 * depth), packed)
                low = (lane >= start + 6 + 2 * depth) & (lane < start + 8 + 2 * depth)
                packed = jnp.where(low, lane_roll(field[t], start + 6 + 4 * depth), packed)
        return packed

    coarse_weight = [
        damping / ((6.0 + 0.5 * total) * 0.25)
        for total in pooled([[r_ext[2 + x, tile_of(t)] for t in near] for x in range(X)])
    ]
    coarse_step = [0.25 * weight for weight in coarse_weight]
    step_edges = [edge_lanes([(64 + 16 * c, coarse_step) for c in range(C)], t) for t in near]
    for t in near:
        q_ext[1, C, tile_of(t)] = coarse_step[t]
        zs_coarse[tile_of(t)] = step_edges[t]
    for x in range(X):
        for t in near:
            w_ext[2 + x, tile_of(t)] = damping / (6.0 + r_ext[2 + x, tile_of(t)])

    levels = local_levels(X)
    for c in range(C):
        for t in near:
            approx, details = [v_at(c, x, t) for x in range(X)], []
            for level in range(levels):
                low, high = approx[0::2], approx[1::2]
                approx = [(a + b) * root_half for a, b in zip(low, high)]
                if level > 0:
                    details = [(a - b) * root_half for a, b in zip(low, high)] + details
            tile, spot = divmod(c * parts + t, combos_per_tile)
            inside = (lane >= spot * chunk) & (lane < (spot + 1) * chunk)
            for k, values in enumerate(approx + details):
                done = (jnp.where(even_l, values, -values) + lane_swap(values)) * root_half
                for j in range(blocks):
                    moved = lane_roll(done, spot * chunk - j * chunk)
                    if spot:
                        moved = jnp.where(inside, moved, c_send[j, tile, k])
                    c_send[j, tile, k] = moved

    settle(fine_copies(), a_recv_sem.at[0])

    for sides, copy in step_copies():
        pl.when(all_exist(sides, False))(copy.start)
    for j in range(blocks):
        pl.when(me["gx"] != j)(c_copy(j, me["gx"]).start)

    for number in range(5 * C + 2):
        for side in range(2):
            depth = depth_of(number)
            ref, at = x_line(number, Y + depth if side else rows_ext - 1 - depth)
            ref[at, :] = y_recv[side, number]
    for high_x in range(2):
        for high_y in range(2):
            xs = [X + d if high_x else -1 - d for d in range(2)]
            ys = [Y + d if high_y else rows_ext - 1 - d for d in range(2)]
            source = xy_recv.at[2 * high_x + high_y]
            for c in range(C):
                for i, (x, y) in enumerate(((xs[0], ys[0]), (xs[1], ys[0]), (xs[0], ys[1]))):
                    v_ext[c, 3 + x, y : y + 1] = source[3 * c + i : 3 * c + i + 1]
                f_ext[c, 2 + xs[0], ys[0] : ys[0] + 1] = source[3 * C + c : 3 * C + c + 1]
            r_ext[2 + xs[0], ys[0] : ys[0] + 1] = source[4 * C : 4 * C + 1]
    for side in range(2):
        for i in range(4):
            z_recv[side, i, Y : Y + 2] = yz_recv[side, 1, 2 * i : 2 * i + 2]
            z_recv[side, i, Y + 6 : Y + 8] = yz_recv[side, 0, 2 * i : 2 * i + 2]

    def weight_of(reaction):
        return jnp.where(reaction < 0.1 * far, damping / (6.0 + reaction), 0.0)

    for x in range(-2, X + 2):
        outside = max(-x, x - X + 1)
        for t in ring:
            if (outside > 0 and t < tiles_y) or (t == tiles_y and outside < 2):
                w_ext[2 + x, tile_of(t)] = weight_of(r_ext[2 + x, tile_of(t)])

    mixed = {}
    for i in range(4):
        for t in ring:
            mixed[i, t] = jnp.where(place < 4, z_recv[1, i, tile_of(t)], z_recv[0, i, tile_of(t)])
    beyond = {}
    for side in range(2):
        for i in range(2):
            for t in near:
                beyond[side, i, t] = jnp.where(
                    place < 4, xz_recv[1, side, i, tile_of(t)], xz_recv[0, side, i, tile_of(t)]
                )
        ends = [
            jnp.where(place < 4, corner_recv[1, side, high], corner_recv[0, side, high]) for high in range(2)
        ]
        beyond[side, 0, tiles_y] = jnp.where(row < 4, ends[1], ends[0])

    def edge_field(number, t):
        i, half = divmod(number, 2)
        value = lane_roll(mixed[i, t], 64 * half)
        if t < tiles_y or number < 4:
            shift = (64, 0, 32, -32)[number % 4]
            low, high = (lane_roll(beyond[side, i // 2, t], shift) for side in range(2))
            value = jnp.where(group < 4, low, jnp.where(group >= 12, high, value))
        return value

    edge_v = {(c, t): edge_field(c, t) for c in range(C) for t in ring}
    edge_f = {(c, t): edge_field(4 + c, t) for c in range(C) for t in ring}
    edge_w = {t: weight_of(edge_field(7, t)) for t in ring}

    def around_rows(get, t, tiles, by):
        after, before = (t + 1) % tiles, (t - 1) % tiles
        own = get(t)
        above = jnp.where(row < 8 - by, row_roll(own, -by), row_roll(get(after), -by))
        below = jnp.where(row >= by, row_roll(own, by), row_roll(get(before), by))
        return below, above

    def main_total(get, edge, c, x, t):
        below, above = around_rows(lambda t: get(c, x, t), t, tiles_y + 1, 1)
        total = (get(c, x - 1, t) + get(c, x + 1, t)) + (below + above)
        beside_z = lane_roll(edge[c, t], -(8 * (x + 4) + 4))
        own = get(c, x, t)
        total = total + jnp.where(lane == 0, beside_z, lane_roll(own, 1))
        return total + jnp.where(lane == Z - 1, beside_z, lane_roll(own, -1))

    def edge_total(get, edge, c, xs, t):
        own = edge[c, t]
        line = own
        for x in xs:
            line = jnp.where(group == x + 4, lane_roll(get(c, x, t), 8 * (x + 4) + 4), line)
        below, above = around_rows(lambda t: edge[c, t], t, tiles_y + 1, 1)
        total = (lane_roll(own, 8) + lane_roll(own, -8)) + (below + above)
        total = total + jnp.where(place == 4, line, lane_roll(own, 1))
        return total + jnp.where(place == 3, line, lane_roll(own, -1))

    u1_at = lambda c, x, t: u1_ext[c, 2 + x, tile_of(t)]
    u2_at = lambda c, x, t: u2_ext[c, 1 + x, tile_of(t)]
    w_at = lambda x, t: w_ext[2 + x, tile_of(t)]

    edge_1, edge_2 = {}, {}
    for c in range(C):
        for t in ring:
            total = edge_total(v_at, edge_v, c, range(-1, X + 1), t)
            edge_1[c, t] = keep * edge_v[c, t] + edge_w[t] * (edge_f[c, t] + total)
        for x in range(-2, X + 2):
            for t in near if x in (-2, X + 1) else ring:
                total = main_total(v_at, edge_v, c, x, t)
                u1_ext[c, 2 + x, tile_of(t)] = keep * v_at(c, x, t) + w_at(x, t) * (f_at(c, x, t) + total)
    for c in range(C):
        for t in near:
            total = edge_total(u1_at, edge_1, c, range(X), t)
            edge_2[c, t] = keep * edge_1[c, t] + edge_w[t] * (edge_f[c, t] + total)
        for x in range(-1, X + 1):
            for t in near if x in (-1, X) else ring:
                total = main_total(u1_at, edge_1, c, x, t)
                u2_ext[c, 1 + x, tile_of(t)] = keep * u1_at(c, x, t) + w_at(x, t) * (f_at(c, x, t) + total)
    sums = [
        [[main_total(u2_at, edge_2, c, x, t) + f_at(c, x, t) for t in near] for x in range(X)] for c in range(C)
    ]

    correction = []
    for c in range(C):
        rhs = pooled([
            [sums[c][x][t] - (6.0 + r_ext[2 + x, tile_of(t)]) * u2_at(c, x, t) for t in near] for x in range(X)
        ])
        correction.append([weight * (0.125 * total) for weight, total in zip(coarse_weight, rhs)])
    for c in range(C):
        for t in near:
            q_ext[1, c, tile_of(t)] = correction[c][t]
    for t in near:
        edges_t = edge_lanes([(16 * c, correction[c]) for c in range(C)], t)
        zs_coarse[tile_of(t)] = jnp.where(lane < 64, edges_t, zs_coarse[tile_of(t)])
    for sides, copy in coarse_copies():
        pl.when(all_exist(sides, False))(copy.start)

    for j in range(blocks):
        @pl.when(me["gx"] == j)
        def _():
            c_recv[j] = c_send[j]

    settle_parts(c_recv_sem.at[0])
    loads[3].wait()
    finish_compressed(range(c_send.shape[1]))

    settle(step_copies(), q_recv_sem.at[1])
    settle(coarse_copies(), q_recv_sem.at[0])

    ring = range(tiles_y + 2)
    after = lambda t: (t + 1) % len(ring)
    before = lambda t: (t - 1) % len(ring)
    main = {(b, c, t): q_ext[b, c, tile_of(t)] for b in range(3) for c in range(C) for t in ring}
    step_main = {(b, t): q_ext[b, C, tile_of(t)] for b in range(3) for t in ring}
    edge = {
        (b, t): jnp.where(slot_at < 8, h_ext[1, b, tile_of(t)], h_ext[0, b, tile_of(t)])
        for b in range(3) for t in ring
    }
    step_edge = {key: lane_roll(value, -64) for key, value in edge.items()}
    first_main, first_edge = dict(main), dict(edge)

    def above(get, t):
        return jnp.where(row < 6, row_roll(get(t), -2), row_roll(get(after(t)), -2))

    def below(get, t):
        return jnp.where(row >= 2, row_roll(get(t), 2), row_roll(get(before(t)), 2))

    def along(get, b, t):
        low, high = get(max(b - 1, 0), t), get(min(b + 1, 2), t)
        across = jnp.where(even_l, jnp.where(even_r, high, low), get(b, t))
        return lane_swap(get(b, t)) + row_swap(across)

    def inject(edge, b, c, t):
        return lane_roll(edge[b, t], -(16 * c + 8))

    def left_of(main, edge, b, c, t):
        return jnp.where(lane < 2, inject(edge, b, c, t), lane_roll(main[b, c, t], 2))

    def right_of(main, edge, b, c, t):
        return jnp.where(lane >= Z - 2, inject(edge, b, c, t), lane_roll(main[b, c, t], -2))

    def coarse_sweep(main, edge, main_at, edge_at):
        new_main, new_edge = dict(main), dict(edge)
        for b, t in main_at:
            for c in range(C):
                get = lambda b, t, c=c: main[b, c, t]
                row_get = lambda t, b=b, c=c: main[b, c, t]
                total = along(get, b, t) + (above(row_get, t) + below(row_get, t))
                total = total + (left_of(main, edge, b, c, t) + right_of(main, edge, b, c, t))
                new_main[b, c, t] = keep * main[b, c, t] + first_main[b, c, t] + step_main[b, t] * total
        for b, t in edge_at:
            get = lambda b, t: edge[b, t]
            row_get = lambda t, b=b: edge[b, t]
            own = lane_roll(main[b, 0, t], 8)
            for c in range(1, C):
                own = jnp.where(lane < 16 * c, own, lane_roll(main[b, c, t], 16 * c + 8))
            total = along(get, b, t) + (above(row_get, t) + below(row_get, t))
            total = total + jnp.where((slot_at == 8) | (slot_at == 9), own, lane_roll(edge[b, t], 2))
            total = total + jnp.where((slot_at == 6) | (slot_at == 7), own, lane_roll(edge[b, t], -2))
            new_edge[b, t] = keep * edge[b, t] + first_edge[b, t] + step_edge[b, t] * total
        return new_main, new_edge

    everywhere = [(b, t) for b in range(3) for t in ring]
    centre = [(1, t) for t in ring]
    sides_near = [(b, t) for b in (0, 2) for t in near]
    main, edge = coarse_sweep(main, edge, everywhere, everywhere)
    main, edge = coarse_sweep(main, edge, everywhere, centre + sides_near)
    main, edge = coarse_sweep(main, edge, centre + sides_near, [(1, t) for t in near])

    def spread_rows(even, odd, pa):
        if pa == 0:
            return jnp.where(even_r, even, row_roll(odd, 1))
        return jnp.where(even_r, row_roll(even, -1), odd)

    def spread_lanes(even, odd, pb):
        if pb == 0:
            return jnp.where(even_l, even, lane_roll(odd, 1))
        return jnp.where(even_l, lane_roll(even, -1), odd)

    for c in range(C):
        for t in near:
            at = tile_of(t)
            row_get = lambda t, c=c: main[1, c, t]
            own = main[1, c, t]
            rows_near = (below(row_get, t), above(row_get, t))
            lanes_near = (left_of(main, edge, 1, c, t), right_of(main, edge, 1, c, t))
            alone = [spread_lanes(own, own, pb) for pb in range(2)]
            spread = [spread_rows(alone[pb], alone[pb], pa) for pa, pb in corner_of]
            low, high = (spread_lanes(main[b, c, t], main[b, c, t], 0) for b in (0, 2))
            spread = [spread_rows(low, low, 1)] + spread + [spread_rows(high, high, 0)]
            based = [3.0 * own + rows_near[a] for a in range(2)]
            wide = [
                [spread_lanes(based[a] + lanes_near[0], based[a] + lanes_near[1], pb) for pb in range(2)]
                for a in range(2)
            ]
            for x in range(X):
                p = x // 2
                pa, pb = corner_of[p]
                added = spread_rows(wide[0][pb], wide[1][pb], pa) + spread[p + 2 * (x % 2)]
                total = sums[c][x][t] + added
                vel_ref[c, x, at] = keep * (u2_at(c, x, t) + spread[p + 1]) + w_at(x, t) * total

    settle(fine_copies(), a_send_sem.at[0])
    settle(step_copies(), q_send_sem.at[1])
    settle(coarse_copies(), q_send_sem.at[0])
    settle_parts(c_send_sem.at[0])


def on_device(counts, velocity_prev, forcing, reaction):
    C, X, Y, Z = velocity_prev.shape
    blocks = counts["gx"]
    kept = X // 2
    chunk = Z // blocks
    tiles = -(-(C * (Y // 8)) // (Z // chunk))
    matrix = jnp.asarray(finish_matrix(X, blocks, 8))
    vmem = pl.BlockSpec(memory_space=pltpu.VMEM)
    space = lambda *shape: pltpu.VMEM(shape, jnp.float32)

    velocity, compressed = pl.pallas_call(
        functools.partial(kernel, counts),
        out_shape=(
            jax.ShapeDtypeStruct((C, X, Y, Z), jnp.float32),
            jax.ShapeDtypeStruct((C, Y, kept * blocks, chunk), jnp.float32),
        ),
        in_specs=[pl.BlockSpec(memory_space=pltpu.HBM)] * 4,
        out_specs=(vmem, vmem),
        scratch_shapes=[
            space(C, X + 6, Y + 8, Z),
            space(C, X + 4, Y + 8, Z),
            space(X + 4, Y + 8, Z),
            space(*matrix.shape),
            space(X + 4, Y + 8, Z),
            space(C, X + 4, Y + 8, Z),
            space(C, X + 2, Y + 8, Z),
            space(2, 5 * C + 2, X, Z),
            space(2, 5 * C + 2, X, Z),
            space(4, 16, Z),
            space(4, 16, Z),
            space(4, Y, Z),
            space(2, 4, Y + 8, Z),
            space(2, 8, Z),
            space(2, 2, 8, Z),
            space(2, Y, Z),
            space(2, 2, 2, Y, Z),
            space(2, 2, 2, 8, Z),
            space(3, C + 1, Y + 16, Z),
            space(2, 3, Y + 16, Z),
            space(Y, Z),
            space(blocks, tiles, kept, 8, Z),
            space(blocks, tiles, kept, 8, Z),
            space(max((blocks - 1) * tiles * kept * 8, 128 * Y), Z),
            pltpu.SemaphoreType.DMA((1,)),
            pltpu.SemaphoreType.DMA((1,)),
            pltpu.SemaphoreType.DMA((2,)),
            pltpu.SemaphoreType.DMA((2,)),
            pltpu.SemaphoreType.DMA((1,)),
            pltpu.SemaphoreType.DMA((1,)),
            pltpu.SemaphoreType.DMA((4,)),
        ],
        compiler_params=pltpu.CompilerParams(collective_id=0, has_side_effects=True, vmem_limit_bytes=40000000),
    )(*(pltpu.with_memory_space_constraint(a, pltpu.HBM) for a in (velocity_prev, forcing, reaction, matrix)))
    return velocity, jnp.swapaxes(compressed, 2, 3)


def solution(mesh):
    counts = {axis: mesh.shape[axis] for axis in ("agg", "gx", "gy")}
    placed = (P(None, "gx", "gy", "agg"), P(None, "gx", "gy", "agg"), P("gx", "gy", "agg"))
    return jax.shard_map(
        functools.partial(on_device, counts),
        mesh=mesh,
        in_specs=placed,
        out_specs=(P(None, "gx", "gy", "agg"), P(None, "gy", ("agg", "gx"), None)),
        check_vma=False,
    )
```

```python
import functools
import itertools
import math

import jax
import jax.numpy as jnp
import numpy as np
from jax import lax
from jax.experimental import pallas as pl
from jax.experimental.pallas import tpu as pltpu
from jax.sharding import PartitionSpec as P

SWEEPS = 2
COARSE_SWEEPS = 4
LX = 5
MESH = pl.DeviceIdType.MESH

damping = 0.8
keep = 1.0 - damping
root_half = 0.7071067811865476


def local_levels(cells_x):
    return min(LX, cells_x.bit_length() - 1)


def finish_matrix(cells_x, blocks, rows):
    levels = local_levels(cells_x)
    kept = cells_x // 2
    eye = np.eye(blocks * kept).reshape(blocks, kept, blocks * kept)
    width = cells_x >> levels
    approx = eye[:, :width].reshape(blocks * width, -1)
    details, at = [], width
    for level in range(levels, 1, -1):
        width = cells_x >> level
        details.append(eye[:, at : at + width].reshape(blocks * width, -1))
        at += width
    for level in range(levels, LX):
        low, high = approx[0::2], approx[1::2]
        approx, detail = (low + high) * root_half, (low - high) * root_half
        details.insert(0, detail)
    along_x = np.concatenate([approx] + details, axis=0)
    along_y = np.zeros((rows, rows))
    for row in range(0, rows, 2):
        along_y[row, row : row + 2] = root_half
        along_y[row + 1, row : row + 2] = root_half, -root_half
    return np.einsum("qk,yr->yqkr", along_x, along_y).reshape(-1, blocks * kept * rows).astype(np.float32)


def around():
    axes = ("gx", "gy", "agg")
    found = []
    for number in range(1, 27):
        turn = [(number // 3**i) % 3 for i in range(3)]
        found.append(tuple((axis, way == 1) for axis, way in zip(axes, turn) if way))
    return sorted(found, key=lambda sides: (-len(sides), sides))


far = 1e30


def kernel(
    sizes, v_hbm, f_hbm, r_hbm, m_hbm, vel_ref, comp_ref, v_ext, f_ext, r_ext, m_ref, w_ext, u1_ext, u2_ext,
    y_send, y_recv, xy_send, xy_recv, z_send, z_recv, yz_send, yz_recv, xz_send, xz_recv, corner_recv,
    q_ext, h_ext, zs_coarse, c_send, c_recv, measure,
    a_send_sem, a_recv_sem, q_send_sem, q_recv_sem, c_send_sem, c_recv_sem, in_sem,
):
    counts = sizes
    C, X, Y, Z = vel_ref.shape
    me = {axis: lax.axis_index(axis) for axis in counts}
    blocks = counts["gx"]
    chunk = Z // blocks
    rows_ext = Y + 8
    f32 = jnp.float32

    loads = [
        pltpu.make_async_copy(src, dst, in_sem.at[i])
        for i, (src, dst) in enumerate((
            (v_hbm, v_ext.at[:, 3 : 3 + X, :Y]),
            (f_hbm, f_ext.at[:, 2 : 2 + X, :Y]),
            (r_hbm, r_ext.at[2 : 2 + X, :Y]),
            (m_hbm, m_ref),
        ))
    ]
    for load in loads:
        load.start()

    def exists(axis, high):
        return me[axis] < counts[axis] - 1 if high else me[axis] > 0

    def all_exist(sides, flip):
        there = None
        for axis, high in sides:
            one = exists(axis, high != flip)
            there = one if there is None else there & one
        return there

    def beside(*sides):
        return {axis: me[axis] + (1 if high else -1) for axis, high in sides}

    barrier = pltpu.get_barrier_semaphore()
    expected = blocks - 1
    for sides in around():
        if len(sides) > 1 or sides[0][0] != "gx":
            there = all_exist(sides, False)
            expected = expected + there.astype(jnp.int32)

            @pl.when(there)
            def _():
                pl.semaphore_signal(barrier, inc=1, device_id=beside(*sides), device_id_type=MESH)

    for step in range(1, blocks):
        pl.semaphore_signal(
            barrier, inc=1, device_id={"gx": lax.rem(me["gx"] + step, blocks)}, device_id_type=MESH
        )

    lane = lax.broadcasted_iota(jnp.int32, (8, Z), 1)
    row = lax.broadcasted_iota(jnp.int32, (8, Z), 0)
    place = lane % 8
    group = lane // 8
    low_half = (lane < 32) | (lane >= 96)
    near_groups = (group % 8 == 2) | (group % 8 == 3) | (group % 8 == 4) | (group % 8 == 5)

    def fine_messages(sides):
        at = {axis: high for axis, high in sides}
        x, y, z = at.get("gx"), at.get("gy"), at.get("agg")
        from_x, from_y, from_z = 0 if x else 1, 0 if y else 1, 0 if z else 1
        if z is None and y is None:
            made = []
            for ref, depth, fill in ((v_ext, 3, 0.0), (f_ext, 2, 0.0), (r_ext, 2, far)):
                here = pl.ds(X if x else depth, depth)
                there = pl.ds(0 if x else depth + X, depth)
                index = (slice(None),) if ref is not r_ext else ()
                made.append((ref.at[index + (here, pl.ds(0, Y))], ref.at[index + (there, pl.ds(0, Y))], fill))
            return made
        if z is None and x is None:
            return [(y_send.at[int(y)], y_recv.at[from_y], None)]
        if z is None:
            return [(xy_send.at[2 * int(x) + int(y)], xy_recv.at[2 * from_x + from_y], None)]
        if x is None and y is None:
            return [(z_send, z_recv.at[from_z, :, pl.ds(0, Y)], None)]
        if x is None:
            return [(yz_send.at[int(y)], yz_recv.at[from_z, from_y], None)]
        if y is None:
            return [(xz_send, xz_recv.at[from_z, from_x], None)]
        return [(xz_send.at[0, pl.ds(Y - 8 if y else 0, 8)], corner_recv.at[from_z, from_x, from_y], 0.0)]

    def remote(src, dst, send_sem, recv_sem, sides):
        return pltpu.make_async_remote_copy(
            src_ref=src, dst_ref=dst, send_sem=send_sem, recv_sem=recv_sem,
            device_id=beside(*sides), device_id_type=MESH,
        )

    def fine_copies():
        return [
            (sides, remote(src, dst, a_send_sem.at[0], a_recv_sem.at[0], sides))
            for sides in around()
            for src, dst, _ in fine_messages(sides)
        ]

    def rows_of(copies):
        found = {}
        for sides, copy in copies:
            axes = tuple(axis for axis, _ in sides)
            if all(high for _, high in sides):
                found[axes] = found.get(axes, 0) + math.prod(copy.src_ref.shape[:-1])
        return found

    def settle(copies, sem):
        sizes = rows_of(copies)
        neighbours = {
            axis: exists(axis, False).astype(jnp.int32) + exists(axis, True).astype(jnp.int32) for axis in counts
        }
        options = {axis: {1: (0,), 2: (1,)}.get(count, (1, 2)) for axis, count in counts.items()}
        for numbers in itertools.product(*options.values()):
            number = dict(zip(options, numbers))
            rows = sum(size * math.prod(number[axis] for axis in axes) for axes, size in sizes.items())
            there = None
            for axis, value in number.items():
                one = neighbours[axis] == value
                there = one if there is None else there & one
            if rows:
                part = measure.at[pl.ds(0, rows)]
                pl.when(there)(pltpu.make_async_copy(part, part, sem).wait)

    def coarse_message(sides, first=0, fields=C):
        at = {axis: 1 if high else -1 for axis, high in sides}
        block = 1 - at.get("gx", 0)
        here, there = {
            0: (slice(0, Y), slice(0, Y)),
            1: (slice(Y - 8, Y), slice(Y + 8, Y + 16)),
            -1: (slice(0, 8), slice(Y, Y + 8)),
        }[at.get("gy", 0)]
        if "agg" in at:
            return zs_coarse.at[here], h_ext.at[0 if at["agg"] > 0 else 1, block, there]
        which = pl.ds(first, fields)
        return q_ext.at[1, which, here], q_ext.at[block, which, there]

    def coarse_copies():
        return [
            (sides, remote(*coarse_message(sides), q_send_sem.at[0], q_recv_sem.at[0], sides))
            for sides in around()
        ]

    def step_copies():
        return [
            (sides, remote(*coarse_message(sides, C, 1), q_send_sem.at[1], q_recv_sem.at[1], sides))
            for sides in around()
            if "agg" not in dict(sides)
        ]

    far_high = jnp.where(low_half, far, 0.0).astype(f32)
    for sides in around():
        @pl.when(jnp.logical_not(all_exist(sides, True)))
        def _():
            axes = tuple(axis for axis, _ in sides)
            for _, target, fill in fine_messages(sides):
                if fill is not None:
                    target[...] = jnp.full(target.shape, fill, f32)
                elif axes == ("gy",):
                    target[: 5 * C] = jnp.zeros((5 * C, 8, Z), f32)
                    target[5 * C :] = jnp.full((2, 8, Z), far, f32)
                elif axes == ("gx", "gy"):
                    target[0:8] = jnp.zeros((8, Z), f32)
                    target[8:16] = jnp.where(row == 4 * C - 8, far, 0.0)
                elif axes == ("agg",):
                    target[:3] = jnp.zeros((3, Y, Z), f32)
                    for t in range(Y // 8):
                        target[3, t * 8 : t * 8 + 8] = far_high
                elif axes == ("gy", "agg"):
                    target[...] = jnp.where(row >= 6, far_high, 0.0)
                else:
                    target[0] = jnp.zeros((Y, Z), f32)
                    for t in range(Y // 8):
                        target[1, t * 8 : t * 8 + 8] = jnp.where(
                            (group == 0) | (group == 1) | (group == 6) | (group == 7), far, 0.0
                        )
            for target in [coarse_message(sides)[1], coarse_message(sides, C, 1)[1]][: 1 + ("agg" not in axes)]:
                target[...] = jnp.zeros(target.shape, f32)

    tiles_y = Y // 8
    near, ring = range(tiles_y), range(tiles_y + 1)
    tile_of = lambda t: slice(t * 8, t * 8 + 8)
    even_l = lane % 2 == 0
    even_r = row % 2 == 0
    lane_roll = lambda t, shift: pltpu.roll(t, shift % Z, 1) if shift % Z else t
    row_roll = lambda t, shift: pltpu.roll(t, shift % 8, 0)
    v_flat = v_ext.reshape(C * (X + 6) * rows_ext, Z)
    f_flat = f_ext.reshape(C * (X + 4) * rows_ext, Z)
    r_flat = r_ext.reshape((X + 4) * rows_ext, Z)

    def x_line(number, y):
        if number < 3 * C:
            c, ref, extra = number // 3, v_flat, 3
        elif number < 5 * C:
            c, ref, extra = (number - 3 * C) // 2, f_flat, 2
        else:
            c, ref, extra = 0, r_flat, 2
        return ref, pl.ds((c * (X + 2 * extra) + extra) * rows_ext + y, X, stride=rows_ext)

    depth_of = lambda number: number % 3 if number < 3 * C else (number - 3 * C) % 2

    loads[0].wait()
    loads[1].wait()
    loads[2].wait()
    for number in range(5 * C + 2):
        for side in range(2):
            depth = depth_of(number)
            ref, at = x_line(number, Y - 1 - depth if side else depth)
            y_send[side, number] = ref[at, :]
    for high_x in range(2):
        for high_y in range(2):
            xs = [X - 1 - d if high_x else d for d in range(2)]
            ys = [Y - 1 - d if high_y else d for d in range(2)]
            target = xy_send.at[2 * high_x + high_y]
            for c in range(C):
                for i, (x, y) in enumerate(((xs[0], ys[0]), (xs[1], ys[0]), (xs[0], ys[1]))):
                    target[3 * c + i : 3 * c + i + 1] = v_ext[c, 3 + x, y : y + 1]
                target[3 * C + c : 3 * C + c + 1] = f_ext[c, 2 + xs[0], ys[0] : ys[0] + 1]
            target[4 * C : 4 * C + 1] = r_ext[2 + xs[0], ys[0] : ys[0] + 1]
    v_at = lambda c, x, t: v_ext[c, 3 + x, tile_of(t)]
    f_at = lambda c, x, t: f_ext[c, 2 + x, tile_of(t)]
    held = (
        (lambda x, t: v_at(0, x, t), lambda x, t: v_at(1, x, t)),
        (lambda x, t: v_at(2, x, t), None),
        (lambda x, t: f_at(0, x, t), lambda x, t: f_at(1, x, t)),
        (lambda x, t: f_at(2, x, t), lambda x, t: r_ext[2 + x, tile_of(t)]),
    )
    for t in near:
        turned = []
        for pair in held:
            packed = jnp.zeros((8, Z), f32)
            for half, get in enumerate(pair):
                if get is not None:
                    for x in range(X):
                        at = (x + 4 + 8 * half) % 16
                        packed = jnp.where(group == at, lane_roll(get(x, t), 8 * at + 3), packed)
            out = jnp.where(place == 3, packed, lane_roll(packed, 6))
            for spot, shift in ((2, -2), (1, -4), (4, 2), (5, 4)):
                out = jnp.where(place == spot, lane_roll(packed, shift), out)
            turned.append(out)
        for i in range(4):
            z_send[i, tile_of(t)] = turned[i]
            for side in range(2):
                if t == (tiles_y - 1 if side else 0):
                    first = 6 if side else 0
                    yz_send[side, 2 * i : 2 * i + 2] = turned[i][first : first + 2]
        for i in range(2):
            xz_send[i, tile_of(t)] = jnp.where(near_groups, turned[2 * i], lane_roll(turned[2 * i + 1], 32))
    pl.semaphore_wait(barrier, expected)
    for sides, copy in fine_copies():
        pl.when(all_exist(sides, False))(copy.start)

    kept = X // 2
    parts = Y // 8
    combos_per_tile = Z // chunk

    def c_copy(j, source):
        return pltpu.make_async_remote_copy(
            src_ref=c_send.at[j],
            dst_ref=c_recv.at[source],
            send_sem=c_send_sem.at[0],
            recv_sem=c_recv_sem.at[0],
            device_id={"gx": j},
            device_id_type=MESH,
        )

    def settle_parts(sem):
        rows = (blocks - 1) * math.prod(c_send.shape[1:-1])
        if rows:
            part = measure.at[pl.ds(0, rows)]
            pltpu.make_async_copy(part, part, sem).wait()

    def finish_compressed(tiles):
        coefs = blocks * kept
        for tile in tiles:
            gathered = c_recv[:, tile].reshape(coefs * 8, Z)
            done = lax.dot_general(
                m_ref[...], gathered, (((1,), (0,)), ((), ())),
                precision=lax.Precision.HIGHEST, preferred_element_type=jnp.float32,
            )
            for place in range(combos_per_tile):
                c, part = divmod(tile * combos_per_tile + place, parts)
                if c < C:
                    for y in range(8):
                        comp_ref[c, part * 8 + y] = done[
                            y * coefs : (y + 1) * coefs, place * chunk : (place + 1) * chunk
                        ]

    lane_swap = lambda t: jnp.where(even_l, lane_roll(t, -1), lane_roll(t, 1))
    row_swap = lambda t: jnp.where(even_r, row_roll(t, -1), row_roll(t, 1))
    slot_at = lane % 16
    corner_of = ((0, 0), (0, 1), (1, 1), (1, 0))

    def pooled(planes):
        pairs = [[planes[x][t] + planes[x + 1][t] for t in near] for x in range(0, X, 2)]
        out = []
        for t in near:
            t0, t1, t2, t3 = (pair[t] for pair in pairs)
            left = jnp.where(even_r, t0, t3) + row_swap(jnp.where(even_r, t3, t0))
            right = jnp.where(even_r, t1, t2) + row_swap(jnp.where(even_r, t2, t1))
            out.append(jnp.where(even_l, left, right) + lane_swap(jnp.where(even_l, right, left)))
        return out

    def edge_lanes(fields, t):
        packed = jnp.zeros((8, Z), f32)
        for start, field in fields:
            for depth in range(1, 5):
                high = (lane >= start + 8 - 2 * depth) & (lane < start + 10 - 2 * depth)
                packed = jnp.where(high, lane_roll(field[t], start + 10 - 4 * depth), packed)
                low = (lane >= start + 6 + 2 * depth) & (lane < start + 8 + 2 * depth)
                packed = jnp.where(low, lane_roll(field[t], start + 6 + 4 * depth), packed)
        return packed

    coarse_weight = [
        damping / ((6.0 + 0.5 * total) * 0.25)
        for total in pooled([[r_ext[2 + x, tile_of(t)] for t in near] for x in range(X)])
    ]
    coarse_step = [0.25 * weight for weight in coarse_weight]
    step_edges = [edge_lanes([(64 + 16 * c, coarse_step) for c in range(C)], t) for t in near]
    for t in near:
        q_ext[1, C, tile_of(t)] = coarse_step[t]
        zs_coarse[tile_of(t)] = step_edges[t]
    for x in range(X):
        for t in near:
            w_ext[2 + x, tile_of(t)] = damping / (6.0 + r_ext[2 + x, tile_of(t)])

    levels = local_levels(X)
    for c in range(C):
        for t in near:
            approx, details = [v_at(c, x, t) for x in range(X)], []
            for level in range(levels):
                low, high = approx[0::2], approx[1::2]
                approx = [(a + b) * root_half for a, b in zip(low, high)]
                if level > 0:
                    details = [(a - b) * root_half for a, b in zip(low, high)] + details
            tile, spot = divmod(c * parts + t, combos_per_tile)
            inside = (lane >= spot * chunk) & (lane < (spot + 1) * chunk)
            for k, values in enumerate(approx + details):
                done = (jnp.where(even_l, values, -values) + lane_swap(values)) * root_half
                for j in range(blocks):
                    moved = lane_roll(done, spot * chunk - j * chunk)
                    if spot:
                        moved = jnp.where(inside, moved, c_send[j, tile, k])
                    c_send[j, tile, k] = moved

    settle(fine_copies(), a_recv_sem.at[0])

    for sides, copy in step_copies():
        pl.when(all_exist(sides, False))(copy.start)
    for j in range(blocks):
        pl.when(me["gx"] != j)(c_copy(j, me["gx"]).start)

    for number in range(5 * C + 2):
        for side in range(2):
            depth = depth_of(number)
            ref, at = x_line(number, Y + depth if side else rows_ext - 1 - depth)
            ref[at, :] = y_recv[side, number]
    for high_x in range(2):
        for high_y in range(2):
            xs = [X + d if high_x else -1 - d for d in range(2)]
            ys = [Y + d if high_y else rows_ext - 1 - d for d in range(2)]
            source = xy_recv.at[2 * high_x + high_y]
            for c in range(C):
                for i, (x, y) in enumerate(((xs[0], ys[0]), (xs[1], ys[0]), (xs[0], ys[1]))):
                    v_ext[c, 3 + x, y : y + 1] = source[3 * c + i : 3 * c + i + 1]
                f_ext[c, 2 + xs[0], ys[0] : ys[0] + 1] = source[3 * C + c : 3 * C + c + 1]
            r_ext[2 + xs[0], ys[0] : ys[0] + 1] = source[4 * C : 4 * C + 1]
    for side in range(2):
        for i in range(4):
            z_recv[side, i, Y : Y + 2] = yz_recv[side, 1, 2 * i : 2 * i + 2]
            z_recv[side, i, Y + 6 : Y + 8] = yz_recv[side, 0, 2 * i : 2 * i + 2]

    def weight_of(reaction):
        return jnp.where(reaction < 0.1 * far, damping / (6.0 + reaction), 0.0)

    for x in range(-2, X + 2):
        outside = max(-x, x - X + 1)
        for t in ring:
            if (outside > 0 and t < tiles_y) or (t == tiles_y and outside < 2):
                w_ext[2 + x, tile_of(t)] = weight_of(r_ext[2 + x, tile_of(t)])

    mixed = {}
    for i in range(4):
        for t in ring:
            mixed[i, t] = jnp.where(place < 4, z_recv[1, i, tile_of(t)], z_recv[0, i, tile_of(t)])
    beyond = {}
    for side in range(2):
        for i in range(2):
            for t in near:
                beyond[side, i, t] = jnp.where(
                    place < 4, xz_recv[1, side, i, tile_of(t)], xz_recv[0, side, i, tile_of(t)]
                )
        ends = [
            jnp.where(place < 4, corner_recv[1, side, high], corner_recv[0, side, high]) for high in range(2)
        ]
        beyond[side, 0, tiles_y] = jnp.where(row < 4, ends[1], ends[0])

    def edge_field(number, t):
        i, half = divmod(number, 2)
        value = lane_roll(mixed[i, t], 64 * half)
        if t < tiles_y or number < 4:
            shift = (64, 0, 32, -32)[number % 4]
            low, high = (lane_roll(beyond[side, i // 2, t], shift) for side in range(2))
            value = jnp.where(group < 4, low, jnp.where(group >= 12, high, value))
        return value

    edge_v = {(c, t): edge_field(c, t) for c in range(C) for t in ring}
    edge_f = {(c, t): edge_field(4 + c, t) for c in range(C) for t in ring}
    edge_w = {t: weight_of(edge_field(7, t)) for t in ring}

    def around_rows(get, t, tiles, by):
        after, before = (t + 1) % tiles, (t - 1) % tiles
        own = get(t)
        above = jnp.where(row < 8 - by, row_roll(own, -by), row_roll(get(after), -by))
        below = jnp.where(row >= by, row_roll(own, by), row_roll(get(before), by))
        return below, above

    def main_total(get, edge, c, x, t):
        below, above = around_rows(lambda t: get(c, x, t), t, tiles_y + 1, 1)
        total = (get(c, x - 1, t) + get(c, x + 1, t)) + (below + above)
        beside_z = lane_roll(edge[c, t], -(8 * (x + 4) + 4))
        own = get(c, x, t)
        total = total + jnp.where(lane == 0, beside_z, lane_roll(own, 1))
        return total + jnp.where(lane == Z - 1, beside_z, lane_roll(own, -1))

    def edge_total(get, edge, c, xs, t):
        own = edge[c, t]
        line = own
        for x in xs:
            line = jnp.where(group == x + 4, lane_roll(get(c, x, t), 8 * (x + 4) + 4), line)
        below, above = around_rows(lambda t: edge[c, t], t, tiles_y + 1, 1)
        total = (lane_roll(own, 8) + lane_roll(own, -8)) + (below + above)
        total = total + jnp.where(place == 4, line, lane_roll(own, 1))
        return total + jnp.where(place == 3, line, lane_roll(own, -1))

    u1_at = lambda c, x, t: u1_ext[c, 2 + x, tile_of(t)]
    u2_at = lambda c, x, t: u2_ext[c, 1 + x, tile_of(t)]
    w_at = lambda x, t: w_ext[2 + x, tile_of(t)]

    edge_1, edge_2 = {}, {}
    for c in range(C):
        for t in ring:
            total = edge_total(v_at, edge_v, c, range(-1, X + 1), t)
            edge_1[c, t] = keep * edge_v[c, t] + edge_w[t] * (edge_f[c, t] + total)
        for x in range(-2, X + 2):
            for t in near if x in (-2, X + 1) else ring:
                total = main_total(v_at, edge_v, c, x, t)
                u1_ext[c, 2 + x, tile_of(t)] = keep * v_at(c, x, t) + w_at(x, t) * (f_at(c, x, t) + total)
    for c in range(C):
        for t in near:
            total = edge_total(u1_at, edge_1, c, range(X), t)
            edge_2[c, t] = keep * edge_1[c, t] + edge_w[t] * (edge_f[c, t] + total)
        for x in range(-1, X + 1):
            for t in near if x in (-1, X) else ring:
                total = main_total(u1_at, edge_1, c, x, t)
                u2_ext[c, 1 + x, tile_of(t)] = keep * u1_at(c, x, t) + w_at(x, t) * (f_at(c, x, t) + total)
    sums = [
        [[main_total(u2_at, edge_2, c, x, t) + f_at(c, x, t) for t in near] for x in range(X)] for c in range(C)
    ]

    correction = []
    for c in range(C):
        rhs = pooled([
            [sums[c][x][t] - (6.0 + r_ext[2 + x, tile_of(t)]) * u2_at(c, x, t) for t in near] for x in range(X)
        ])
        correction.append([weight * (0.125 * total) for weight, total in zip(coarse_weight, rhs)])
    for c in range(C):
        for t in near:
            q_ext[1, c, tile_of(t)] = correction[c][t]
    for t in near:
        edges_t = edge_lanes([(16 * c, correction[c]) for c in range(C)], t)
        zs_coarse[tile_of(t)] = jnp.where(lane < 64, edges_t, zs_coarse[tile_of(t)])
    for sides, copy in coarse_copies():
        pl.when(all_exist(sides, False))(copy.start)

    for j in range(blocks):
        @pl.when(me["gx"] == j)
        def _():
            c_recv[j] = c_send[j]

    settle_parts(c_recv_sem.at[0])
    loads[3].wait()
    finish_compressed(range(c_send.shape[1]))

    settle(step_copies(), q_recv_sem.at[1])
    settle(coarse_copies(), q_recv_sem.at[0])

    ring = range(tiles_y + 2)
    after = lambda t: (t + 1) % len(ring)
    before = lambda t: (t - 1) % len(ring)
    main = {(b, c, t): q_ext[b, c, tile_of(t)] for b in range(3) for c in range(C) for t in ring}
    step_main = {(b, t): q_ext[b, C, tile_of(t)] for b in range(3) for t in ring}
    edge = {
        (b, t): jnp.where(slot_at < 8, h_ext[1, b, tile_of(t)], h_ext[0, b, tile_of(t)])
        for b in range(3) for t in ring
    }
    step_edge = {key: lane_roll(value, -64) for key, value in edge.items()}
    first_main, first_edge = dict(main), dict(edge)

    def above(get, t):
        return jnp.where(row < 6, row_roll(get(t), -2), row_roll(get(after(t)), -2))

    def below(get, t):
        return jnp.where(row >= 2, row_roll(get(t), 2), row_roll(get(before(t)), 2))

    def along(get, b, t):
        low, high = get(max(b - 1, 0), t), get(min(b + 1, 2), t)
        across = jnp.where(even_l, jnp.where(even_r, high, low), get(b, t))
        return lane_swap(get(b, t)) + row_swap(across)

    def inject(edge, b, c, t):
        return lane_roll(edge[b, t], -(16 * c + 8))

    def left_of(main, edge, b, c, t):
        return jnp.where(lane < 2, inject(edge, b, c, t), lane_roll(main[b, c, t], 2))

    def right_of(main, edge, b, c, t):
        return jnp.where(lane >= Z - 2, inject(edge, b, c, t), lane_roll(main[b, c, t], -2))

    def coarse_sweep(main, edge, main_at, edge_at):
        new_main, new_edge = dict(main), dict(edge)
        for b, t in main_at:
            for c in range(C):
                get = lambda b, t, c=c: main[b, c, t]
                row_get = lambda t, b=b, c=c: main[b, c, t]
                total = along(get, b, t) + (above(row_get, t) + below(row_get, t))
                total = total + (left_of(main, edge, b, c, t) + right_of(main, edge, b, c, t))
                new_main[b, c, t] = keep * main[b, c, t] + first_main[b, c, t] + step_main[b, t] * total
        for b, t in edge_at:
            get = lambda b, t: edge[b, t]
            row_get = lambda t, b=b: edge[b, t]
            own = lane_roll(main[b, 0, t], 8)
            for c in range(1, C):
                own = jnp.where(lane < 16 * c, own, lane_roll(main[b, c, t], 16 * c + 8))
            total = along(get, b, t) + (above(row_get, t) + below(row_get, t))
            total = total + jnp.where((slot_at == 8) | (slot_at == 9), own, lane_roll(edge[b, t], 2))
            total = total + jnp.where((slot_at == 6) | (slot_at == 7), own, lane_roll(edge[b, t], -2))
            new_edge[b, t] = keep * edge[b, t] + first_edge[b, t] + step_edge[b, t] * total
        return new_main, new_edge

    everywhere = [(b, t) for b in range(3) for t in ring]
    centre = [(1, t) for t in ring]
    sides_near = [(b, t) for b in (0, 2) for t in near]
    main, edge = coarse_sweep(main, edge, everywhere, everywhere)
    main, edge = coarse_sweep(main, edge, everywhere, centre + sides_near)
    main, edge = coarse_sweep(main, edge, centre + sides_near, [(1, t) for t in near])

    def spread_rows(even, odd, pa):
        if pa == 0:
            return jnp.where(even_r, even, row_roll(odd, 1))
        return jnp.where(even_r, row_roll(even, -1), odd)

    def spread_lanes(even, odd, pb):
        if pb == 0:
            return jnp.where(even_l, even, lane_roll(odd, 1))
        return jnp.where(even_l, lane_roll(even, -1), odd)

    for c in range(C):
        for t in near:
            at = tile_of(t)
            row_get = lambda t, c=c: main[1, c, t]
            own = main[1, c, t]
            rows_near = (below(row_get, t), above(row_get, t))
            lanes_near = (left_of(main, edge, 1, c, t), right_of(main, edge, 1, c, t))
            alone = [spread_lanes(own, own, pb) for pb in range(2)]
            spread = [spread_rows(alone[pb], alone[pb], pa) for pa, pb in corner_of]
            low, high = (spread_lanes(main[b, c, t], main[b, c, t], 0) for b in (0, 2))
            spread = [spread_rows(low, low, 1)] + spread + [spread_rows(high, high, 0)]
            based = [3.0 * own + rows_near[a] for a in range(2)]
            wide = [
                [spread_lanes(based[a] + lanes_near[0], based[a] + lanes_near[1], pb) for pb in range(2)]
                for a in range(2)
            ]
            for x in range(X):
                p = x // 2
                pa, pb = corner_of[p]
                added = spread_rows(wide[0][pb], wide[1][pb], pa) + spread[p + 2 * (x % 2)]
                total = sums[c][x][t] + added
                vel_ref[c, x, at] = keep * (u2_at(c, x, t) + spread[p + 1]) + w_at(x, t) * total

    settle(fine_copies(), a_send_sem.at[0])
    settle(step_copies(), q_send_sem.at[1])
    settle(coarse_copies(), q_send_sem.at[0])
    settle_parts(c_send_sem.at[0])


def write_out(vel_ref, comp_ref, vel_hbm, comp_hbm, sem):
    copies = [
        pltpu.make_async_copy(comp_ref, comp_hbm, sem.at[0]),
        pltpu.make_async_copy(vel_ref, vel_hbm, sem.at[1]),
    ]
    for copy in copies:
        copy.start()
    for copy in copies:
        copy.wait()


def on_device(counts, velocity_prev, forcing, reaction):
    C, X, Y, Z = velocity_prev.shape
    blocks = counts["gx"]
    kept = X // 2
    chunk = Z // blocks
    tiles = -(-(C * (Y // 8)) // (Z // chunk))
    matrix = jnp.asarray(finish_matrix(X, blocks, 8))
    vmem = pl.BlockSpec(memory_space=pltpu.VMEM)
    space = lambda *shape: pltpu.VMEM(shape, jnp.float32)

    velocity, compressed = pl.pallas_call(
        functools.partial(kernel, counts),
        out_shape=(
            jax.ShapeDtypeStruct((C, X, Y, Z), jnp.float32),
            jax.ShapeDtypeStruct((C, Y, kept * blocks, chunk), jnp.float32),
        ),
        in_specs=[pl.BlockSpec(memory_space=pltpu.HBM)] * 4,
        out_specs=(vmem, vmem),
        scratch_shapes=[
            space(C, X + 6, Y + 8, Z),
            space(C, X + 4, Y + 8, Z),
            space(X + 4, Y + 8, Z),
            space(*matrix.shape),
            space(X + 4, Y + 8, Z),
            space(C, X + 4, Y + 8, Z),
            space(C, X + 2, Y + 8, Z),
            space(2, 5 * C + 2, X, Z),
            space(2, 5 * C + 2, X, Z),
            space(4, 16, Z),
            space(4, 16, Z),
            space(4, Y, Z),
            space(2, 4, Y + 8, Z),
            space(2, 8, Z),
            space(2, 2, 8, Z),
            space(2, Y, Z),
            space(2, 2, 2, Y, Z),
            space(2, 2, 2, 8, Z),
            space(3, C + 1, Y + 16, Z),
            space(2, 3, Y + 16, Z),
            space(Y, Z),
            space(blocks, tiles, kept, 8, Z),
            space(blocks, tiles, kept, 8, Z),
            space(max((blocks - 1) * tiles * kept * 8, 128 * Y), Z),
            pltpu.SemaphoreType.DMA((1,)),
            pltpu.SemaphoreType.DMA((1,)),
            pltpu.SemaphoreType.DMA((2,)),
            pltpu.SemaphoreType.DMA((2,)),
            pltpu.SemaphoreType.DMA((1,)),
            pltpu.SemaphoreType.DMA((1,)),
            pltpu.SemaphoreType.DMA((4,)),
        ],
        compiler_params=pltpu.CompilerParams(collective_id=0, has_side_effects=True, vmem_limit_bytes=40000000),
    )(*(pltpu.with_memory_space_constraint(a, pltpu.HBM) for a in (velocity_prev, forcing, reaction, matrix)))
    velocity, compressed = pl.pallas_call(
        write_out,
        out_shape=(
            jax.ShapeDtypeStruct(velocity.shape, jnp.float32),
            jax.ShapeDtypeStruct(compressed.shape, jnp.float32),
        ),
        in_specs=[vmem, vmem],
        out_specs=[pl.BlockSpec(memory_space=pltpu.HBM)] * 2,
        scratch_shapes=[pltpu.SemaphoreType.DMA((2,))],
        compiler_params=pltpu.CompilerParams(vmem_limit_bytes=4000000),
    )(velocity, compressed)
    return velocity, jnp.swapaxes(compressed, 2, 3)


def solution(mesh):
    counts = {axis: mesh.shape[axis] for axis in ("agg", "gx", "gy")}
    placed = (P(None, "gx", "gy", "agg"), P(None, "gx", "gy", "agg"), P("gx", "gy", "agg"))
    return jax.shard_map(
        functools.partial(on_device, counts),
        mesh=mesh,
        in_specs=placed,
        out_specs=(P(None, "gx", "gy", "agg"), P(None, "gy", ("agg", "gx"), None)),
        check_vma=False,
    )
```

```python
import functools
import itertools
import math

import jax
import jax.numpy as jnp
import numpy as np
from jax import lax
from jax.experimental import pallas as pl
from jax.experimental.pallas import tpu as pltpu
from jax.sharding import PartitionSpec as P

SWEEPS = 2
COARSE_SWEEPS = 4
LX = 5
MESH = pl.DeviceIdType.MESH

damping = 0.8
keep = 1.0 - damping
root_half = 0.7071067811865476


def local_levels(cells_x):
    return min(LX, cells_x.bit_length() - 1)


def finish_matrix(cells_x, blocks, rows):
    levels = local_levels(cells_x)
    kept = cells_x // 2
    eye = np.eye(blocks * kept).reshape(blocks, kept, blocks * kept)
    width = cells_x >> levels
    approx = eye[:, :width].reshape(blocks * width, -1)
    details, at = [], width
    for level in range(levels, 1, -1):
        width = cells_x >> level
        details.append(eye[:, at : at + width].reshape(blocks * width, -1))
        at += width
    for level in range(levels, LX):
        low, high = approx[0::2], approx[1::2]
        approx, detail = (low + high) * root_half, (low - high) * root_half
        details.insert(0, detail)
    along_x = np.concatenate([approx] + details, axis=0)
    along_y = np.zeros((rows, rows))
    for row in range(0, rows, 2):
        along_y[row, row : row + 2] = root_half
        along_y[row + 1, row : row + 2] = root_half, -root_half
    return np.einsum("qk,yr->yqkr", along_x, along_y).reshape(-1, blocks * kept * rows).astype(np.float32)


def around():
    axes = ("gx", "gy", "agg")
    found = []
    for number in range(1, 27):
        turn = [(number // 3**i) % 3 for i in range(3)]
        found.append(tuple((axis, way == 1) for axis, way in zip(axes, turn) if way))
    return sorted(found, key=lambda sides: (-len(sides), sides))


far = 1e30


def kernel(
    sizes, v_hbm, f_hbm, r_hbm, m_hbm, vel_ref, comp_ref, v_ext, f_ext, r_ext, m_ref, w_ext, u1_ext, u2_ext,
    y_send, y_recv, xy_send, xy_recv, z_send, z_recv, yz_send, yz_recv, xz_send, xz_recv, corner_recv,
    q_ext, h_ext, zs_coarse, c_send, c_recv, measure,
    a_send_sem, a_recv_sem, q_send_sem, q_recv_sem, c_send_sem, c_recv_sem, in_sem,
):
    counts = sizes
    C, X, Y, Z = vel_ref.shape
    me = {axis: lax.axis_index(axis) for axis in counts}
    blocks = counts["gx"]
    chunk = Z // blocks
    rows_ext = Y + 8
    f32 = jnp.float32

    loads = [
        pltpu.make_async_copy(src, dst, in_sem.at[i])
        for i, (src, dst) in enumerate((
            (v_hbm, v_ext.at[:, 3 : 3 + X, :Y]),
            (f_hbm, f_ext.at[:, 2 : 2 + X, :Y]),
            (r_hbm, r_ext.at[2 : 2 + X, :Y]),
            (m_hbm, m_ref),
        ))
    ]
    for load in loads:
        load.start()

    def exists(axis, high):
        return me[axis] < counts[axis] - 1 if high else me[axis] > 0

    def all_exist(sides, flip):
        there = None
        for axis, high in sides:
            one = exists(axis, high != flip)
            there = one if there is None else there & one
        return there

    def beside(*sides):
        return {axis: me[axis] + (1 if high else -1) for axis, high in sides}

    barrier = pltpu.get_barrier_semaphore()
    expected = blocks - 1
    for sides in around():
        if len(sides) > 1 or sides[0][0] != "gx":
            there = all_exist(sides, False)
            expected = expected + there.astype(jnp.int32)

            @pl.when(there)
            def _():
                pl.semaphore_signal(barrier, inc=1, device_id=beside(*sides), device_id_type=MESH)

    for step in range(1, blocks):
        pl.semaphore_signal(
            barrier, inc=1, device_id={"gx": lax.rem(me["gx"] + step, blocks)}, device_id_type=MESH
        )

    lane = lax.broadcasted_iota(jnp.int32, (8, Z), 1)
    row = lax.broadcasted_iota(jnp.int32, (8, Z), 0)
    place = lane % 8
    group = lane // 8
    low_half = (lane < 32) | (lane >= 96)
    near_groups = (group % 8 == 2) | (group % 8 == 3) | (group % 8 == 4) | (group % 8 == 5)

    def fine_messages(sides):
        at = {axis: high for axis, high in sides}
        x, y, z = at.get("gx"), at.get("gy"), at.get("agg")
        from_x, from_y, from_z = 0 if x else 1, 0 if y else 1, 0 if z else 1
        if z is None and y is None:
            made = []
            for ref, depth, fill in ((v_ext, 3, 0.0), (f_ext, 2, 0.0), (r_ext, 2, far)):
                here = pl.ds(X if x else depth, depth)
                there = pl.ds(0 if x else depth + X, depth)
                index = (slice(None),) if ref is not r_ext else ()
                made.append((ref.at[index + (here, pl.ds(0, Y))], ref.at[index + (there, pl.ds(0, Y))], fill))
            return made
        if z is None and x is None:
            return [(y_send.at[int(y)], y_recv.at[from_y], None)]
        if z is None:
            return [(xy_send.at[2 * int(x) + int(y)], xy_recv.at[2 * from_x + from_y], None)]
        if x is None and y is None:
            return [(z_send, z_recv.at[from_z, :, pl.ds(0, Y)], None)]
        if x is None:
            return [(yz_send.at[int(y)], yz_recv.at[from_z, from_y], None)]
        if y is None:
            return [(xz_send, xz_recv.at[from_z, from_x], None)]
        return [(xz_send.at[0, pl.ds(Y - 8 if y else 0, 8)], corner_recv.at[from_z, from_x, from_y], 0.0)]

    def remote(src, dst, send_sem, recv_sem, sides):
        return pltpu.make_async_remote_copy(
            src_ref=src, dst_ref=dst, send_sem=send_sem, recv_sem=recv_sem,
            device_id=beside(*sides), device_id_type=MESH,
        )

    def fine_copies():
        return [
            (sides, remote(src, dst, a_send_sem.at[0], a_recv_sem.at[0], sides))
            for sides in around()
            for src, dst, _ in fine_messages(sides)
        ]

    def rows_of(copies):
        found = {}
        for sides, copy in copies:
            axes = tuple(axis for axis, _ in sides)
            if all(high for _, high in sides):
                found[axes] = found.get(axes, 0) + math.prod(copy.src_ref.shape[:-1])
        return found

    def settle(copies, sem):
        sizes = rows_of(copies)
        neighbours = {
            axis: exists(axis, False).astype(jnp.int32) + exists(axis, True).astype(jnp.int32) for axis in counts
        }
        options = {axis: {1: (0,), 2: (1,)}.get(count, (1, 2)) for axis, count in counts.items()}
        for numbers in itertools.product(*options.values()):
            number = dict(zip(options, numbers))
            rows = sum(size * math.prod(number[axis] for axis in axes) for axes, size in sizes.items())
            there = None
            for axis, value in number.items():
                one = neighbours[axis] == value
                there = one if there is None else there & one
            if rows:
                part = measure.at[pl.ds(0, rows)]
                pl.when(there)(pltpu.make_async_copy(part, part, sem).wait)

    def coarse_message(sides, first=0, fields=C):
        at = {axis: 1 if high else -1 for axis, high in sides}
        block = 1 - at.get("gx", 0)
        here, there = {
            0: (slice(0, Y), slice(0, Y)),
            1: (slice(Y - 8, Y), slice(Y + 8, Y + 16)),
            -1: (slice(0, 8), slice(Y, Y + 8)),
        }[at.get("gy", 0)]
        if "agg" in at:
            return zs_coarse.at[here], h_ext.at[0 if at["agg"] > 0 else 1, block, there]
        which = pl.ds(first, fields)
        return q_ext.at[1, which, here], q_ext.at[block, which, there]

    def coarse_copies():
        return [
            (sides, remote(*coarse_message(sides), q_send_sem.at[0], q_recv_sem.at[0], sides))
            for sides in around()
        ]

    def step_copies():
        return [
            (sides, remote(*coarse_message(sides, C, 1), q_send_sem.at[1], q_recv_sem.at[1], sides))
            for sides in around()
            if "agg" not in dict(sides)
        ]

    far_high = jnp.where(low_half, far, 0.0).astype(f32)
    for sides in around():
        @pl.when(jnp.logical_not(all_exist(sides, True)))
        def _():
            axes = tuple(axis for axis, _ in sides)
            for _, target, fill in fine_messages(sides):
                if fill is not None:
                    target[...] = jnp.full(target.shape, fill, f32)
                elif axes == ("gy",):
                    target[: 5 * C] = jnp.zeros((5 * C, 8, Z), f32)
                    target[5 * C :] = jnp.full((2, 8, Z), far, f32)
                elif axes == ("gx", "gy"):
                    target[0:8] = jnp.zeros((8, Z), f32)
                    target[8:16] = jnp.where(row == 4 * C - 8, far, 0.0)
                elif axes == ("agg",):
                    target[:3] = jnp.zeros((3, Y, Z), f32)
                    for t in range(Y // 8):
                        target[3, t * 8 : t * 8 + 8] = far_high
                elif axes == ("gy", "agg"):
                    target[...] = jnp.where(row >= 6, far_high, 0.0)
                else:
                    target[0] = jnp.zeros((Y, Z), f32)
                    for t in range(Y // 8):
                        target[1, t * 8 : t * 8 + 8] = jnp.where(
                            (group == 0) | (group == 1) | (group == 6) | (group == 7), far, 0.0
                        )
            for target in [coarse_message(sides)[1], coarse_message(sides, C, 1)[1]][: 1 + ("agg" not in axes)]:
                target[...] = jnp.zeros(target.shape, f32)

    tiles_y = Y // 8
    near, ring = range(tiles_y), range(tiles_y + 1)
    tile_of = lambda t: slice(t * 8, t * 8 + 8)
    even_l = lane % 2 == 0
    even_r = row % 2 == 0
    lane_roll = lambda t, shift: pltpu.roll(t, shift % Z, 1) if shift % Z else t
    row_roll = lambda t, shift: pltpu.roll(t, shift % 8, 0)
    v_flat = v_ext.reshape(C * (X + 6) * rows_ext, Z)
    f_flat = f_ext.reshape(C * (X + 4) * rows_ext, Z)
    r_flat = r_ext.reshape((X + 4) * rows_ext, Z)

    def x_line(number, y):
        if number < 3 * C:
            c, ref, extra = number // 3, v_flat, 3
        elif number < 5 * C:
            c, ref, extra = (number - 3 * C) // 2, f_flat, 2
        else:
            c, ref, extra = 0, r_flat, 2
        return ref, pl.ds((c * (X + 2 * extra) + extra) * rows_ext + y, X, stride=rows_ext)

    depth_of = lambda number: number % 3 if number < 3 * C else (number - 3 * C) % 2

    loads[0].wait()
    loads[1].wait()
    loads[2].wait()
    for number in range(5 * C + 2):
        for side in range(2):
            depth = depth_of(number)
            ref, at = x_line(number, Y - 1 - depth if side else depth)
            y_send[side, number] = ref[at, :]
    for high_x in range(2):
        for high_y in range(2):
            xs = [X - 1 - d if high_x else d for d in range(2)]
            ys = [Y - 1 - d if high_y else d for d in range(2)]
            target = xy_send.at[2 * high_x + high_y]
            for c in range(C):
                for i, (x, y) in enumerate(((xs[0], ys[0]), (xs[1], ys[0]), (xs[0], ys[1]))):
                    target[3 * c + i : 3 * c + i + 1] = v_ext[c, 3 + x, y : y + 1]
                target[3 * C + c : 3 * C + c + 1] = f_ext[c, 2 + xs[0], ys[0] : ys[0] + 1]
            target[4 * C : 4 * C + 1] = r_ext[2 + xs[0], ys[0] : ys[0] + 1]
    v_at = lambda c, x, t: v_ext[c, 3 + x, tile_of(t)]
    f_at = lambda c, x, t: f_ext[c, 2 + x, tile_of(t)]
    held = (
        (lambda x, t: v_at(0, x, t), lambda x, t: v_at(1, x, t)),
        (lambda x, t: v_at(2, x, t), None),
        (lambda x, t: f_at(0, x, t), lambda x, t: f_at(1, x, t)),
        (lambda x, t: f_at(2, x, t), lambda x, t: r_ext[2 + x, tile_of(t)]),
    )
    from_ends = jnp.where(place < 4, 3 - place, Z + 3 - place)
    for t in near:
        turned = []
        for pair in held:
            packed = jnp.zeros((8, Z), f32)
            for half, get in enumerate(pair):
                if get is not None:
                    for x in range(X):
                        at = (x + 4 + 8 * half) % 16
                        packed = jnp.where(group == at, jnp.take_along_axis(get(x, t), from_ends, axis=1), packed)
            turned.append(packed)
        for i in range(4):
            z_send[i, tile_of(t)] = turned[i]
            for side in range(2):
                if t == (tiles_y - 1 if side else 0):
                    first = 6 if side else 0
                    yz_send[side, 2 * i : 2 * i + 2] = turned[i][first : first + 2]
        for i in range(2):
            xz_send[i, tile_of(t)] = jnp.where(near_groups, turned[2 * i], lane_roll(turned[2 * i + 1], 32))
    pl.semaphore_wait(barrier, expected)
    for sides, copy in fine_copies():
        pl.when(all_exist(sides, False))(copy.start)

    kept = X // 2
    parts = Y // 8
    combos_per_tile = Z // chunk

    def c_copy(j, source):
        return pltpu.make_async_remote_copy(
            src_ref=c_send.at[j],
            dst_ref=c_recv.at[source],
            send_sem=c_send_sem.at[0],
            recv_sem=c_recv_sem.at[0],
            device_id={"gx": j},
            device_id_type=MESH,
        )

    def settle_parts(sem):
        rows = (blocks - 1) * math.prod(c_send.shape[1:-1])
        if rows:
            part = measure.at[pl.ds(0, rows)]
            pltpu.make_async_copy(part, part, sem).wait()

    def finish_compressed(tiles):
        coefs = blocks * kept
        for tile in tiles:
            gathered = c_recv[:, tile].reshape(coefs * 8, Z)
            done = lax.dot_general(
                m_ref[...], gathered, (((1,), (0,)), ((), ())),
                precision=lax.Precision.HIGHEST, preferred_element_type=jnp.float32,
            )
            for place in range(combos_per_tile):
                c, part = divmod(tile * combos_per_tile + place, parts)
                if c < C:
                    for y in range(8):
                        comp_ref[c, part * 8 + y] = done[
                            y * coefs : (y + 1) * coefs, place * chunk : (place + 1) * chunk
                        ]

    lane_take = lambda t, source: jnp.take_along_axis(t, source, axis=1)
    pair_of = lane + 1 - 2 * (lane % 2)
    lane_swap = lambda t: lane_take(t, pair_of)
    row_swap = lambda t: jnp.where(even_r, row_roll(t, -1), row_roll(t, 1))
    slot_at = lane % 16
    corner_of = ((0, 0), (0, 1), (1, 1), (1, 0))

    def pooled(planes):
        pairs = [[planes[x][t] + planes[x + 1][t] for t in near] for x in range(0, X, 2)]
        out = []
        for t in near:
            t0, t1, t2, t3 = (pair[t] for pair in pairs)
            left = jnp.where(even_r, t0, t3) + row_swap(jnp.where(even_r, t3, t0))
            right = jnp.where(even_r, t1, t2) + row_swap(jnp.where(even_r, t2, t1))
            out.append(jnp.where(even_l, left, right) + lane_swap(jnp.where(even_l, right, left)))
        return out

    from_far = jnp.where(slot_at < 8, 6, Z + 6) - slot_at + 2 * (slot_at % 2)

    def edge_lanes(fields, t):
        packed = jnp.zeros((8, Z), f32)
        for start, field in fields:
            packed = jnp.where((lane >= start) & (lane < start + 16), lane_take(field[t], from_far), packed)
        return packed

    coarse_weight = [
        damping / ((6.0 + 0.5 * total) * 0.25)
        for total in pooled([[r_ext[2 + x, tile_of(t)] for t in near] for x in range(X)])
    ]
    coarse_step = [0.25 * weight for weight in coarse_weight]
    step_edges = [edge_lanes([(64 + 16 * c, coarse_step) for c in range(C)], t) for t in near]
    for t in near:
        q_ext[1, C, tile_of(t)] = coarse_step[t]
        zs_coarse[tile_of(t)] = step_edges[t]
    for x in range(X):
        for t in near:
            w_ext[2 + x, tile_of(t)] = damping / (6.0 + r_ext[2 + x, tile_of(t)])

    levels = local_levels(X)
    for c in range(C):
        for t in near:
            approx, details = [v_at(c, x, t) for x in range(X)], []
            for level in range(levels):
                low, high = approx[0::2], approx[1::2]
                approx = [(a + b) * root_half for a, b in zip(low, high)]
                if level > 0:
                    details = [(a - b) * root_half for a, b in zip(low, high)] + details
            tile, spot = divmod(c * parts + t, combos_per_tile)
            inside = (lane >= spot * chunk) & (lane < (spot + 1) * chunk)
            for k, values in enumerate(approx + details):
                done = (jnp.where(even_l, values, -values) + lane_swap(values)) * root_half
                for j in range(blocks):
                    moved = lane_roll(done, spot * chunk - j * chunk)
                    if spot:
                        moved = jnp.where(inside, moved, c_send[j, tile, k])
                    c_send[j, tile, k] = moved

    for c in range(C):
        for x in range(X):
            for t in near:
                own = v_at(c, x, t)
                total = f_at(c, x, t) + jnp.where(lane == 0, 0.0, lane_roll(own, 1))
                total = total + jnp.where(lane == Z - 1, 0.0, lane_roll(own, -1))
                for other in range(max(x - 1, 0), min(x + 2, X)):
                    if other != x:
                        total = total + v_at(c, other, t)
                for other, shift, inner in ((t + 1, -1, row < 7), (t - 1, 1, row >= 1)):
                    beyond = row_roll(v_at(c, x, other), shift) if other in near else 0.0
                    total = total + jnp.where(inner, row_roll(own, shift), beyond)
                u1_ext[c, 2 + x, tile_of(t)] = keep * own + w_ext[2 + x, tile_of(t)] * total

    settle(fine_copies(), a_recv_sem.at[0])

    for sides, copy in step_copies():
        pl.when(all_exist(sides, False))(copy.start)
    for j in range(blocks):
        pl.when(me["gx"] != j)(c_copy(j, me["gx"]).start)

    for number in range(5 * C + 2):
        for side in range(2):
            depth = depth_of(number)
            ref, at = x_line(number, Y + depth if side else rows_ext - 1 - depth)
            ref[at, :] = y_recv[side, number]
    for high_x in range(2):
        for high_y in range(2):
            xs = [X + d if high_x else -1 - d for d in range(2)]
            ys = [Y + d if high_y else rows_ext - 1 - d for d in range(2)]
            source = xy_recv.at[2 * high_x + high_y]
            for c in range(C):
                for i, (x, y) in enumerate(((xs[0], ys[0]), (xs[1], ys[0]), (xs[0], ys[1]))):
                    v_ext[c, 3 + x, y : y + 1] = source[3 * c + i : 3 * c + i + 1]
                f_ext[c, 2 + xs[0], ys[0] : ys[0] + 1] = source[3 * C + c : 3 * C + c + 1]
            r_ext[2 + xs[0], ys[0] : ys[0] + 1] = source[4 * C : 4 * C + 1]
    for side in range(2):
        for i in range(4):
            z_recv[side, i, Y : Y + 2] = yz_recv[side, 1, 2 * i : 2 * i + 2]
            z_recv[side, i, Y + 6 : Y + 8] = yz_recv[side, 0, 2 * i : 2 * i + 2]

    def weight_of(reaction):
        return jnp.where(reaction < 0.1 * far, damping / (6.0 + reaction), 0.0)

    for x in range(-2, X + 2):
        outside = max(-x, x - X + 1)
        for t in ring:
            if (outside > 0 and t < tiles_y) or (t == tiles_y and outside < 2):
                w_ext[2 + x, tile_of(t)] = weight_of(r_ext[2 + x, tile_of(t)])

    mixed = {}
    for i in range(4):
        for t in ring:
            mixed[i, t] = jnp.where(place < 4, z_recv[1, i, tile_of(t)], z_recv[0, i, tile_of(t)])
    beyond = {}
    for side in range(2):
        for i in range(2):
            for t in near:
                beyond[side, i, t] = jnp.where(
                    place < 4, xz_recv[1, side, i, tile_of(t)], xz_recv[0, side, i, tile_of(t)]
                )
        ends = [
            jnp.where(place < 4, corner_recv[1, side, high], corner_recv[0, side, high]) for high in range(2)
        ]
        beyond[side, 0, tiles_y] = jnp.where(row < 4, ends[1], ends[0])

    def edge_field(number, t):
        i, half = divmod(number, 2)
        value = lane_roll(mixed[i, t], 64 * half)
        if t < tiles_y or number < 4:
            shift = (64, 0, 32, -32)[number % 4]
            low, high = (lane_roll(beyond[side, i // 2, t], shift) for side in range(2))
            value = jnp.where(group < 4, low, jnp.where(group >= 12, high, value))
        return value

    edge_v = {(c, t): edge_field(c, t) for c in range(C) for t in ring}
    edge_f = {(c, t): edge_field(4 + c, t) for c in range(C) for t in ring}
    edge_w = {t: weight_of(edge_field(7, t)) for t in ring}

    def around_rows(get, t, tiles, by):
        after, before = (t + 1) % tiles, (t - 1) % tiles
        own = get(t)
        above = jnp.where(row < 8 - by, row_roll(own, -by), row_roll(get(after), -by))
        below = jnp.where(row >= by, row_roll(own, by), row_roll(get(before), by))
        return below, above

    def rows_beside(at, t):
        get = lambda t: at(tile_of(t))
        if t < tiles_y:
            above = at(pl.ds(t * 8 + 1, 8))
        else:
            above = jnp.where(row < 7, row_roll(get(t), -1), row_roll(get(0), -1))
        if t > 0:
            below = at(pl.ds(t * 8 - 1, 8))
        else:
            below = jnp.where(row >= 1, row_roll(get(t), 1), row_roll(get(tiles_y), 1))
        return below, above

    def main_total(get, edge, c, x, t):
        below, above = rows_beside(lambda rows: get(c, x, rows), t)
        get = lambda c, x, t, get=get: get(c, x, tile_of(t))
        total = (get(c, x - 1, t) + get(c, x + 1, t)) + (below + above)
        beside_z = lane_roll(edge[c, t], -(8 * (x + 4) + 4))
        own = get(c, x, t)
        total = total + jnp.where(lane == 0, beside_z, lane_roll(own, 1))
        return total + jnp.where(lane == Z - 1, beside_z, lane_roll(own, -1))

    def edge_total(get, edge, c, xs, t):
        own = edge[c, t]
        line = own
        for x in xs:
            line = jnp.where(group == x + 4, lane_roll(get(c, x, t), 8 * (x + 4) + 4), line)
        below, above = around_rows(lambda t: edge[c, t], t, tiles_y + 1, 1)
        total = (lane_roll(own, 8) + lane_roll(own, -8)) + (below + above)
        total = total + jnp.where(place == 4, line, lane_roll(own, 1))
        return total + jnp.where(place == 3, line, lane_roll(own, -1))

    u1_at = lambda c, x, t: u1_ext[c, 2 + x, tile_of(t)]
    u2_at = lambda c, x, t: u2_ext[c, 1 + x, tile_of(t)]
    v_rows = lambda c, x, rows: v_ext[c, 3 + x, rows]
    u1_rows = lambda c, x, rows: u1_ext[c, 2 + x, rows]
    u2_rows = lambda c, x, rows: u2_ext[c, 1 + x, rows]
    w_at = lambda x, t: w_ext[2 + x, tile_of(t)]

    edge_1, edge_2 = {}, {}
    for c in range(C):
        for t in ring:
            total = edge_total(v_at, edge_v, c, range(-1, X + 1), t)
            edge_1[c, t] = keep * edge_v[c, t] + edge_w[t] * (edge_f[c, t] + total)
        for x in range(-2, X + 2):
            if 0 <= x < X:
                for t in near:
                    beside_z = lane_roll(edge_v[c, t], -(8 * (x + 4) + 4))
                    total = jnp.where((lane == 0) | (lane == Z - 1), beside_z, 0.0)
                    if t == 0:
                        total = total + jnp.where(row == 0, row_roll(v_at(c, x, tiles_y), 1), 0.0)
                    if t == tiles_y - 1:
                        total = total + jnp.where(row == 7, row_roll(v_at(c, x, tiles_y), -1), 0.0)
                    if x in (0, X - 1):
                        total = total + v_at(c, -1 if x == 0 else X, t)
                    u1_ext[c, 2 + x, tile_of(t)] = u1_at(c, x, t) + w_at(x, t) * total
            for t in near if x in (-2, X + 1) else [tiles_y] if 0 <= x < X else ring:
                total = main_total(v_rows, edge_v, c, x, t)
                u1_ext[c, 2 + x, tile_of(t)] = keep * v_at(c, x, t) + w_at(x, t) * (f_at(c, x, t) + total)
    for c in range(C):
        for t in near:
            total = edge_total(u1_at, edge_1, c, range(X), t)
            edge_2[c, t] = keep * edge_1[c, t] + edge_w[t] * (edge_f[c, t] + total)
        for x in range(-1, X + 1):
            for t in near if x in (-1, X) else ring:
                total = main_total(u1_rows, edge_1, c, x, t)
                u2_ext[c, 1 + x, tile_of(t)] = keep * u1_at(c, x, t) + w_at(x, t) * (f_at(c, x, t) + total)
    sums = [
        [[main_total(u2_rows, edge_2, c, x, t) + f_at(c, x, t) for t in near] for x in range(X)] for c in range(C)
    ]

    correction = []
    for c in range(C):
        rhs = pooled([
            [sums[c][x][t] - (6.0 + r_ext[2 + x, tile_of(t)]) * u2_at(c, x, t) for t in near] for x in range(X)
        ])
        correction.append([weight * (0.125 * total) for weight, total in zip(coarse_weight, rhs)])
    for c in range(C):
        for t in near:
            q_ext[1, c, tile_of(t)] = correction[c][t]
    for t in near:
        edges_t = edge_lanes([(16 * c, correction[c]) for c in range(C)], t)
        zs_coarse[tile_of(t)] = jnp.where(lane < 64, edges_t, zs_coarse[tile_of(t)])
    for sides, copy in coarse_copies():
        pl.when(all_exist(sides, False))(copy.start)

    for j in range(blocks):
        @pl.when(me["gx"] == j)
        def _():
            c_recv[j] = c_send[j]

    settle_parts(c_recv_sem.at[0])
    loads[3].wait()
    finish_compressed(range(c_send.shape[1]))

    settle(step_copies(), q_recv_sem.at[1])
    settle(coarse_copies(), q_recv_sem.at[0])

    ring = range(tiles_y + 2)
    after = lambda t: (t + 1) % len(ring)
    before = lambda t: (t - 1) % len(ring)
    main = {(b, c, t): q_ext[b, c, tile_of(t)] for b in range(3) for c in range(C) for t in ring}
    step_main = {(b, t): q_ext[b, C, tile_of(t)] for b in range(3) for t in ring}
    edge = {
        (b, t): jnp.where(slot_at < 8, h_ext[1, b, tile_of(t)], h_ext[0, b, tile_of(t)])
        for b in range(3) for t in ring
    }
    step_edge = {key: lane_roll(value, -64) for key, value in edge.items()}
    first_main, first_edge = dict(main), dict(edge)

    def above(get, t):
        return jnp.where(row < 6, row_roll(get(t), -2), row_roll(get(after(t)), -2))

    def below(get, t):
        return jnp.where(row >= 2, row_roll(get(t), 2), row_roll(get(before(t)), 2))

    def along(get, b, t):
        low, high = get(max(b - 1, 0), t), get(min(b + 1, 2), t)
        across = jnp.where(even_l, jnp.where(even_r, high, low), get(b, t))
        return lane_swap(get(b, t)) + row_swap(across)

    def inject(edge, b, c, t):
        return lane_roll(edge[b, t], -(16 * c + 8))

    def left_of(main, edge, b, c, t):
        return jnp.where(lane < 2, inject(edge, b, c, t), lane_roll(main[b, c, t], 2))

    def right_of(main, edge, b, c, t):
        return jnp.where(lane >= Z - 2, inject(edge, b, c, t), lane_roll(main[b, c, t], -2))

    def coarse_sweep(main, edge, main_at, edge_at):
        new_main, new_edge = dict(main), dict(edge)
        for b, t in main_at:
            for c in range(C):
                get = lambda b, t, c=c: main[b, c, t]
                row_get = lambda t, b=b, c=c: main[b, c, t]
                total = along(get, b, t) + (above(row_get, t) + below(row_get, t))
                total = total + (left_of(main, edge, b, c, t) + right_of(main, edge, b, c, t))
                new_main[b, c, t] = keep * main[b, c, t] + first_main[b, c, t] + step_main[b, t] * total
        for b, t in edge_at:
            get = lambda b, t: edge[b, t]
            row_get = lambda t, b=b: edge[b, t]
            own = lane_roll(main[b, 0, t], 8)
            for c in range(1, C):
                own = jnp.where(lane < 16 * c, own, lane_roll(main[b, c, t], 16 * c + 8))
            total = along(get, b, t) + (above(row_get, t) + below(row_get, t))
            total = total + jnp.where((slot_at == 8) | (slot_at == 9), own, lane_roll(edge[b, t], 2))
            total = total + jnp.where((slot_at == 6) | (slot_at == 7), own, lane_roll(edge[b, t], -2))
            new_edge[b, t] = keep * edge[b, t] + first_edge[b, t] + step_edge[b, t] * total
        return new_main, new_edge

    everywhere = [(b, t) for b in range(3) for t in ring]
    centre = [(1, t) for t in ring]
    sides_near = [(b, t) for b in (0, 2) for t in near]
    main, edge = coarse_sweep(main, edge, everywhere, everywhere)
    main, edge = coarse_sweep(main, edge, everywhere, centre + sides_near)
    main, edge = coarse_sweep(main, edge, centre + sides_near, [(1, t) for t in near])

    def spread_rows(even, odd, pa):
        if pa == 0:
            return jnp.where(even_r, even, row_roll(odd, 1))
        return jnp.where(even_r, row_roll(even, -1), odd)

    def spread_lanes(even, odd, pb):
        if pb == 0:
            return jnp.where(even_l, even, lane_roll(odd, 1))
        return jnp.where(even_l, lane_roll(even, -1), odd)

    for c in range(C):
        for t in near:
            at = tile_of(t)
            row_get = lambda t, c=c: main[1, c, t]
            own = main[1, c, t]
            rows_near = (below(row_get, t), above(row_get, t))
            lanes_near = (left_of(main, edge, 1, c, t), right_of(main, edge, 1, c, t))
            alone = [spread_lanes(own, own, pb) for pb in range(2)]
            spread = [spread_rows(alone[pb], alone[pb], pa) for pa, pb in corner_of]
            low, high = (spread_lanes(main[b, c, t], main[b, c, t], 0) for b in (0, 2))
            spread = [spread_rows(low, low, 1)] + spread + [spread_rows(high, high, 0)]
            based = [3.0 * own + rows_near[a] for a in range(2)]
            wide = [
                [spread_lanes(based[a] + lanes_near[0], based[a] + lanes_near[1], pb) for pb in range(2)]
                for a in range(2)
            ]
            for x in range(X):
                p = x // 2
                pa, pb = corner_of[p]
                added = spread_rows(wide[0][pb], wide[1][pb], pa) + spread[p + 2 * (x % 2)]
                total = sums[c][x][t] + added
                vel_ref[c, x, at] = keep * (u2_at(c, x, t) + spread[p + 1]) + w_at(x, t) * total

    settle(fine_copies(), a_send_sem.at[0])
    settle(step_copies(), q_send_sem.at[1])
    settle(coarse_copies(), q_send_sem.at[0])
    settle_parts(c_send_sem.at[0])


def write_out(vel_ref, comp_ref, vel_hbm, comp_hbm, sem):
    copies = [
        pltpu.make_async_copy(comp_ref, comp_hbm, sem.at[0]),
        pltpu.make_async_copy(vel_ref, vel_hbm, sem.at[1]),
    ]
    for copy in copies:
        copy.start()
    for copy in copies:
        copy.wait()


def on_device(counts, velocity_prev, forcing, reaction):
    C, X, Y, Z = velocity_prev.shape
    blocks = counts["gx"]
    kept = X // 2
    chunk = Z // blocks
    tiles = -(-(C * (Y // 8)) // (Z // chunk))
    matrix = jnp.asarray(finish_matrix(X, blocks, 8))
    vmem = pl.BlockSpec(memory_space=pltpu.VMEM)
    space = lambda *shape: pltpu.VMEM(shape, jnp.float32)

    velocity, compressed = pl.pallas_call(
        functools.partial(kernel, counts),
        out_shape=(
            jax.ShapeDtypeStruct((C, X, Y, Z), jnp.float32),
            jax.ShapeDtypeStruct((C, Y, kept * blocks, chunk), jnp.float32),
        ),
        in_specs=[pl.BlockSpec(memory_space=pltpu.HBM)] * 4,
        out_specs=(vmem, vmem),
        scratch_shapes=[
            space(C, X + 6, Y + 8, Z),
            space(C, X + 4, Y + 8, Z),
            space(X + 4, Y + 8, Z),
            space(*matrix.shape),
            space(X + 4, Y + 8, Z),
            space(C, X + 4, Y + 8, Z),
            space(C, X + 2, Y + 8, Z),
            space(2, 5 * C + 2, X, Z),
            space(2, 5 * C + 2, X, Z),
            space(4, 16, Z),
            space(4, 16, Z),
            space(4, Y, Z),
            space(2, 4, Y + 8, Z),
            space(2, 8, Z),
            space(2, 2, 8, Z),
            space(2, Y, Z),
            space(2, 2, 2, Y, Z),
            space(2, 2, 2, 8, Z),
            space(3, C + 1, Y + 16, Z),
            space(2, 3, Y + 16, Z),
            space(Y, Z),
            space(blocks, tiles, kept, 8, Z),
            space(blocks, tiles, kept, 8, Z),
            space(max((blocks - 1) * tiles * kept * 8, 128 * Y), Z),
            pltpu.SemaphoreType.DMA((1,)),
            pltpu.SemaphoreType.DMA((1,)),
            pltpu.SemaphoreType.DMA((2,)),
            pltpu.SemaphoreType.DMA((2,)),
            pltpu.SemaphoreType.DMA((1,)),
            pltpu.SemaphoreType.DMA((1,)),
            pltpu.SemaphoreType.DMA((4,)),
        ],
        compiler_params=pltpu.CompilerParams(collective_id=0, has_side_effects=True, vmem_limit_bytes=40000000),
    )(*(pltpu.with_memory_space_constraint(a, pltpu.HBM) for a in (velocity_prev, forcing, reaction, matrix)))
    velocity, compressed = pl.pallas_call(
        write_out,
        out_shape=(
            jax.ShapeDtypeStruct(velocity.shape, jnp.float32),
            jax.ShapeDtypeStruct(compressed.shape, jnp.float32),
        ),
        in_specs=[vmem, vmem],
        out_specs=[pl.BlockSpec(memory_space=pltpu.HBM)] * 2,
        scratch_shapes=[pltpu.SemaphoreType.DMA((2,))],
        compiler_params=pltpu.CompilerParams(vmem_limit_bytes=4000000),
    )(velocity, compressed)
    return velocity, jnp.swapaxes(compressed, 2, 3)


def solution(mesh):
    counts = {axis: mesh.shape[axis] for axis in ("agg", "gx", "gy")}
    placed = (P(None, "gx", "gy", "agg"), P(None, "gx", "gy", "agg"), P("gx", "gy", "agg"))
    return jax.shard_map(
        functools.partial(on_device, counts),
        mesh=mesh,
        in_specs=placed,
        out_specs=(P(None, "gx", "gy", "agg"), P(None, "gy", ("agg", "gx"), None)),
        check_vma=False,
    )
```

```python
import functools
import itertools
import math

import jax
import jax.numpy as jnp
import numpy as np
from jax import lax
from jax.experimental import pallas as pl
from jax.experimental.pallas import tpu as pltpu
from jax.sharding import PartitionSpec as P

SWEEPS = 2
COARSE_SWEEPS = 4
LX = 5
MESH = pl.DeviceIdType.MESH

damping = 0.8
keep = 1.0 - damping
root_half = 0.7071067811865476


def local_levels(cells_x):
    return min(LX, cells_x.bit_length() - 1)


def finish_matrix(cells_x, blocks, rows):
    levels = local_levels(cells_x)
    kept = cells_x // 2
    eye = np.eye(blocks * kept).reshape(blocks, kept, blocks * kept)
    width = cells_x >> levels
    approx = eye[:, :width].reshape(blocks * width, -1)
    details, at = [], width
    for level in range(levels, 1, -1):
        width = cells_x >> level
        details.append(eye[:, at : at + width].reshape(blocks * width, -1))
        at += width
    for level in range(levels, LX):
        low, high = approx[0::2], approx[1::2]
        approx, detail = (low + high) * root_half, (low - high) * root_half
        details.insert(0, detail)
    along_x = np.concatenate([approx] + details, axis=0)
    along_y = np.zeros((rows, rows))
    for row in range(0, rows, 2):
        along_y[row, row : row + 2] = root_half
        along_y[row + 1, row : row + 2] = root_half, -root_half
    return np.einsum("qk,yr->yqkr", along_x, along_y).reshape(-1, blocks * kept * rows).astype(np.float32)


def around():
    axes = ("gx", "gy", "agg")
    found = []
    for number in range(1, 27):
        turn = [(number // 3**i) % 3 for i in range(3)]
        found.append(tuple((axis, way == 1) for axis, way in zip(axes, turn) if way))
    return sorted(found, key=lambda sides: (-len(sides), sides))


far = 1e30


def kernel(
    sizes, v_hbm, f_hbm, r_hbm, m_hbm, vel_ref, comp_ref, v_ext, f_ext, r_ext, m_ref, w_ext, u1_ext, u2_ext,
    y_send, y_recv, xy_send, xy_recv, z_send, z_recv, yz_send, yz_recv, xz_send, xz_recv, corner_recv,
    q_ext, h_ext, zs_coarse, c_send, c_recv, measure, band_ref, pairs_ref,
    a_send_sem, a_recv_sem, q_send_sem, q_recv_sem, c_send_sem, c_recv_sem, in_sem,
):
    counts = sizes
    C, X, Y, Z = vel_ref.shape
    me = {axis: lax.axis_index(axis) for axis in counts}
    blocks = counts["gx"]
    chunk = Z // blocks
    rows_ext = Y + 8
    f32 = jnp.float32

    loads = [
        pltpu.make_async_copy(src, dst, in_sem.at[i])
        for i, (src, dst) in enumerate((
            (v_hbm, v_ext.at[:, 3 : 3 + X, :Y]),
            (f_hbm, f_ext.at[:, 2 : 2 + X, :Y]),
            (r_hbm, r_ext.at[2 : 2 + X, :Y]),
            (m_hbm, m_ref),
        ))
    ]
    for load in loads:
        load.start()

    def exists(axis, high):
        return me[axis] < counts[axis] - 1 if high else me[axis] > 0

    def all_exist(sides, flip):
        there = None
        for axis, high in sides:
            one = exists(axis, high != flip)
            there = one if there is None else there & one
        return there

    def beside(*sides):
        return {axis: me[axis] + (1 if high else -1) for axis, high in sides}

    barrier = pltpu.get_barrier_semaphore()
    expected = blocks - 1
    for sides in around():
        if len(sides) > 1 or sides[0][0] != "gx":
            there = all_exist(sides, False)
            expected = expected + there.astype(jnp.int32)

            @pl.when(there)
            def _():
                pl.semaphore_signal(barrier, inc=1, device_id=beside(*sides), device_id_type=MESH)

    for step in range(1, blocks):
        pl.semaphore_signal(
            barrier, inc=1, device_id={"gx": lax.rem(me["gx"] + step, blocks)}, device_id_type=MESH
        )

    lane = lax.broadcasted_iota(jnp.int32, (8, Z), 1)
    row = lax.broadcasted_iota(jnp.int32, (8, Z), 0)
    place = lane % 8
    group = lane // 8
    low_half = (lane < 32) | (lane >= 96)
    near_groups = (group % 8 == 2) | (group % 8 == 3) | (group % 8 == 4) | (group % 8 == 5)

    def fine_messages(sides):
        at = {axis: high for axis, high in sides}
        x, y, z = at.get("gx"), at.get("gy"), at.get("agg")
        from_x, from_y, from_z = 0 if x else 1, 0 if y else 1, 0 if z else 1
        if z is None and y is None:
            made = []
            for ref, depth, fill in ((v_ext, 3, 0.0), (f_ext, 2, 0.0), (r_ext, 2, far)):
                here = pl.ds(X if x else depth, depth)
                there = pl.ds(0 if x else depth + X, depth)
                index = (slice(None),) if ref is not r_ext else ()
                made.append((ref.at[index + (here, pl.ds(0, Y))], ref.at[index + (there, pl.ds(0, Y))], fill))
            return made
        if z is None and x is None:
            return [(y_send.at[int(y)], y_recv.at[from_y], None)]
        if z is None:
            return [(xy_send.at[2 * int(x) + int(y)], xy_recv.at[2 * from_x + from_y], None)]
        if x is None and y is None:
            return [(z_send, z_recv.at[from_z, :, pl.ds(0, Y)], None)]
        if x is None:
            return [(yz_send.at[int(y)], yz_recv.at[from_z, from_y], None)]
        if y is None:
            return [(xz_send, xz_recv.at[from_z, from_x], None)]
        return [(xz_send.at[0, pl.ds(Y - 8 if y else 0, 8)], corner_recv.at[from_z, from_x, from_y], 0.0)]

    def remote(src, dst, send_sem, recv_sem, sides):
        return pltpu.make_async_remote_copy(
            src_ref=src, dst_ref=dst, send_sem=send_sem, recv_sem=recv_sem,
            device_id=beside(*sides), device_id_type=MESH,
        )

    def fine_copies():
        return [
            (sides, remote(src, dst, a_send_sem.at[0], a_recv_sem.at[0], sides))
            for sides in around()
            for src, dst, _ in fine_messages(sides)
        ]

    def rows_of(copies):
        found = {}
        for sides, copy in copies:
            axes = tuple(axis for axis, _ in sides)
            if all(high for _, high in sides):
                found[axes] = found.get(axes, 0) + math.prod(copy.src_ref.shape[:-1])
        return found

    def settle(copies, sem):
        sizes = rows_of(copies)
        neighbours = {
            axis: exists(axis, False).astype(jnp.int32) + exists(axis, True).astype(jnp.int32) for axis in counts
        }
        options = {axis: {1: (0,), 2: (1,)}.get(count, (1, 2)) for axis, count in counts.items()}
        for numbers in itertools.product(*options.values()):
            number = dict(zip(options, numbers))
            rows = sum(size * math.prod(number[axis] for axis in axes) for axes, size in sizes.items())
            there = None
            for axis, value in number.items():
                one = neighbours[axis] == value
                there = one if there is None else there & one
            if rows:
                part = measure.at[pl.ds(0, rows)]
                pl.when(there)(pltpu.make_async_copy(part, part, sem).wait)

    def coarse_message(sides, first=0, fields=C):
        at = {axis: 1 if high else -1 for axis, high in sides}
        block = 1 - at.get("gx", 0)
        here, there = {
            0: (slice(0, Y), slice(0, Y)),
            1: (slice(Y - 8, Y), slice(Y + 8, Y + 16)),
            -1: (slice(0, 8), slice(Y, Y + 8)),
        }[at.get("gy", 0)]
        if "agg" in at:
            return zs_coarse.at[here], h_ext.at[0 if at["agg"] > 0 else 1, block, there]
        which = pl.ds(first, fields)
        return q_ext.at[1, which, here], q_ext.at[block, which, there]

    def coarse_copies():
        return [
            (sides, remote(*coarse_message(sides), q_send_sem.at[0], q_recv_sem.at[0], sides))
            for sides in around()
        ]

    def step_copies():
        return [
            (sides, remote(*coarse_message(sides, C, 1), q_send_sem.at[1], q_recv_sem.at[1], sides))
            for sides in around()
            if "agg" not in dict(sides)
        ]

    far_high = jnp.where(low_half, far, 0.0).astype(f32)
    for sides in around():
        @pl.when(jnp.logical_not(all_exist(sides, True)))
        def _():
            axes = tuple(axis for axis, _ in sides)
            for _, target, fill in fine_messages(sides):
                if fill is not None:
                    target[...] = jnp.full(target.shape, fill, f32)
                elif axes == ("gy",):
                    target[: 5 * C] = jnp.zeros((5 * C, 8, Z), f32)
                    target[5 * C :] = jnp.full((2, 8, Z), far, f32)
                elif axes == ("gx", "gy"):
                    target[0:8] = jnp.zeros((8, Z), f32)
                    target[8:16] = jnp.where(row == 4 * C - 8, far, 0.0)
                elif axes == ("agg",):
                    target[:3] = jnp.zeros((3, Y, Z), f32)
                    for t in range(Y // 8):
                        target[3, t * 8 : t * 8 + 8] = far_high
                elif axes == ("gy", "agg"):
                    target[...] = jnp.where(row >= 6, far_high, 0.0)
                else:
                    target[0] = jnp.zeros((Y, Z), f32)
                    for t in range(Y // 8):
                        target[1, t * 8 : t * 8 + 8] = jnp.where(
                            (group == 0) | (group == 1) | (group == 6) | (group == 7), far, 0.0
                        )
            for target in [coarse_message(sides)[1], coarse_message(sides, C, 1)[1]][: 1 + ("agg" not in axes)]:
                target[...] = jnp.zeros(target.shape, f32)

    tiles_y = Y // 8
    near, ring = range(tiles_y), range(tiles_y + 1)
    tile_of = lambda t: slice(t * 8, t * 8 + 8)
    even_l = lane % 2 == 0
    even_r = row % 2 == 0
    lane_roll = lambda t, shift: pltpu.roll(t, shift % Z, 1) if shift % Z else t
    row_roll = lambda t, shift: pltpu.roll(t, shift % 8, 0)
    v_flat = v_ext.reshape(C * (X + 6) * rows_ext, Z)
    f_flat = f_ext.reshape(C * (X + 4) * rows_ext, Z)
    r_flat = r_ext.reshape((X + 4) * rows_ext, Z)

    def x_line(number, y):
        if number < 3 * C:
            c, ref, extra = number // 3, v_flat, 3
        elif number < 5 * C:
            c, ref, extra = (number - 3 * C) // 2, f_flat, 2
        else:
            c, ref, extra = 0, r_flat, 2
        return ref, pl.ds((c * (X + 2 * extra) + extra) * rows_ext + y, X, stride=rows_ext)

    depth_of = lambda number: number % 3 if number < 3 * C else (number - 3 * C) % 2

    loads[0].wait()
    loads[1].wait()
    loads[2].wait()
    for number in range(5 * C + 2):
        for side in range(2):
            depth = depth_of(number)
            ref, at = x_line(number, Y - 1 - depth if side else depth)
            y_send[side, number] = ref[at, :]
    for high_x in range(2):
        for high_y in range(2):
            xs = [X - 1 - d if high_x else d for d in range(2)]
            ys = [Y - 1 - d if high_y else d for d in range(2)]
            target = xy_send.at[2 * high_x + high_y]
            for c in range(C):
                for i, (x, y) in enumerate(((xs[0], ys[0]), (xs[1], ys[0]), (xs[0], ys[1]))):
                    target[3 * c + i : 3 * c + i + 1] = v_ext[c, 3 + x, y : y + 1]
                target[3 * C + c : 3 * C + c + 1] = f_ext[c, 2 + xs[0], ys[0] : ys[0] + 1]
            target[4 * C : 4 * C + 1] = r_ext[2 + xs[0], ys[0] : ys[0] + 1]
    v_at = lambda c, x, t: v_ext[c, 3 + x, tile_of(t)]
    f_at = lambda c, x, t: f_ext[c, 2 + x, tile_of(t)]
    held = (
        (lambda x, t: v_at(0, x, t), lambda x, t: v_at(1, x, t)),
        (lambda x, t: v_at(2, x, t), None),
        (lambda x, t: f_at(0, x, t), lambda x, t: f_at(1, x, t)),
        (lambda x, t: f_at(2, x, t), lambda x, t: r_ext[2 + x, tile_of(t)]),
    )
    from_ends = jnp.where(place < 4, 3 - place, Z + 3 - place)
    for t in near:
        turned = []
        for pair in held:
            packed = jnp.zeros((8, Z), f32)
            for half, get in enumerate(pair):
                if get is not None:
                    for x in range(X):
                        at = (x + 4 + 8 * half) % 16
                        packed = jnp.where(group == at, jnp.take_along_axis(get(x, t), from_ends, axis=1), packed)
            turned.append(packed)
        for i in range(4):
            z_send[i, tile_of(t)] = turned[i]
            for side in range(2):
                if t == (tiles_y - 1 if side else 0):
                    first = 6 if side else 0
                    yz_send[side, 2 * i : 2 * i + 2] = turned[i][first : first + 2]
        for i in range(2):
            xz_send[i, tile_of(t)] = jnp.where(near_groups, turned[2 * i], lane_roll(turned[2 * i + 1], 32))
    pl.semaphore_wait(barrier, expected)
    for sides, copy in fine_copies():
        pl.when(all_exist(sides, False))(copy.start)

    kept = X // 2
    parts = Y // 8
    combos_per_tile = Z // chunk

    def c_copy(j, source):
        return pltpu.make_async_remote_copy(
            src_ref=c_send.at[j],
            dst_ref=c_recv.at[source],
            send_sem=c_send_sem.at[0],
            recv_sem=c_recv_sem.at[0],
            device_id={"gx": j},
            device_id_type=MESH,
        )

    def settle_parts(sem):
        rows = (blocks - 1) * math.prod(c_send.shape[1:-1])
        if rows:
            part = measure.at[pl.ds(0, rows)]
            pltpu.make_async_copy(part, part, sem).wait()

    def finish_compressed(tiles):
        coefs = blocks * kept
        for tile in tiles:
            gathered = c_recv[:, tile].reshape(coefs * 8, Z)
            done = lax.dot_general(
                m_ref[...], gathered, (((1,), (0,)), ((), ())),
                precision=lax.Precision.HIGHEST, preferred_element_type=jnp.float32,
            )
            for place in range(combos_per_tile):
                c, part = divmod(tile * combos_per_tile + place, parts)
                if c < C:
                    for y in range(8):
                        comp_ref[c, part * 8 + y] = done[
                            y * coefs : (y + 1) * coefs, place * chunk : (place + 1) * chunk
                        ]

    lane_take = lambda t, source: jnp.take_along_axis(t, source, axis=1)
    pair_of = lane + 1 - 2 * (lane % 2)
    lane_swap = lambda t: lane_take(t, pair_of)
    row_swap = lambda t: jnp.where(even_r, row_roll(t, -1), row_roll(t, 1))
    slot_at = lane % 16
    corner_of = ((0, 0), (0, 1), (1, 1), (1, 0))

    def pooled(planes):
        pairs = [[planes[x][t] + planes[x + 1][t] for t in near] for x in range(0, X, 2)]
        out = []
        for t in near:
            t0, t1, t2, t3 = (pair[t] for pair in pairs)
            left = jnp.where(even_r, t0, t3) + row_swap(jnp.where(even_r, t3, t0))
            right = jnp.where(even_r, t1, t2) + row_swap(jnp.where(even_r, t2, t1))
            out.append(jnp.where(even_l, left, right) + lane_swap(jnp.where(even_l, right, left)))
        return out

    from_far = jnp.where(slot_at < 8, 6, Z + 6) - slot_at + 2 * (slot_at % 2)

    def edge_lanes(fields, t):
        packed = jnp.zeros((8, Z), f32)
        for start, field in fields:
            packed = jnp.where((lane >= start) & (lane < start + 16), lane_take(field[t], from_far), packed)
        return packed

    coarse_weight = [
        damping / ((6.0 + 0.5 * total) * 0.25)
        for total in pooled([[r_ext[2 + x, tile_of(t)] for t in near] for x in range(X)])
    ]
    coarse_step = [0.25 * weight for weight in coarse_weight]
    step_edges = [edge_lanes([(64 + 16 * c, coarse_step) for c in range(C)], t) for t in near]
    for t in near:
        q_ext[1, C, tile_of(t)] = coarse_step[t]
        zs_coarse[tile_of(t)] = step_edges[t]
    for x in range(X):
        for t in near:
            w_ext[2 + x, tile_of(t)] = damping / (6.0 + r_ext[2 + x, tile_of(t)])

    source = lax.broadcasted_iota(jnp.int32, (Z, Z), 0)
    target = lax.broadcasted_iota(jnp.int32, (Z, Z), 1)
    apart = jnp.abs(source - target)
    band = jnp.where(apart == 1, 1.0, 0.0).astype(jnp.bfloat16)
    paired = (apart == 2) | ((apart == 1) & (source // 2 == target // 2))
    pairs = jnp.where(paired, 1.0, 0.0).astype(jnp.bfloat16)
    for part in range(3):
        band_ref[part * Z : part * Z + Z] = band
        pairs_ref[part * Z : part * Z + Z] = pairs

    def lane_sums(tiles, matrix):
        stack = jnp.concatenate(tiles, axis=0)
        high = stack.astype(jnp.bfloat16)
        rest = stack - high.astype(f32)
        middle = rest.astype(jnp.bfloat16)
        low = (rest - middle.astype(f32)).astype(jnp.bfloat16)
        done = lax.dot_general(
            jnp.concatenate([high, middle, low], axis=1), matrix[...], (((1,), (0,)), ((), ())),
            preferred_element_type=f32,
        )
        return [done[i * 8 : i * 8 + 8] for i in range(len(tiles))]

    levels = local_levels(X)
    for c in range(C):
        for t in near:
            approx, details = [v_at(c, x, t) for x in range(X)], []
            for level in range(levels):
                low, high = approx[0::2], approx[1::2]
                approx = [(a + b) * root_half for a, b in zip(low, high)]
                if level > 0:
                    details = [(a - b) * root_half for a, b in zip(low, high)] + details
            tile, spot = divmod(c * parts + t, combos_per_tile)
            inside = (lane >= spot * chunk) & (lane < (spot + 1) * chunk)
            for k, values in enumerate(approx + details):
                done = (jnp.where(even_l, values, -values) + lane_swap(values)) * root_half
                for j in range(blocks):
                    moved = lane_roll(done, spot * chunk - j * chunk)
                    if spot:
                        moved = jnp.where(inside, moved, c_send[j, tile, k])
                    c_send[j, tile, k] = moved

    for c in range(C):
        for x in range(X):
            for t in near:
                own = v_at(c, x, t)
                total = f_at(c, x, t) + jnp.where(lane == 0, 0.0, lane_roll(own, 1))
                total = total + jnp.where(lane == Z - 1, 0.0, lane_roll(own, -1))
                for other in range(max(x - 1, 0), min(x + 2, X)):
                    if other != x:
                        total = total + v_at(c, other, t)
                for other, shift, inner in ((t + 1, -1, row < 7), (t - 1, 1, row >= 1)):
                    beyond = row_roll(v_at(c, x, other), shift) if other in near else 0.0
                    total = total + jnp.where(inner, row_roll(own, shift), beyond)
                u1_ext[c, 2 + x, tile_of(t)] = keep * own + w_ext[2 + x, tile_of(t)] * total

    settle(fine_copies(), a_recv_sem.at[0])

    for sides, copy in step_copies():
        pl.when(all_exist(sides, False))(copy.start)
    for j in range(blocks):
        pl.when(me["gx"] != j)(c_copy(j, me["gx"]).start)

    for number in range(5 * C + 2):
        for side in range(2):
            depth = depth_of(number)
            ref, at = x_line(number, Y + depth if side else rows_ext - 1 - depth)
            ref[at, :] = y_recv[side, number]
    for high_x in range(2):
        for high_y in range(2):
            xs = [X + d if high_x else -1 - d for d in range(2)]
            ys = [Y + d if high_y else rows_ext - 1 - d for d in range(2)]
            source = xy_recv.at[2 * high_x + high_y]
            for c in range(C):
                for i, (x, y) in enumerate(((xs[0], ys[0]), (xs[1], ys[0]), (xs[0], ys[1]))):
                    v_ext[c, 3 + x, y : y + 1] = source[3 * c + i : 3 * c + i + 1]
                f_ext[c, 2 + xs[0], ys[0] : ys[0] + 1] = source[3 * C + c : 3 * C + c + 1]
            r_ext[2 + xs[0], ys[0] : ys[0] + 1] = source[4 * C : 4 * C + 1]
    for side in range(2):
        for i in range(4):
            z_recv[side, i, Y : Y + 2] = yz_recv[side, 1, 2 * i : 2 * i + 2]
            z_recv[side, i, Y + 6 : Y + 8] = yz_recv[side, 0, 2 * i : 2 * i + 2]

    def weight_of(reaction):
        return jnp.where(reaction < 0.1 * far, damping / (6.0 + reaction), 0.0)

    for x in range(-2, X + 2):
        outside = max(-x, x - X + 1)
        for t in ring:
            if (outside > 0 and t < tiles_y) or (t == tiles_y and outside < 2):
                w_ext[2 + x, tile_of(t)] = weight_of(r_ext[2 + x, tile_of(t)])

    mixed = {}
    for i in range(4):
        for t in ring:
            mixed[i, t] = jnp.where(place < 4, z_recv[1, i, tile_of(t)], z_recv[0, i, tile_of(t)])
    beyond = {}
    for side in range(2):
        for i in range(2):
            for t in near:
                beyond[side, i, t] = jnp.where(
                    place < 4, xz_recv[1, side, i, tile_of(t)], xz_recv[0, side, i, tile_of(t)]
                )
        ends = [
            jnp.where(place < 4, corner_recv[1, side, high], corner_recv[0, side, high]) for high in range(2)
        ]
        beyond[side, 0, tiles_y] = jnp.where(row < 4, ends[1], ends[0])

    def edge_field(number, t):
        i, half = divmod(number, 2)
        value = lane_roll(mixed[i, t], 64 * half)
        if t < tiles_y or number < 4:
            shift = (64, 0, 32, -32)[number % 4]
            low, high = (lane_roll(beyond[side, i // 2, t], shift) for side in range(2))
            value = jnp.where(group < 4, low, jnp.where(group >= 12, high, value))
        return value

    edge_v = {(c, t): edge_field(c, t) for c in range(C) for t in ring}
    edge_f = {(c, t): edge_field(4 + c, t) for c in range(C) for t in ring}
    edge_w = {t: weight_of(edge_field(7, t)) for t in ring}

    def around_rows(get, t, tiles, by):
        after, before = (t + 1) % tiles, (t - 1) % tiles
        own = get(t)
        above = jnp.where(row < 8 - by, row_roll(own, -by), row_roll(get(after), -by))
        below = jnp.where(row >= by, row_roll(own, by), row_roll(get(before), by))
        return below, above

    def rows_beside(at, t):
        get = lambda t: at(tile_of(t))
        if t < tiles_y:
            above = at(pl.ds(t * 8 + 1, 8))
        else:
            above = jnp.where(row < 7, row_roll(get(t), -1), row_roll(get(0), -1))
        if t > 0:
            below = at(pl.ds(t * 8 - 1, 8))
        else:
            below = jnp.where(row >= 1, row_roll(get(t), 1), row_roll(get(tiles_y), 1))
        return below, above

    def main_total(get, edge, c, x, t, along_z=None):
        below, above = rows_beside(lambda rows: get(c, x, rows), t)
        get = lambda c, x, t, get=get: get(c, x, tile_of(t))
        total = (get(c, x - 1, t) + get(c, x + 1, t)) + (below + above)
        beside_z = lane_roll(edge[c, t], -(8 * (x + 4) + 4))
        if along_z is not None:
            return total + (along_z + jnp.where((lane == 0) | (lane == Z - 1), beside_z, 0.0))
        own = get(c, x, t)
        total = total + jnp.where(lane == 0, beside_z, lane_roll(own, 1))
        return total + jnp.where(lane == Z - 1, beside_z, lane_roll(own, -1))

    def edge_total(get, edge, c, xs, t):
        own = edge[c, t]
        line = own
        for x in xs:
            line = jnp.where(group == x + 4, lane_roll(get(c, x, t), 8 * (x + 4) + 4), line)
        below, above = around_rows(lambda t: edge[c, t], t, tiles_y + 1, 1)
        total = (lane_roll(own, 8) + lane_roll(own, -8)) + (below + above)
        total = total + jnp.where(place == 4, line, lane_roll(own, 1))
        return total + jnp.where(place == 3, line, lane_roll(own, -1))

    u1_at = lambda c, x, t: u1_ext[c, 2 + x, tile_of(t)]
    u2_at = lambda c, x, t: u2_ext[c, 1 + x, tile_of(t)]
    v_rows = lambda c, x, rows: v_ext[c, 3 + x, rows]
    u1_rows = lambda c, x, rows: u1_ext[c, 2 + x, rows]
    u2_rows = lambda c, x, rows: u2_ext[c, 1 + x, rows]
    w_at = lambda x, t: w_ext[2 + x, tile_of(t)]

    edge_1, edge_2 = {}, {}
    for c in range(C):
        for t in ring:
            total = edge_total(v_at, edge_v, c, range(-1, X + 1), t)
            edge_1[c, t] = keep * edge_v[c, t] + edge_w[t] * (edge_f[c, t] + total)
        chosen = [
            (x, t)
            for x in range(-2, X + 2)
            for t in (near if x in (-2, X + 1) else [tiles_y] if 0 <= x < X else ring)
        ]
        along_z = dict(zip(chosen, lane_sums([v_at(c, x, t) for x, t in chosen], band_ref)))
        for x in range(-2, X + 2):
            if 0 <= x < X:
                for t in near:
                    beside_z = lane_roll(edge_v[c, t], -(8 * (x + 4) + 4))
                    total = jnp.where((lane == 0) | (lane == Z - 1), beside_z, 0.0)
                    if t == 0:
                        total = total + jnp.where(row == 0, row_roll(v_at(c, x, tiles_y), 1), 0.0)
                    if t == tiles_y - 1:
                        total = total + jnp.where(row == 7, row_roll(v_at(c, x, tiles_y), -1), 0.0)
                    if x in (0, X - 1):
                        total = total + v_at(c, -1 if x == 0 else X, t)
                    u1_ext[c, 2 + x, tile_of(t)] = u1_at(c, x, t) + w_at(x, t) * total
            for t in near if x in (-2, X + 1) else [tiles_y] if 0 <= x < X else ring:
                total = main_total(v_rows, edge_v, c, x, t, along_z[x, t])
                u1_ext[c, 2 + x, tile_of(t)] = keep * v_at(c, x, t) + w_at(x, t) * (f_at(c, x, t) + total)
    for c in range(C):
        for t in near:
            total = edge_total(u1_at, edge_1, c, range(X), t)
            edge_2[c, t] = keep * edge_1[c, t] + edge_w[t] * (edge_f[c, t] + total)
        chosen = [(x, t) for x in range(-1, X + 1) for t in (near if x in (-1, X) else ring)]
        along_z = dict(zip(chosen, lane_sums([u1_at(c, x, t) for x, t in chosen], band_ref)))
        for x in range(-1, X + 1):
            for t in near if x in (-1, X) else ring:
                total = main_total(u1_rows, edge_1, c, x, t, along_z[x, t])
                u2_ext[c, 1 + x, tile_of(t)] = keep * u1_at(c, x, t) + w_at(x, t) * (f_at(c, x, t) + total)
    sums = []
    for c in range(C):
        chosen = [(x, t) for x in range(X) for t in near]
        along_z = dict(zip(chosen, lane_sums([u2_at(c, x, t) for x, t in chosen], band_ref)))
        sums.append([
            [main_total(u2_rows, edge_2, c, x, t, along_z[x, t]) + f_at(c, x, t) for t in near] for x in range(X)
        ])

    correction = []
    for c in range(C):
        rhs = pooled([
            [sums[c][x][t] - (6.0 + r_ext[2 + x, tile_of(t)]) * u2_at(c, x, t) for t in near] for x in range(X)
        ])
        correction.append([weight * (0.125 * total) for weight, total in zip(coarse_weight, rhs)])
    for c in range(C):
        for t in near:
            q_ext[1, c, tile_of(t)] = correction[c][t]
    for t in near:
        edges_t = edge_lanes([(16 * c, correction[c]) for c in range(C)], t)
        zs_coarse[tile_of(t)] = jnp.where(lane < 64, edges_t, zs_coarse[tile_of(t)])
    for sides, copy in coarse_copies():
        pl.when(all_exist(sides, False))(copy.start)

    for j in range(blocks):
        @pl.when(me["gx"] == j)
        def _():
            c_recv[j] = c_send[j]

    settle_parts(c_recv_sem.at[0])
    loads[3].wait()
    finish_compressed(range(c_send.shape[1]))

    settle(step_copies(), q_recv_sem.at[1])
    settle(coarse_copies(), q_recv_sem.at[0])

    ring = range(tiles_y + 2)
    after = lambda t: (t + 1) % len(ring)
    before = lambda t: (t - 1) % len(ring)
    main = {(b, c, t): q_ext[b, c, tile_of(t)] for b in range(3) for c in range(C) for t in ring}
    step_main = {(b, t): q_ext[b, C, tile_of(t)] for b in range(3) for t in ring}
    edge = {
        (b, t): jnp.where(slot_at < 8, h_ext[1, b, tile_of(t)], h_ext[0, b, tile_of(t)])
        for b in range(3) for t in ring
    }
    step_edge = {key: lane_roll(value, -64) for key, value in edge.items()}
    first_main, first_edge = dict(main), dict(edge)

    def above(get, t):
        return jnp.where(row < 6, row_roll(get(t), -2), row_roll(get(after(t)), -2))

    def below(get, t):
        return jnp.where(row >= 2, row_roll(get(t), 2), row_roll(get(before(t)), 2))

    def along(get, b, t):
        low, high = get(max(b - 1, 0), t), get(min(b + 1, 2), t)
        across = jnp.where(even_l, jnp.where(even_r, high, low), get(b, t))
        return row_swap(across)

    def inject(edge, b, c, t):
        return lane_roll(edge[b, t], -(16 * c + 8))

    def left_of(main, edge, b, c, t):
        return jnp.where(lane < 2, inject(edge, b, c, t), lane_roll(main[b, c, t], 2))

    def right_of(main, edge, b, c, t):
        return jnp.where(lane >= Z - 2, inject(edge, b, c, t), lane_roll(main[b, c, t], -2))

    def coarse_sweep(main, edge, main_at, edge_at):
        new_main, new_edge = dict(main), dict(edge)
        for c in range(C):
            lanes = dict(zip(main_at, lane_sums([main[b, c, t] for b, t in main_at], pairs_ref)))
            for b, t in main_at:
                get = lambda b, t, c=c: main[b, c, t]
                row_get = lambda t, b=b, c=c: main[b, c, t]
                total = along(get, b, t) + (above(row_get, t) + below(row_get, t))
                ends = jnp.where((lane < 2) | (lane >= Z - 2), inject(edge, b, c, t), 0.0)
                total = total + (lanes[b, t] + ends)
                new_main[b, c, t] = keep * main[b, c, t] + first_main[b, c, t] + step_main[b, t] * total
        for b, t in edge_at:
            get = lambda b, t: edge[b, t]
            row_get = lambda t, b=b: edge[b, t]
            own = lane_roll(main[b, 0, t], 8)
            for c in range(1, C):
                own = jnp.where(lane < 16 * c, own, lane_roll(main[b, c, t], 16 * c + 8))
            total = along(get, b, t) + lane_swap(edge[b, t]) + (above(row_get, t) + below(row_get, t))
            total = total + jnp.where((slot_at == 8) | (slot_at == 9), own, lane_roll(edge[b, t], 2))
            total = total + jnp.where((slot_at == 6) | (slot_at == 7), own, lane_roll(edge[b, t], -2))
            new_edge[b, t] = keep * edge[b, t] + first_edge[b, t] + step_edge[b, t] * total
        return new_main, new_edge

    everywhere = [(b, t) for b in range(3) for t in ring]
    centre = [(1, t) for t in ring]
    sides_near = [(b, t) for b in (0, 2) for t in near]
    main, edge = coarse_sweep(main, edge, everywhere, everywhere)
    main, edge = coarse_sweep(main, edge, everywhere, centre + sides_near)
    main, edge = coarse_sweep(main, edge, centre + sides_near, [(1, t) for t in near])

    def spread_rows(even, odd, pa):
        if pa == 0:
            return jnp.where(even_r, even, row_roll(odd, 1))
        return jnp.where(even_r, row_roll(even, -1), odd)

    def spread_lanes(even, odd, pb):
        if pb == 0:
            return jnp.where(even_l, even, lane_roll(odd, 1))
        return jnp.where(even_l, lane_roll(even, -1), odd)

    for c in range(C):
        for t in near:
            at = tile_of(t)
            row_get = lambda t, c=c: main[1, c, t]
            own = main[1, c, t]
            rows_near = (below(row_get, t), above(row_get, t))
            lanes_near = (left_of(main, edge, 1, c, t), right_of(main, edge, 1, c, t))
            alone = [spread_lanes(own, own, pb) for pb in range(2)]
            spread = [spread_rows(alone[pb], alone[pb], pa) for pa, pb in corner_of]
            low, high = (spread_lanes(main[b, c, t], main[b, c, t], 0) for b in (0, 2))
            spread = [spread_rows(low, low, 1)] + spread + [spread_rows(high, high, 0)]
            based = [3.0 * own + rows_near[a] for a in range(2)]
            wide = [
                [spread_lanes(based[a] + lanes_near[0], based[a] + lanes_near[1], pb) for pb in range(2)]
                for a in range(2)
            ]
            for x in range(X):
                p = x // 2
                pa, pb = corner_of[p]
                added = spread_rows(wide[0][pb], wide[1][pb], pa) + spread[p + 2 * (x % 2)]
                total = sums[c][x][t] + added
                vel_ref[c, x, at] = keep * (u2_at(c, x, t) + spread[p + 1]) + w_at(x, t) * total

    settle(fine_copies(), a_send_sem.at[0])
    settle(step_copies(), q_send_sem.at[1])
    settle(coarse_copies(), q_send_sem.at[0])
    settle_parts(c_send_sem.at[0])


def write_out(vel_ref, comp_ref, vel_hbm, comp_hbm, sem):
    copies = [
        pltpu.make_async_copy(comp_ref, comp_hbm, sem.at[0]),
        pltpu.make_async_copy(vel_ref, vel_hbm, sem.at[1]),
    ]
    for copy in copies:
        copy.start()
    for copy in copies:
        copy.wait()


def on_device(counts, velocity_prev, forcing, reaction):
    C, X, Y, Z = velocity_prev.shape
    blocks = counts["gx"]
    kept = X // 2
    chunk = Z // blocks
    tiles = -(-(C * (Y // 8)) // (Z // chunk))
    matrix = jnp.asarray(finish_matrix(X, blocks, 8))
    vmem = pl.BlockSpec(memory_space=pltpu.VMEM)
    space = lambda *shape: pltpu.VMEM(shape, jnp.float32)

    velocity, compressed = pl.pallas_call(
        functools.partial(kernel, counts),
        out_shape=(
            jax.ShapeDtypeStruct((C, X, Y, Z), jnp.float32),
            jax.ShapeDtypeStruct((C, Y, kept * blocks, chunk), jnp.float32),
        ),
        in_specs=[pl.BlockSpec(memory_space=pltpu.HBM)] * 4,
        out_specs=(vmem, vmem),
        scratch_shapes=[
            space(C, X + 6, Y + 8, Z),
            space(C, X + 4, Y + 8, Z),
            space(X + 4, Y + 8, Z),
            space(*matrix.shape),
            space(X + 4, Y + 8, Z),
            space(C, X + 4, Y + 8, Z),
            space(C, X + 2, Y + 8, Z),
            space(2, 5 * C + 2, X, Z),
            space(2, 5 * C + 2, X, Z),
            space(4, 16, Z),
            space(4, 16, Z),
            space(4, Y, Z),
            space(2, 4, Y + 8, Z),
            space(2, 8, Z),
            space(2, 2, 8, Z),
            space(2, Y, Z),
            space(2, 2, 2, Y, Z),
            space(2, 2, 2, 8, Z),
            space(3, C + 1, Y + 16, Z),
            space(2, 3, Y + 16, Z),
            space(Y, Z),
            space(blocks, tiles, kept, 8, Z),
            space(blocks, tiles, kept, 8, Z),
            space(max((blocks - 1) * tiles * kept * 8, 128 * Y), Z),
            pltpu.VMEM((3 * Z, Z), jnp.bfloat16),
            pltpu.VMEM((3 * Z, Z), jnp.bfloat16),
            pltpu.SemaphoreType.DMA((1,)),
            pltpu.SemaphoreType.DMA((1,)),
            pltpu.SemaphoreType.DMA((2,)),
            pltpu.SemaphoreType.DMA((2,)),
            pltpu.SemaphoreType.DMA((1,)),
            pltpu.SemaphoreType.DMA((1,)),
            pltpu.SemaphoreType.DMA((4,)),
        ],
        compiler_params=pltpu.CompilerParams(collective_id=0, has_side_effects=True, vmem_limit_bytes=40000000),
    )(*(pltpu.with_memory_space_constraint(a, pltpu.HBM) for a in (velocity_prev, forcing, reaction, matrix)))
    velocity, compressed = pl.pallas_call(
        write_out,
        out_shape=(
            jax.ShapeDtypeStruct(velocity.shape, jnp.float32),
            jax.ShapeDtypeStruct(compressed.shape, jnp.float32),
        ),
        in_specs=[vmem, vmem],
        out_specs=[pl.BlockSpec(memory_space=pltpu.HBM)] * 2,
        scratch_shapes=[pltpu.SemaphoreType.DMA((2,))],
        compiler_params=pltpu.CompilerParams(vmem_limit_bytes=4000000),
    )(velocity, compressed)
    return velocity, jnp.swapaxes(compressed, 2, 3)


def solution(mesh):
    counts = {axis: mesh.shape[axis] for axis in ("agg", "gx", "gy")}
    placed = (P(None, "gx", "gy", "agg"), P(None, "gx", "gy", "agg"), P("gx", "gy", "agg"))
    return jax.shard_map(
        functools.partial(on_device, counts),
        mesh=mesh,
        in_specs=placed,
        out_specs=(P(None, "gx", "gy", "agg"), P(None, "gy", ("agg", "gx"), None)),
        check_vma=False,
    )
```

```python
import functools
import itertools
import math

import jax
import jax.numpy as jnp
import numpy as np
from jax import lax
from jax.experimental import pallas as pl
from jax.experimental.pallas import tpu as pltpu
from jax.sharding import PartitionSpec as P

SWEEPS = 2
COARSE_SWEEPS = 4
LX = 5
MESH = pl.DeviceIdType.MESH

damping = 0.8
keep = 1.0 - damping
root_half = 0.7071067811865476


def local_levels(cells_x):
    return min(LX, cells_x.bit_length() - 1)


def finish_matrix(cells_x, blocks, rows):
    levels = local_levels(cells_x)
    kept = cells_x // 2
    eye = np.eye(blocks * kept).reshape(blocks, kept, blocks * kept)
    width = cells_x >> levels
    approx = eye[:, :width].reshape(blocks * width, -1)
    details, at = [], width
    for level in range(levels, 1, -1):
        width = cells_x >> level
        details.append(eye[:, at : at + width].reshape(blocks * width, -1))
        at += width
    for level in range(levels, LX):
        low, high = approx[0::2], approx[1::2]
        approx, detail = (low + high) * root_half, (low - high) * root_half
        details.insert(0, detail)
    along_x = np.concatenate([approx] + details, axis=0)
    along_y = np.zeros((rows, rows))
    for row in range(0, rows, 2):
        along_y[row, row : row + 2] = root_half
        along_y[row + 1, row : row + 2] = root_half, -root_half
    return np.einsum("qk,yr->yqkr", along_x, along_y).reshape(-1, blocks * kept * rows).astype(np.float32)


def around():
    axes = ("gx", "gy", "agg")
    found = []
    for number in range(1, 27):
        turn = [(number // 3**i) % 3 for i in range(3)]
        found.append(tuple((axis, way == 1) for axis, way in zip(axes, turn) if way))
    return sorted(found, key=lambda sides: (-len(sides), sides))


def lane_sums(tiles, matrix):
    stack = jnp.concatenate(tiles, axis=0)
    high = stack.astype(jnp.bfloat16)
    rest = stack - high.astype(jnp.float32)
    middle = rest.astype(jnp.bfloat16)
    low = (rest - middle.astype(jnp.float32)).astype(jnp.bfloat16)
    done = lax.dot_general(
        jnp.concatenate([high, middle, low], axis=1), matrix[...], (((1,), (0,)), ((), ())),
        preferred_element_type=jnp.float32,
    )
    return [done[i * 8 : i * 8 + 8] for i in range(len(tiles))]


far = 1e30


def kernel(
    sizes, v_hbm, f_hbm, r_hbm, m_hbm, comp_ref, base_ref, w_ext, q_ext, h_ext, pairs_ref,
    v_ext, f_ext, r_ext, m_ref, u1_ext, u2_ext,
    y_send, y_recv, xy_send, xy_recv, z_send, z_recv, yz_send, yz_recv, xz_send, xz_recv, corner_recv,
    zs_coarse, c_send, c_recv, measure, band_ref,
    a_send_sem, a_recv_sem, q_send_sem, q_recv_sem, c_send_sem, c_recv_sem, in_sem,
):
    counts = sizes
    C, X, Y, Z = base_ref.shape
    me = {axis: lax.axis_index(axis) for axis in counts}
    blocks = counts["gx"]
    chunk = Z // blocks
    rows_ext = Y + 8
    f32 = jnp.float32

    loads = [
        pltpu.make_async_copy(src, dst, in_sem.at[i])
        for i, (src, dst) in enumerate((
            (v_hbm, v_ext.at[:, 3 : 3 + X, :Y]),
            (f_hbm, f_ext.at[:, 2 : 2 + X, :Y]),
            (r_hbm, r_ext.at[2 : 2 + X, :Y]),
            (m_hbm, m_ref),
        ))
    ]
    for load in loads:
        load.start()

    def exists(axis, high):
        return me[axis] < counts[axis] - 1 if high else me[axis] > 0

    def all_exist(sides, flip):
        there = None
        for axis, high in sides:
            one = exists(axis, high != flip)
            there = one if there is None else there & one
        return there

    def beside(*sides):
        return {axis: me[axis] + (1 if high else -1) for axis, high in sides}

    barrier = pltpu.get_barrier_semaphore()
    expected = blocks - 1
    for sides in around():
        if len(sides) > 1 or sides[0][0] != "gx":
            there = all_exist(sides, False)
            expected = expected + there.astype(jnp.int32)

            @pl.when(there)
            def _():
                pl.semaphore_signal(barrier, inc=1, device_id=beside(*sides), device_id_type=MESH)

    for step in range(1, blocks):
        pl.semaphore_signal(
            barrier, inc=1, device_id={"gx": lax.rem(me["gx"] + step, blocks)}, device_id_type=MESH
        )

    lane = lax.broadcasted_iota(jnp.int32, (8, Z), 1)
    row = lax.broadcasted_iota(jnp.int32, (8, Z), 0)
    place = lane % 8
    group = lane // 8
    low_half = (lane < 32) | (lane >= 96)

    def fine_messages(sides):
        at = {axis: high for axis, high in sides}
        x, y, z = at.get("gx"), at.get("gy"), at.get("agg")
        from_x, from_y, from_z = 0 if x else 1, 0 if y else 1, 0 if z else 1
        if z is None and y is None:
            made = []
            for ref, depth, fill in ((v_ext, 3, 0.0), (f_ext, 2, 0.0), (r_ext, 2, far)):
                here = pl.ds(X if x else depth, depth)
                there = pl.ds(0 if x else depth + X, depth)
                index = (slice(None),) if ref is not r_ext else ()
                made.append((ref.at[index + (here, pl.ds(0, Y))], ref.at[index + (there, pl.ds(0, Y))], fill))
            return made
        if z is None and x is None:
            return [(y_send.at[int(y)], y_recv.at[from_y], None)]
        if z is None:
            return [(xy_send.at[2 * int(x) + int(y)], xy_recv.at[2 * from_x + from_y], None)]
        if x is None and y is None:
            return [(z_send, z_recv.at[from_z, :, pl.ds(0, Y)], None)]
        if x is None:
            return [(yz_send.at[int(y)], yz_recv.at[from_z, from_y], None)]
        if y is None:
            return [(xz_send, xz_recv.at[from_z, from_x], None)]
        return [(xz_send.at[0, pl.ds(Y - 8 if y else 0, 8)], corner_recv.at[from_z, from_x, from_y], 0.0)]

    def remote(src, dst, send_sem, recv_sem, sides):
        return pltpu.make_async_remote_copy(
            src_ref=src, dst_ref=dst, send_sem=send_sem, recv_sem=recv_sem,
            device_id=beside(*sides), device_id_type=MESH,
        )

    def fine_copies():
        return [
            (sides, remote(src, dst, a_send_sem.at[0], a_recv_sem.at[0], sides))
            for sides in around()
            for src, dst, _ in fine_messages(sides)
        ]

    def rows_of(copies):
        found = {}
        for sides, copy in copies:
            axes = tuple(axis for axis, _ in sides)
            if all(high for _, high in sides):
                found[axes] = found.get(axes, 0) + math.prod(copy.src_ref.shape[:-1])
        return found

    def settle(copies, sem):
        sizes = rows_of(copies)
        neighbours = {
            axis: exists(axis, False).astype(jnp.int32) + exists(axis, True).astype(jnp.int32) for axis in counts
        }
        options = {axis: {1: (0,), 2: (1,)}.get(count, (1, 2)) for axis, count in counts.items()}
        for numbers in itertools.product(*options.values()):
            number = dict(zip(options, numbers))
            rows = sum(size * math.prod(number[axis] for axis in axes) for axes, size in sizes.items())
            there = None
            for axis, value in number.items():
                one = neighbours[axis] == value
                there = one if there is None else there & one
            if rows:
                part = measure.at[pl.ds(0, rows)]
                pl.when(there)(pltpu.make_async_copy(part, part, sem).wait)

    def coarse_message(sides, first=0, fields=C):
        at = {axis: 1 if high else -1 for axis, high in sides}
        block = 1 - at.get("gx", 0)
        here, there = {
            0: (slice(0, Y), slice(0, Y)),
            1: (slice(Y - 8, Y), slice(Y + 8, Y + 16)),
            -1: (slice(0, 8), slice(Y, Y + 8)),
        }[at.get("gy", 0)]
        if "agg" in at:
            return zs_coarse.at[here], h_ext.at[0 if at["agg"] > 0 else 1, block, there]
        which = pl.ds(first, fields)
        return q_ext.at[1, which, here], q_ext.at[block, which, there]

    def coarse_copies():
        return [
            (sides, remote(*coarse_message(sides), q_send_sem.at[0], q_recv_sem.at[0], sides))
            for sides in around()
        ]

    def step_copies():
        return [
            (sides, remote(*coarse_message(sides, C, 1), q_send_sem.at[1], q_recv_sem.at[1], sides))
            for sides in around()
            if "agg" not in dict(sides)
        ]

    far_high = jnp.where(low_half, far, 0.0).astype(f32)
    for sides in around():
        @pl.when(jnp.logical_not(all_exist(sides, True)))
        def _():
            axes = tuple(axis for axis, _ in sides)
            for _, target, fill in fine_messages(sides):
                if fill is not None:
                    target[...] = jnp.full(target.shape, fill, f32)
                elif axes == ("gy",):
                    target[: 5 * C] = jnp.zeros((5 * C, 8, Z), f32)
                    target[5 * C :] = jnp.full((2, 8, Z), far, f32)
                elif axes == ("gx", "gy"):
                    target[0:8] = jnp.zeros((8, Z), f32)
                    target[8:16] = jnp.where(row == 4 * C - 8, far, 0.0)
                elif axes == ("agg",):
                    target[:3] = jnp.zeros((3, Y, Z), f32)
                    for t in range(Y // 8):
                        target[3, t * 8 : t * 8 + 8] = far_high
                elif axes == ("gy", "agg"):
                    target[...] = jnp.where(row >= 6, far_high, 0.0)
                else:
                    target[0] = jnp.zeros((Y, Z), f32)
                    for t in range(Y // 8):
                        target[1, t * 8 : t * 8 + 8] = jnp.where(
                            (group == 0) | (group == 1) | (group == 6) | (group == 7), far, 0.0
                        )
            for target in [coarse_message(sides)[1], coarse_message(sides, C, 1)[1]][: 1 + ("agg" not in axes)]:
                target[...] = jnp.zeros(target.shape, f32)

    tiles_y = Y // 8
    near, ring = range(tiles_y), range(tiles_y + 1)
    tile_of = lambda t: slice(t * 8, t * 8 + 8)
    even_l = lane % 2 == 0
    even_r = row % 2 == 0
    lane_roll = lambda t, shift: pltpu.roll(t, shift % Z, 1) if shift % Z else t
    row_roll = lambda t, shift: pltpu.roll(t, shift % 8, 0)
    lane_take = lambda t, source: jnp.take_along_axis(t, source, axis=1)
    v_flat = v_ext.reshape(C * (X + 6) * rows_ext, Z)
    f_flat = f_ext.reshape(C * (X + 4) * rows_ext, Z)
    r_flat = r_ext.reshape((X + 4) * rows_ext, Z)

    def x_line(number, y):
        if number < 3 * C:
            c, ref, extra = number // 3, v_flat, 3
        elif number < 5 * C:
            c, ref, extra = (number - 3 * C) // 2, f_flat, 2
        else:
            c, ref, extra = 0, r_flat, 2
        return ref, pl.ds((c * (X + 2 * extra) + extra) * rows_ext + y, X, stride=rows_ext)

    depth_of = lambda number: number % 3 if number < 3 * C else (number - 3 * C) % 2

    loads[0].wait()
    loads[1].wait()
    loads[2].wait()
    for number in range(5 * C + 2):
        for side in range(2):
            depth = depth_of(number)
            ref, at = x_line(number, Y - 1 - depth if side else depth)
            y_send[side, number] = ref[at, :]
    for high_x in range(2):
        for high_y in range(2):
            xs = [X - 1 - d if high_x else d for d in range(2)]
            ys = [Y - 1 - d if high_y else d for d in range(2)]
            target = xy_send.at[2 * high_x + high_y]
            for c in range(C):
                for i, (x, y) in enumerate(((xs[0], ys[0]), (xs[1], ys[0]), (xs[0], ys[1]))):
                    target[3 * c + i : 3 * c + i + 1] = v_ext[c, 3 + x, y : y + 1]
                target[3 * C + c : 3 * C + c + 1] = f_ext[c, 2 + xs[0], ys[0] : ys[0] + 1]
            target[4 * C : 4 * C + 1] = r_ext[2 + xs[0], ys[0] : ys[0] + 1]
    v_at = lambda c, x, t: v_ext[c, 3 + x, tile_of(t)]
    f_at = lambda c, x, t: f_ext[c, 2 + x, tile_of(t)]
    held = (
        (lambda x, t: v_at(0, x, t), lambda x, t: v_at(1, x, t)),
        (lambda x, t: v_at(2, x, t), None),
        (lambda x, t: f_at(0, x, t), lambda x, t: f_at(1, x, t)),
        (lambda x, t: f_at(2, x, t), lambda x, t: r_ext[2 + x, tile_of(t)]),
    )
    from_ends = jnp.where(place < 4, 3 - place, Z + 3 - place)
    for t in near:
        turned, crossed = [], []
        for i, pair in enumerate(held):
            packed = jnp.zeros((8, Z), f32)
            across = jnp.zeros((8, Z), f32) if i % 2 == 0 else crossed.pop()
            for half, get in enumerate(pair):
                if get is not None:
                    for x in range(X):
                        ends = lane_take(get(x, t), from_ends)
                        packed = jnp.where(group == (x + 4 + 8 * half) % 16, ends, packed)
                        if x < 2 or x >= X - 2:
                            across = jnp.where(group == (x + 4 + 8 * half + 4 * (i % 2)) % 16, ends, across)
            turned.append(packed)
            crossed.append(across)
        for i in range(4):
            z_send[i, tile_of(t)] = turned[i]
            for side in range(2):
                if t == (tiles_y - 1 if side else 0):
                    first = 6 if side else 0
                    yz_send[side, 2 * i : 2 * i + 2] = turned[i][first : first + 2]
        for i in range(2):
            xz_send[i, tile_of(t)] = crossed[i]
    pl.semaphore_wait(barrier, expected)
    for sides, copy in fine_copies():
        pl.when(all_exist(sides, False))(copy.start)

    kept = X // 2
    parts = Y // 8
    combos_per_tile = Z // chunk

    def c_copy(j, source):
        return pltpu.make_async_remote_copy(
            src_ref=c_send.at[j],
            dst_ref=c_recv.at[source],
            send_sem=c_send_sem.at[0],
            recv_sem=c_recv_sem.at[0],
            device_id={"gx": j},
            device_id_type=MESH,
        )

    def settle_parts(sem):
        rows = (blocks - 1) * math.prod(c_send.shape[1:-1])
        if rows:
            part = measure.at[pl.ds(0, rows)]
            pltpu.make_async_copy(part, part, sem).wait()

    def finish_compressed(tiles):
        coefs = blocks * kept
        for tile in tiles:
            gathered = c_recv[:, tile].reshape(coefs * 8, Z)
            done = lax.dot_general(
                m_ref[...], gathered, (((1,), (0,)), ((), ())),
                precision=lax.Precision.HIGHEST, preferred_element_type=jnp.float32,
            )
            for place in range(combos_per_tile):
                c, part = divmod(tile * combos_per_tile + place, parts)
                if c < C:
                    for y in range(8):
                        comp_ref[c, part * 8 + y] = done[
                            y * coefs : (y + 1) * coefs, place * chunk : (place + 1) * chunk
                        ]

    pair_of = lane + 1 - 2 * (lane % 2)
    lane_swap = lambda t: lane_take(t, pair_of)
    row_swap = lambda t: jnp.where(even_r, row_roll(t, -1), row_roll(t, 1))
    slot_at = lane % 16
    corner_of = ((0, 0), (0, 1), (1, 1), (1, 0))

    def pooled_halves(planes):
        pairs = [[planes[x][t] + planes[x + 1][t] for t in near] for x in range(0, X, 2)]
        out = []
        for t in near:
            t0, t1, t2, t3 = (pair[t] for pair in pairs)
            left = jnp.where(even_r, t0, t3) + row_swap(jnp.where(even_r, t3, t0))
            right = jnp.where(even_r, t1, t2) + row_swap(jnp.where(even_r, t2, t1))
            out.append((jnp.where(even_l, left, right), jnp.where(even_l, right, left)))
        return out

    def pooled(planes):
        return [own + lane_swap(other) for own, other in pooled_halves(planes)]

    from_far = jnp.where(slot_at < 8, 6, Z + 6) - slot_at + 2 * (slot_at % 2)

    from_far_pair = from_far + 1 - 2 * (from_far % 2)

    def edge_lanes(fields, t):
        packed = jnp.zeros((8, Z), f32)
        for start, field in fields:
            packed = jnp.where((lane >= start) & (lane < start + 16), lane_take(field[t], from_far), packed)
        return packed

    coarse_weight = [
        damping / ((6.0 + 0.5 * total) * 0.25)
        for total in pooled([[r_ext[2 + x, tile_of(t)] for t in near] for x in range(X)])
    ]
    coarse_step = [0.25 * weight for weight in coarse_weight]
    step_edges = [edge_lanes([(64 + 16 * c, coarse_step) for c in range(C)], t) for t in near]
    weight_edges = [edge_lanes([(16 * c, coarse_weight) for c in range(C)], t) for t in near]
    for t in near:
        q_ext[1, C, tile_of(t)] = coarse_step[t]
    for x in range(X):
        for t in near:
            w_ext[2 + x, tile_of(t)] = damping / (6.0 + r_ext[2 + x, tile_of(t)])

    source = lax.broadcasted_iota(jnp.int32, (Z, Z), 0)
    target = lax.broadcasted_iota(jnp.int32, (Z, Z), 1)
    apart = jnp.abs(source - target)
    band = jnp.where(apart == 1, 1.0, 0.0).astype(jnp.bfloat16)
    paired = (apart == 2) | ((apart == 1) & (source // 2 == target // 2))
    pairs = jnp.where(paired, 1.0, 0.0).astype(jnp.bfloat16)
    for part in range(3):
        band_ref[part * Z : part * Z + Z] = band
        pairs_ref[part * Z : part * Z + Z] = pairs

    levels = local_levels(X)
    for c in range(C):
        for t in near:
            approx, details = [v_at(c, x, t) for x in range(X)], []
            for level in range(levels):
                low, high = approx[0::2], approx[1::2]
                approx = [(a + b) * root_half for a, b in zip(low, high)]
                if level > 0:
                    details = [(a - b) * root_half for a, b in zip(low, high)] + details
            tile, spot = divmod(c * parts + t, combos_per_tile)
            inside = (lane >= spot * chunk) & (lane < (spot + 1) * chunk)
            for k, values in enumerate(approx + details):
                done = (jnp.where(even_l, values, -values) + lane_swap(values)) * root_half
                for j in range(blocks):
                    moved = lane_roll(done, spot * chunk - j * chunk)
                    if spot:
                        moved = jnp.where(inside, moved, c_send[j, tile, k])
                    c_send[j, tile, k] = moved

    for c in range(C):
        for x in range(X):
            for t in near:
                own = v_at(c, x, t)
                total = f_at(c, x, t) + jnp.where(lane == 0, 0.0, lane_roll(own, 1))
                total = total + jnp.where(lane == Z - 1, 0.0, lane_roll(own, -1))
                for other in range(max(x - 1, 0), min(x + 2, X)):
                    if other != x:
                        total = total + v_at(c, other, t)
                for other, shift, inner in ((t + 1, -1, row < 7), (t - 1, 1, row >= 1)):
                    beyond = row_roll(v_at(c, x, other), shift) if other in near else 0.0
                    total = total + jnp.where(inner, row_roll(own, shift), beyond)
                u1_ext[c, 2 + x, tile_of(t)] = keep * own + w_ext[2 + x, tile_of(t)] * total

    settle(fine_copies(), a_recv_sem.at[0])

    for sides, copy in step_copies():
        pl.when(all_exist(sides, False))(copy.start)
    for j in range(blocks):
        pl.when(me["gx"] != j)(c_copy(j, me["gx"]).start)

    for number in range(5 * C + 2):
        for side in range(2):
            depth = depth_of(number)
            ref, at = x_line(number, Y + depth if side else rows_ext - 1 - depth)
            ref[at, :] = y_recv[side, number]
    for high_x in range(2):
        for high_y in range(2):
            xs = [X + d if high_x else -1 - d for d in range(2)]
            ys = [Y + d if high_y else rows_ext - 1 - d for d in range(2)]
            source = xy_recv.at[2 * high_x + high_y]
            for c in range(C):
                for i, (x, y) in enumerate(((xs[0], ys[0]), (xs[1], ys[0]), (xs[0], ys[1]))):
                    v_ext[c, 3 + x, y : y + 1] = source[3 * c + i : 3 * c + i + 1]
                f_ext[c, 2 + xs[0], ys[0] : ys[0] + 1] = source[3 * C + c : 3 * C + c + 1]
            r_ext[2 + xs[0], ys[0] : ys[0] + 1] = source[4 * C : 4 * C + 1]
    for side in range(2):
        for i in range(4):
            z_recv[side, i, Y : Y + 2] = yz_recv[side, 1, 2 * i : 2 * i + 2]
            z_recv[side, i, Y + 6 : Y + 8] = yz_recv[side, 0, 2 * i : 2 * i + 2]

    def weight_of(reaction):
        return jnp.where(reaction < 0.1 * far, damping / (6.0 + reaction), 0.0)

    for x in range(-2, X + 2):
        outside = max(-x, x - X + 1)
        for t in ring:
            if (outside > 0 and t < tiles_y) or (t == tiles_y and outside < 2):
                w_ext[2 + x, tile_of(t)] = weight_of(r_ext[2 + x, tile_of(t)])

    mixed = {}
    for i in range(4):
        for t in ring:
            mixed[i, t] = jnp.where(place < 4, z_recv[1, i, tile_of(t)], z_recv[0, i, tile_of(t)])
    beyond = {}
    for side in range(2):
        for i in range(2):
            for t in near:
                beyond[side, i, t] = jnp.where(
                    place < 4, xz_recv[1, side, i, tile_of(t)], xz_recv[0, side, i, tile_of(t)]
                )
        ends = [
            jnp.where(place < 4, corner_recv[1, side, high], corner_recv[0, side, high]) for high in range(2)
        ]
        beyond[side, 0, tiles_y] = jnp.where(row < 4, ends[1], ends[0])

    def edge_field(number, t):
        i, half = divmod(number, 2)
        value = lane_roll(mixed[i, t], 64 * half)
        if t < tiles_y or number < 4:
            shift = (64, 0, 32, -32)[number % 4]
            low, high = (lane_roll(beyond[side, i // 2, t], shift) for side in range(2))
            value = jnp.where(group < 4, low, jnp.where(group >= 12, high, value))
        return value

    edge_v = {(c, t): edge_field(c, t) for c in range(C) for t in ring}
    edge_f = {(c, t): edge_field(4 + c, t) for c in range(C) for t in ring}
    edge_w = {t: weight_of(edge_field(7, t)) for t in ring}

    def around_rows(get, t, tiles, by):
        after, before = (t + 1) % tiles, (t - 1) % tiles
        own = get(t)
        above = jnp.where(row < 8 - by, row_roll(own, -by), row_roll(get(after), -by))
        below = jnp.where(row >= by, row_roll(own, by), row_roll(get(before), by))
        return below, above

    def rows_beside(at, t):
        get = lambda t: at(tile_of(t))
        if t < tiles_y:
            above = at(pl.ds(t * 8 + 1, 8))
        else:
            above = jnp.where(row < 7, row_roll(get(t), -1), row_roll(get(0), -1))
        if t > 0:
            below = at(pl.ds(t * 8 - 1, 8))
        else:
            below = jnp.where(row >= 1, row_roll(get(t), 1), row_roll(get(tiles_y), 1))
        return below, above

    def main_total(get, edge, c, x, t, along_z=None):
        below, above = rows_beside(lambda rows: get(c, x, rows), t)
        get = lambda c, x, t, get=get: get(c, x, tile_of(t))
        total = (get(c, x - 1, t) + get(c, x + 1, t)) + (below + above)
        beside_z = lane_roll(edge[c, t], -(8 * (x + 4) + 4))
        if along_z is not None:
            return total + (along_z + jnp.where((lane == 0) | (lane == Z - 1), beside_z, 0.0))
        own = get(c, x, t)
        total = total + jnp.where(lane == 0, beside_z, lane_roll(own, 1))
        return total + jnp.where(lane == Z - 1, beside_z, lane_roll(own, -1))

    def edge_total(get, edge, c, xs, t):
        own = edge[c, t]
        line = own
        for x in xs:
            line = jnp.where(group == x + 4, lane_roll(get(c, x, t), 8 * (x + 4) + 4), line)
        below, above = around_rows(lambda t: edge[c, t], t, tiles_y + 1, 1)
        total = (lane_roll(own, 8) + lane_roll(own, -8)) + (below + above)
        total = total + jnp.where(place == 4, line, lane_roll(own, 1))
        return total + jnp.where(place == 3, line, lane_roll(own, -1))

    u1_at = lambda c, x, t: u1_ext[c, 2 + x, tile_of(t)]
    u2_at = lambda c, x, t: u2_ext[c, 1 + x, tile_of(t)]
    v_rows = lambda c, x, rows: v_ext[c, 3 + x, rows]
    u1_rows = lambda c, x, rows: u1_ext[c, 2 + x, rows]
    u2_rows = lambda c, x, rows: u2_ext[c, 1 + x, rows]
    w_at = lambda x, t: w_ext[2 + x, tile_of(t)]

    edge_1, edge_2 = {}, {}
    for c in range(C):
        for t in ring:
            total = edge_total(v_at, edge_v, c, range(-1, X + 1), t)
            edge_1[c, t] = keep * edge_v[c, t] + edge_w[t] * (edge_f[c, t] + total)
        chosen = [
            (x, t)
            for x in range(-2, X + 2)
            for t in (near if x in (-2, X + 1) else [tiles_y] if 0 <= x < X else ring)
        ]
        along_z = dict(zip(chosen, lane_sums([v_at(c, x, t) for x, t in chosen], band_ref)))
        for x in range(-2, X + 2):
            if 0 <= x < X:
                for t in near:
                    beside_z = lane_roll(edge_v[c, t], -(8 * (x + 4) + 4))
                    total = jnp.where((lane == 0) | (lane == Z - 1), beside_z, 0.0)
                    if t == 0:
                        total = total + jnp.where(row == 0, row_roll(v_at(c, x, tiles_y), 1), 0.0)
                    if t == tiles_y - 1:
                        total = total + jnp.where(row == 7, row_roll(v_at(c, x, tiles_y), -1), 0.0)
                    if x in (0, X - 1):
                        total = total + v_at(c, -1 if x == 0 else X, t)
                    u1_ext[c, 2 + x, tile_of(t)] = u1_at(c, x, t) + w_at(x, t) * total
            for t in near if x in (-2, X + 1) else [tiles_y] if 0 <= x < X else ring:
                total = main_total(v_rows, edge_v, c, x, t, along_z[x, t])
                u1_ext[c, 2 + x, tile_of(t)] = keep * v_at(c, x, t) + w_at(x, t) * (f_at(c, x, t) + total)
    for c in range(C):
        for t in near:
            total = edge_total(u1_at, edge_1, c, range(X), t)
            edge_2[c, t] = keep * edge_1[c, t] + edge_w[t] * (edge_f[c, t] + total)
        chosen = [(x, t) for x in range(-1, X + 1) for t in (near if x in (-1, X) else ring)]
        along_z = dict(zip(chosen, lane_sums([u1_at(c, x, t) for x, t in chosen], band_ref)))
        for x in range(-1, X + 1):
            for t in near if x in (-1, X) else ring:
                total = main_total(u1_rows, edge_1, c, x, t, along_z[x, t])
                u2_ext[c, 1 + x, tile_of(t)] = keep * u1_at(c, x, t) + w_at(x, t) * (f_at(c, x, t) + total)
    sums = []
    for c in range(C):
        chosen = [(x, t) for x in range(X) for t in near]
        along_z = dict(zip(chosen, lane_sums([u2_at(c, x, t) for x, t in chosen], band_ref)))
        sums.append([
            [main_total(u2_rows, edge_2, c, x, t, along_z[x, t]) + f_at(c, x, t) for t in near] for x in range(X)
        ])

    halves = [
        pooled_halves([
            [sums[c][x][t] - (6.0 + r_ext[2 + x, tile_of(t)]) * u2_at(c, x, t) for t in near] for x in range(X)
        ])
        for c in range(C)
    ]
    for t in near:
        total = jnp.zeros((8, Z), f32)
        for c in range(C):
            own, other = halves[c][t]
            here = (lane >= 16 * c) & (lane < 16 * c + 16)
            total = jnp.where(here, lane_take(own, from_far) + lane_take(other, from_far_pair), total)
        zs_coarse[tile_of(t)] = jnp.where(lane < 64, weight_edges[t] * (0.125 * total), step_edges[t])
        for c in range(C):
            own, other = halves[c][t]
            q_ext[1, c, tile_of(t)] = coarse_weight[t] * (0.125 * (own + lane_swap(other)))
    for sides, copy in coarse_copies():
        pl.when(all_exist(sides, False))(copy.start)

    for c in range(C):
        for x in range(X):
            for t in near:
                base_ref[c, x, tile_of(t)] = keep * u2_at(c, x, t) + w_at(x, t) * sums[c][x][t]

    for j in range(blocks):
        @pl.when(me["gx"] == j)
        def _():
            c_recv[j] = c_send[j]

    settle_parts(c_recv_sem.at[0])
    loads[3].wait()
    finish_compressed(range(c_send.shape[1]))

    settle(step_copies(), q_recv_sem.at[1])
    settle(coarse_copies(), q_recv_sem.at[0])

    settle(fine_copies(), a_send_sem.at[0])
    settle(step_copies(), q_send_sem.at[1])
    settle(coarse_copies(), q_send_sem.at[0])
    settle_parts(c_send_sem.at[0])


def finish(base_ref, w_ext, q_ext, h_ext, pairs_ref, comp_ref, vel_hbm, comp_hbm, vel_ref, sem):
    C, X, Y, Z = base_ref.shape
    f32 = jnp.float32
    comp_copy = pltpu.make_async_copy(comp_ref, comp_hbm, sem.at[C])
    comp_copy.start()
    tiles_y = Y // 8
    near = range(tiles_y)
    tile_of = lambda t: slice(t * 8, t * 8 + 8)
    lane = lax.broadcasted_iota(jnp.int32, (8, Z), 1)
    row = lax.broadcasted_iota(jnp.int32, (8, Z), 0)
    even_l = lane % 2 == 0
    even_r = row % 2 == 0
    slot_at = lane % 16
    corner_of = ((0, 0), (0, 1), (1, 1), (1, 0))
    pair_of = lane + 1 - 2 * (lane % 2)
    lane_roll = lambda t, shift: pltpu.roll(t, shift % Z, 1) if shift % Z else t
    row_roll = lambda t, shift: pltpu.roll(t, shift % 8, 0)
    lane_swap = lambda t: jnp.take_along_axis(t, pair_of, axis=1)
    row_swap = lambda t: jnp.where(even_r, row_roll(t, -1), row_roll(t, 1))

    ring = range(tiles_y + 2)
    after = lambda t: (t + 1) % len(ring)
    before = lambda t: (t - 1) % len(ring)
    main = {(b, c, t): q_ext[b, c, tile_of(t)] for b in range(3) for c in range(C) for t in ring}
    step_main = {(b, t): q_ext[b, C, tile_of(t)] for b in range(3) for t in ring}
    edge = {
        (b, t): jnp.where(slot_at < 8, h_ext[1, b, tile_of(t)], h_ext[0, b, tile_of(t)])
        for b in range(3) for t in ring
    }
    step_edge = {key: lane_roll(value, -64) for key, value in edge.items()}
    first_main, first_edge = dict(main), dict(edge)

    def above(get, t):
        return jnp.where(row < 6, row_roll(get(t), -2), row_roll(get(after(t)), -2))

    def below(get, t):
        return jnp.where(row >= 2, row_roll(get(t), 2), row_roll(get(before(t)), 2))

    def along(get, b, t):
        low, high = get(max(b - 1, 0), t), get(min(b + 1, 2), t)
        across = jnp.where(even_l, jnp.where(even_r, high, low), get(b, t))
        return row_swap(across)

    def inject(edge, b, c, t):
        return lane_roll(edge[b, t], -(16 * c + 8))

    def left_of(main, edge, b, c, t):
        return jnp.where(lane < 2, inject(edge, b, c, t), lane_roll(main[b, c, t], 2))

    def right_of(main, edge, b, c, t):
        return jnp.where(lane >= Z - 2, inject(edge, b, c, t), lane_roll(main[b, c, t], -2))

    def coarse_sweep(main, edge, main_at, edge_at):
        new_main, new_edge = dict(main), dict(edge)
        for c in range(C):
            lanes = dict(zip(main_at, lane_sums([main[b, c, t] for b, t in main_at], pairs_ref)))
            for b, t in main_at:
                get = lambda b, t, c=c: main[b, c, t]
                row_get = lambda t, b=b, c=c: main[b, c, t]
                total = along(get, b, t) + (above(row_get, t) + below(row_get, t))
                ends = jnp.where((lane < 2) | (lane >= Z - 2), inject(edge, b, c, t), 0.0)
                total = total + (lanes[b, t] + ends)
                new_main[b, c, t] = keep * main[b, c, t] + first_main[b, c, t] + step_main[b, t] * total
        for b, t in edge_at:
            get = lambda b, t: edge[b, t]
            row_get = lambda t, b=b: edge[b, t]
            own = lane_roll(main[b, 0, t], 8)
            for c in range(1, C):
                own = jnp.where(lane < 16 * c, own, lane_roll(main[b, c, t], 16 * c + 8))
            total = along(get, b, t) + lane_swap(edge[b, t]) + (above(row_get, t) + below(row_get, t))
            total = total + jnp.where((slot_at == 8) | (slot_at == 9), own, lane_roll(edge[b, t], 2))
            total = total + jnp.where((slot_at == 6) | (slot_at == 7), own, lane_roll(edge[b, t], -2))
            new_edge[b, t] = keep * edge[b, t] + first_edge[b, t] + step_edge[b, t] * total
        return new_main, new_edge

    everywhere = [(b, t) for b in range(3) for t in ring]
    centre = [(1, t) for t in ring]
    sides_near = [(b, t) for b in (0, 2) for t in near]
    main, edge = coarse_sweep(main, edge, everywhere, everywhere)
    main, edge = coarse_sweep(main, edge, everywhere, centre + sides_near)
    main, edge = coarse_sweep(main, edge, centre + sides_near, [(1, t) for t in near])

    def spread_rows(even, odd, pa):
        if pa == 0:
            return jnp.where(even_r, even, row_roll(odd, 1))
        return jnp.where(even_r, row_roll(even, -1), odd)

    def spread_lanes(even, odd, pb):
        if pb == 0:
            return jnp.where(even_l, even, lane_roll(odd, 1))
        return jnp.where(even_l, lane_roll(even, -1), odd)

    copies = []
    for c in range(C):
        for t in near:
            at = tile_of(t)
            row_get = lambda t, c=c: main[1, c, t]
            own = main[1, c, t]
            rows_near = (below(row_get, t), above(row_get, t))
            lanes_near = (left_of(main, edge, 1, c, t), right_of(main, edge, 1, c, t))
            alone = [spread_lanes(own, own, pb) for pb in range(2)]
            spread = [spread_rows(alone[pb], alone[pb], pa) for pa, pb in corner_of]
            low, high = (spread_lanes(main[b, c, t], main[b, c, t], 0) for b in (0, 2))
            spread = [spread_rows(low, low, 1)] + spread + [spread_rows(high, high, 0)]
            based = [3.0 * own + rows_near[a] for a in range(2)]
            wide = [
                [spread_lanes(based[a] + lanes_near[0], based[a] + lanes_near[1], pb) for pb in range(2)]
                for a in range(2)
            ]
            for x in range(X):
                p = x // 2
                pa, pb = corner_of[p]
                added = spread_rows(wide[0][pb], wide[1][pb], pa) + spread[p + 2 * (x % 2)]
                vel_ref[c, x, at] = base_ref[c, x, at] + keep * spread[p + 1] + w_ext[2 + x, at] * added
        copies.append(pltpu.make_async_copy(vel_ref.at[c], vel_hbm.at[c], sem.at[c]))
        copies[-1].start()
    for copy in [comp_copy] + copies:
        copy.wait()


def on_device(counts, velocity_prev, forcing, reaction):
    C, X, Y, Z = velocity_prev.shape
    blocks = counts["gx"]
    kept = X // 2
    chunk = Z // blocks
    tiles = -(-(C * (Y // 8)) // (Z // chunk))
    matrix = jnp.asarray(finish_matrix(X, blocks, 8))
    vmem = pl.BlockSpec(memory_space=pltpu.VMEM)
    space = lambda *shape: pltpu.VMEM(shape, jnp.float32)

    compressed, *kept_arrays = pl.pallas_call(
        functools.partial(kernel, counts),
        out_shape=[
            jax.ShapeDtypeStruct((C, Y, kept * blocks, chunk), jnp.float32),
            jax.ShapeDtypeStruct((C, X, Y, Z), jnp.float32),
            jax.ShapeDtypeStruct((X + 4, Y + 8, Z), jnp.float32),
            jax.ShapeDtypeStruct((3, C + 1, Y + 16, Z), jnp.float32),
            jax.ShapeDtypeStruct((2, 3, Y + 16, Z), jnp.float32),
            jax.ShapeDtypeStruct((3 * Z, Z), jnp.bfloat16),
        ],
        in_specs=[pl.BlockSpec(memory_space=pltpu.HBM)] * 4,
        out_specs=[vmem] * 6,
        scratch_shapes=[
            space(C, X + 6, Y + 8, Z),
            space(C, X + 4, Y + 8, Z),
            space(X + 4, Y + 8, Z),
            space(*matrix.shape),
            space(C, X + 4, Y + 8, Z),
            space(C, X + 2, Y + 8, Z),
            space(2, 5 * C + 2, X, Z),
            space(2, 5 * C + 2, X, Z),
            space(4, 16, Z),
            space(4, 16, Z),
            space(4, Y, Z),
            space(2, 4, Y + 8, Z),
            space(2, 8, Z),
            space(2, 2, 8, Z),
            space(2, Y, Z),
            space(2, 2, 2, Y, Z),
            space(2, 2, 2, 8, Z),
            space(Y, Z),
            space(blocks, tiles, kept, 8, Z),
            space(blocks, tiles, kept, 8, Z),
            space(max((blocks - 1) * tiles * kept * 8, 128 * Y), Z),
            pltpu.VMEM((3 * Z, Z), jnp.bfloat16),
            pltpu.SemaphoreType.DMA((1,)),
            pltpu.SemaphoreType.DMA((1,)),
            pltpu.SemaphoreType.DMA((2,)),
            pltpu.SemaphoreType.DMA((2,)),
            pltpu.SemaphoreType.DMA((1,)),
            pltpu.SemaphoreType.DMA((1,)),
            pltpu.SemaphoreType.DMA((4,)),
        ],
        compiler_params=pltpu.CompilerParams(collective_id=0, has_side_effects=True, vmem_limit_bytes=40000000),
    )(*(pltpu.with_memory_space_constraint(a, pltpu.HBM) for a in (velocity_prev, forcing, reaction, matrix)))
    velocity, compressed = pl.pallas_call(
        finish,
        out_shape=(
            jax.ShapeDtypeStruct((C, X, Y, Z), jnp.float32),
            jax.ShapeDtypeStruct(compressed.shape, jnp.float32),
        ),
        in_specs=[vmem] * 6,
        out_specs=[pl.BlockSpec(memory_space=pltpu.HBM)] * 2,
        scratch_shapes=[space(C, X, Y, Z), pltpu.SemaphoreType.DMA((C + 1,))],
        compiler_params=pltpu.CompilerParams(vmem_limit_bytes=16000000),
    )(*kept_arrays, compressed)
    return velocity, jnp.swapaxes(compressed, 2, 3)


def solution(mesh):
    counts = {axis: mesh.shape[axis] for axis in ("agg", "gx", "gy")}
    placed = (P(None, "gx", "gy", "agg"), P(None, "gx", "gy", "agg"), P("gx", "gy", "agg"))
    return jax.shard_map(
        functools.partial(on_device, counts),
        mesh=mesh,
        in_specs=placed,
        out_specs=(P(None, "gx", "gy", "agg"), P(None, "gy", ("agg", "gx"), None)),
        check_vma=False,
    )
```

```python
import functools
import itertools
import math

import jax
import jax.numpy as jnp
import numpy as np
from jax import lax
from jax.experimental import pallas as pl
from jax.experimental.pallas import tpu as pltpu
from jax.sharding import PartitionSpec as P

SWEEPS = 2
COARSE_SWEEPS = 4
LX = 5
MESH = pl.DeviceIdType.MESH

damping = 0.8
keep = 1.0 - damping
root_half = 0.7071067811865476


def local_levels(cells_x):
    return min(LX, cells_x.bit_length() - 1)


def finish_matrix(cells_x, blocks, rows):
    levels = local_levels(cells_x)
    kept = cells_x // 2
    eye = np.eye(blocks * kept).reshape(blocks, kept, blocks * kept)
    width = cells_x >> levels
    approx = eye[:, :width].reshape(blocks * width, -1)
    details, at = [], width
    for level in range(levels, 1, -1):
        width = cells_x >> level
        details.append(eye[:, at : at + width].reshape(blocks * width, -1))
        at += width
    for level in range(levels, LX):
        low, high = approx[0::2], approx[1::2]
        approx, detail = (low + high) * root_half, (low - high) * root_half
        details.insert(0, detail)
    along_x = np.concatenate([approx] + details, axis=0)
    along_y = np.zeros((rows, rows))
    for row in range(0, rows, 2):
        along_y[row, row : row + 2] = root_half
        along_y[row + 1, row : row + 2] = root_half, -root_half
    return np.einsum("qk,yr->yqkr", along_x, along_y).reshape(-1, blocks * kept * rows).astype(np.float32)


def around():
    axes = ("gx", "gy", "agg")
    found = []
    for number in range(1, 27):
        turn = [(number // 3**i) % 3 for i in range(3)]
        found.append(tuple((axis, way == 1) for axis, way in zip(axes, turn) if way))
    return sorted(found, key=lambda sides: (-len(sides), sides))


def lane_sums(tiles, matrix):
    stack = jnp.concatenate(tiles, axis=0)
    high = stack.astype(jnp.bfloat16)
    rest = stack - high.astype(jnp.float32)
    middle = rest.astype(jnp.bfloat16)
    low = (rest - middle.astype(jnp.float32)).astype(jnp.bfloat16)
    done = lax.dot_general(
        jnp.concatenate([high, middle, low], axis=1), matrix[...], (((1,), (0,)), ((), ())),
        preferred_element_type=jnp.float32,
    )
    return [done[i * 8 : i * 8 + 8] for i in range(len(tiles))]


far = 1e30


def kernel(
    sizes, v_hbm, f_hbm, r_hbm, m_hbm, comp_ref, base_ref, w_ext, q_ext, h_ext, pairs_ref,
    v_ext, f_ext, r_ext, m_ref, u1_ext, u2_ext,
    y_send, y_recv, xy_send, xy_recv, z_send, z_recv, yz_send, yz_recv, xz_send, xz_recv, corner_recv,
    zs_coarse, c_send, c_recv, measure, band_ref,
    a_send_sem, a_recv_sem, q_send_sem, q_recv_sem, c_send_sem, c_recv_sem, in_sem,
):
    counts = sizes
    C, X, Y, Z = base_ref.shape
    me = {axis: lax.axis_index(axis) for axis in counts}
    blocks = counts["gx"]
    chunk = Z // blocks
    rows_ext = Y + 8
    f32 = jnp.float32

    loads = [
        pltpu.make_async_copy(src, dst, in_sem.at[i])
        for i, (src, dst) in enumerate(
            [(v_hbm.at[c], v_ext.at[c, 3 : 3 + X, :Y]) for c in range(C)]
            + [(f_hbm.at[c], f_ext.at[c, 2 : 2 + X, :Y]) for c in range(C)]
            + [(r_hbm, r_ext.at[2 : 2 + X, :Y]), (m_hbm, m_ref)]
        )
    ]
    for load in loads:
        load.start()

    def exists(axis, high):
        return me[axis] < counts[axis] - 1 if high else me[axis] > 0

    def all_exist(sides, flip):
        there = None
        for axis, high in sides:
            one = exists(axis, high != flip)
            there = one if there is None else there & one
        return there

    def beside(*sides):
        return {axis: me[axis] + (1 if high else -1) for axis, high in sides}

    barrier = pltpu.get_barrier_semaphore()
    expected = blocks - 1
    for sides in around():
        if len(sides) > 1 or sides[0][0] != "gx":
            there = all_exist(sides, False)
            expected = expected + there.astype(jnp.int32)

            @pl.when(there)
            def _():
                pl.semaphore_signal(barrier, inc=1, device_id=beside(*sides), device_id_type=MESH)

    for step in range(1, blocks):
        pl.semaphore_signal(
            barrier, inc=1, device_id={"gx": lax.rem(me["gx"] + step, blocks)}, device_id_type=MESH
        )

    lane = lax.broadcasted_iota(jnp.int32, (8, Z), 1)
    row = lax.broadcasted_iota(jnp.int32, (8, Z), 0)
    place = lane % 8
    group = lane // 8
    low_half = (lane < 32) | (lane >= 96)

    def fine_messages(sides):
        at = {axis: high for axis, high in sides}
        x, y, z = at.get("gx"), at.get("gy"), at.get("agg")
        from_x, from_y, from_z = 0 if x else 1, 0 if y else 1, 0 if z else 1
        if z is None and y is None:
            made = []
            for ref, depth, fill in ((v_ext, 3, 0.0), (f_ext, 2, 0.0), (r_ext, 2, far)):
                here = pl.ds(X if x else depth, depth)
                there = pl.ds(0 if x else depth + X, depth)
                index = (slice(None),) if ref is not r_ext else ()
                made.append((ref.at[index + (here, pl.ds(0, Y))], ref.at[index + (there, pl.ds(0, Y))], fill))
            return made
        if z is None and x is None:
            return [(y_send.at[int(y)], y_recv.at[from_y], None)]
        if z is None:
            return [(xy_send.at[2 * int(x) + int(y)], xy_recv.at[2 * from_x + from_y], None)]
        if x is None and y is None:
            return [(z_send, z_recv.at[from_z, :, pl.ds(0, Y)], None)]
        if x is None:
            return [(yz_send.at[int(y)], yz_recv.at[from_z, from_y], None)]
        if y is None:
            return [(xz_send, xz_recv.at[from_z, from_x], None)]
        return [(xz_send.at[0, pl.ds(Y - 8 if y else 0, 8)], corner_recv.at[from_z, from_x, from_y], 0.0)]

    def remote(src, dst, send_sem, recv_sem, sides):
        return pltpu.make_async_remote_copy(
            src_ref=src, dst_ref=dst, send_sem=send_sem, recv_sem=recv_sem,
            device_id=beside(*sides), device_id_type=MESH,
        )

    def fine_copies():
        return [
            (sides, remote(src, dst, a_send_sem.at[0], a_recv_sem.at[0], sides))
            for sides in around()
            for src, dst, _ in fine_messages(sides)
        ]

    def rows_of(copies):
        found = {}
        for sides, copy in copies:
            axes = tuple(axis for axis, _ in sides)
            if all(high for _, high in sides):
                found[axes] = found.get(axes, 0) + math.prod(copy.src_ref.shape[:-1])
        return found

    def settle(copies, sem):
        sizes = rows_of(copies)
        neighbours = {
            axis: exists(axis, False).astype(jnp.int32) + exists(axis, True).astype(jnp.int32) for axis in counts
        }
        options = {axis: {1: (0,), 2: (1,)}.get(count, (1, 2)) for axis, count in counts.items()}
        for numbers in itertools.product(*options.values()):
            number = dict(zip(options, numbers))
            rows = sum(size * math.prod(number[axis] for axis in axes) for axes, size in sizes.items())
            there = None
            for axis, value in number.items():
                one = neighbours[axis] == value
                there = one if there is None else there & one
            if rows:
                part = measure.at[pl.ds(0, rows)]
                pl.when(there)(pltpu.make_async_copy(part, part, sem).wait)

    def coarse_message(sides, first=0, fields=C):
        at = {axis: 1 if high else -1 for axis, high in sides}
        block = 1 - at.get("gx", 0)
        here, there = {
            0: (slice(0, Y), slice(0, Y)),
            1: (slice(Y - 8, Y), slice(Y + 8, Y + 16)),
            -1: (slice(0, 8), slice(Y, Y + 8)),
        }[at.get("gy", 0)]
        if "agg" in at:
            return zs_coarse.at[here], h_ext.at[0 if at["agg"] > 0 else 1, block, there]
        which = pl.ds(first, fields)
        return q_ext.at[1, which, here], q_ext.at[block, which, there]

    def coarse_copies():
        return [
            (sides, remote(*coarse_message(sides), q_send_sem.at[0], q_recv_sem.at[0], sides))
            for sides in around()
        ]

    def step_copies():
        return [
            (sides, remote(*coarse_message(sides, C, 1), q_send_sem.at[1], q_recv_sem.at[1], sides))
            for sides in around()
            if "agg" not in dict(sides)
        ]

    far_high = jnp.where(low_half, far, 0.0).astype(f32)
    for sides in around():
        @pl.when(jnp.logical_not(all_exist(sides, True)))
        def _():
            axes = tuple(axis for axis, _ in sides)
            for _, target, fill in fine_messages(sides):
                if fill is not None:
                    target[...] = jnp.full(target.shape, fill, f32)
                elif axes == ("gy",):
                    target[: 5 * C] = jnp.zeros((5 * C, 8, Z), f32)
                    target[5 * C :] = jnp.full((2, 8, Z), far, f32)
                elif axes == ("gx", "gy"):
                    target[0:8] = jnp.zeros((8, Z), f32)
                    target[8:16] = jnp.where(row == 4 * C - 8, far, 0.0)
                elif axes == ("agg",):
                    target[:3] = jnp.zeros((3, Y, Z), f32)
                    for t in range(Y // 8):
                        target[3, t * 8 : t * 8 + 8] = far_high
                elif axes == ("gy", "agg"):
                    target[...] = jnp.where(row >= 6, far_high, 0.0)
                else:
                    target[0] = jnp.zeros((Y, Z), f32)
                    for t in range(Y // 8):
                        target[1, t * 8 : t * 8 + 8] = jnp.where(
                            (group == 0) | (group == 1) | (group == 6) | (group == 7), far, 0.0
                        )
            for target in [coarse_message(sides)[1], coarse_message(sides, C, 1)[1]][: 1 + ("agg" not in axes)]:
                target[...] = jnp.zeros(target.shape, f32)

    tiles_y = Y // 8
    near, ring = range(tiles_y), range(tiles_y + 1)
    tile_of = lambda t: slice(t * 8, t * 8 + 8)
    even_l = lane % 2 == 0
    even_r = row % 2 == 0
    lane_roll = lambda t, shift: pltpu.roll(t, shift % Z, 1) if shift % Z else t
    row_roll = lambda t, shift: pltpu.roll(t, shift % 8, 0)
    lane_take = lambda t, source: jnp.take_along_axis(t, source, axis=1)
    v_flat = v_ext.reshape(C * (X + 6) * rows_ext, Z)
    f_flat = f_ext.reshape(C * (X + 4) * rows_ext, Z)
    r_flat = r_ext.reshape((X + 4) * rows_ext, Z)

    def x_line(number, y):
        if number < 3 * C:
            c, ref, extra = number // 3, v_flat, 3
        elif number < 5 * C:
            c, ref, extra = (number - 3 * C) // 2, f_flat, 2
        else:
            c, ref, extra = 0, r_flat, 2
        return ref, pl.ds((c * (X + 2 * extra) + extra) * rows_ext + y, X, stride=rows_ext)

    depth_of = lambda number: number % 3 if number < 3 * C else (number - 3 * C) % 2

    v_at = lambda c, x, t: v_ext[c, 3 + x, tile_of(t)]
    f_at = lambda c, x, t: f_ext[c, 2 + x, tile_of(t)]
    held = (
        (lambda x, t: v_at(0, x, t), lambda x, t: v_at(1, x, t)),
        (lambda x, t: v_at(2, x, t), None),
        (lambda x, t: f_at(0, x, t), lambda x, t: f_at(1, x, t)),
        (lambda x, t: f_at(2, x, t), lambda x, t: r_ext[2 + x, tile_of(t)]),
    )
    from_ends = jnp.where(place < 4, 3 - place, Z + 3 - place)
    needed = ((0, 1), (2,), (3, 4), (5, 6))
    across = {}
    for i, pair in enumerate(held):
        for number in needed[i]:
            loads[number].wait()
        for t in near:
            packed = jnp.zeros((8, Z), f32)
            crossed = across.get(t, packed) if i % 2 else packed
            for half, get in enumerate(pair):
                if get is not None:
                    for x in range(X):
                        ends = lane_take(get(x, t), from_ends)
                        packed = jnp.where(group == (x + 4 + 8 * half) % 16, ends, packed)
                        if x < 2 or x >= X - 2:
                            crossed = jnp.where(group == (x + 4 + 8 * half + 4 * (i % 2)) % 16, ends, crossed)
            across[t] = crossed
            z_send[i, tile_of(t)] = packed
            if i % 2:
                xz_send[i // 2, tile_of(t)] = crossed
            for side in range(2):
                if t == (tiles_y - 1 if side else 0):
                    first = 6 if side else 0
                    yz_send[side, 2 * i : 2 * i + 2] = packed[first : first + 2]
    for number in range(5 * C + 2):
        for side in range(2):
            depth = depth_of(number)
            ref, at = x_line(number, Y - 1 - depth if side else depth)
            y_send[side, number] = ref[at, :]
    for high_x in range(2):
        for high_y in range(2):
            xs = [X - 1 - d if high_x else d for d in range(2)]
            ys = [Y - 1 - d if high_y else d for d in range(2)]
            target = xy_send.at[2 * high_x + high_y]
            for c in range(C):
                for i, (x, y) in enumerate(((xs[0], ys[0]), (xs[1], ys[0]), (xs[0], ys[1]))):
                    target[3 * c + i : 3 * c + i + 1] = v_ext[c, 3 + x, y : y + 1]
                target[3 * C + c : 3 * C + c + 1] = f_ext[c, 2 + xs[0], ys[0] : ys[0] + 1]
            target[4 * C : 4 * C + 1] = r_ext[2 + xs[0], ys[0] : ys[0] + 1]
    pl.semaphore_wait(barrier, expected)
    for sides, copy in fine_copies():
        pl.when(all_exist(sides, False))(copy.start)

    kept = X // 2
    parts = Y // 8
    combos_per_tile = Z // chunk

    def c_copy(j, source):
        return pltpu.make_async_remote_copy(
            src_ref=c_send.at[j],
            dst_ref=c_recv.at[source],
            send_sem=c_send_sem.at[0],
            recv_sem=c_recv_sem.at[0],
            device_id={"gx": j},
            device_id_type=MESH,
        )

    def settle_parts(sem):
        rows = (blocks - 1) * math.prod(c_send.shape[1:-1])
        if rows:
            part = measure.at[pl.ds(0, rows)]
            pltpu.make_async_copy(part, part, sem).wait()

    def finish_compressed(tiles):
        coefs = blocks * kept
        for tile in tiles:
            gathered = c_recv[:, tile].reshape(coefs * 8, Z)
            done = lax.dot_general(
                m_ref[...], gathered, (((1,), (0,)), ((), ())),
                precision=lax.Precision.HIGHEST, preferred_element_type=jnp.float32,
            )
            for place in range(combos_per_tile):
                c, part = divmod(tile * combos_per_tile + place, parts)
                if c < C:
                    for y in range(8):
                        comp_ref[c, part * 8 + y] = done[
                            y * coefs : (y + 1) * coefs, place * chunk : (place + 1) * chunk
                        ]

    pair_of = lane + 1 - 2 * (lane % 2)
    lane_swap = lambda t: lane_take(t, pair_of)
    row_swap = lambda t: jnp.where(even_r, row_roll(t, -1), row_roll(t, 1))
    slot_at = lane % 16
    corner_of = ((0, 0), (0, 1), (1, 1), (1, 0))

    def pooled_halves(planes):
        pairs = [[planes[x][t] + planes[x + 1][t] for t in near] for x in range(0, X, 2)]
        out = []
        for t in near:
            t0, t1, t2, t3 = (pair[t] for pair in pairs)
            left = jnp.where(even_r, t0, t3) + row_swap(jnp.where(even_r, t3, t0))
            right = jnp.where(even_r, t1, t2) + row_swap(jnp.where(even_r, t2, t1))
            out.append((jnp.where(even_l, left, right), jnp.where(even_l, right, left)))
        return out

    def pooled(planes):
        return [own + lane_swap(other) for own, other in pooled_halves(planes)]

    from_far = jnp.where(slot_at < 8, 6, Z + 6) - slot_at + 2 * (slot_at % 2)

    from_far_pair = from_far + 1 - 2 * (from_far % 2)

    def edge_lanes(fields, t):
        packed = jnp.zeros((8, Z), f32)
        for start, field in fields:
            packed = jnp.where((lane >= start) & (lane < start + 16), lane_take(field[t], from_far), packed)
        return packed

    coarse_weight = [
        damping / ((6.0 + 0.5 * total) * 0.25)
        for total in pooled([[r_ext[2 + x, tile_of(t)] for t in near] for x in range(X)])
    ]
    coarse_step = [0.25 * weight for weight in coarse_weight]
    step_edges = [edge_lanes([(64 + 16 * c, coarse_step) for c in range(C)], t) for t in near]
    weight_edges = [edge_lanes([(16 * c, coarse_weight) for c in range(C)], t) for t in near]
    for t in near:
        q_ext[1, C, tile_of(t)] = coarse_step[t]
    for x in range(X):
        for t in near:
            w_ext[2 + x, tile_of(t)] = damping / (6.0 + r_ext[2 + x, tile_of(t)])

    source = lax.broadcasted_iota(jnp.int32, (Z, Z), 0)
    target = lax.broadcasted_iota(jnp.int32, (Z, Z), 1)
    apart = jnp.abs(source - target)
    band = jnp.where(apart == 1, 1.0, 0.0).astype(jnp.bfloat16)
    paired = (apart == 2) | ((apart == 1) & (source // 2 == target // 2))
    pairs = jnp.where(paired, 1.0, 0.0).astype(jnp.bfloat16)
    for part in range(3):
        band_ref[part * Z : part * Z + Z] = band
        pairs_ref[part * Z : part * Z + Z] = pairs

    levels = local_levels(X)
    for c in range(C):
        for t in near:
            approx, details = [v_at(c, x, t) for x in range(X)], []
            for level in range(levels):
                low, high = approx[0::2], approx[1::2]
                approx = [(a + b) * root_half for a, b in zip(low, high)]
                if level > 0:
                    details = [(a - b) * root_half for a, b in zip(low, high)] + details
            tile, spot = divmod(c * parts + t, combos_per_tile)
            inside = (lane >= spot * chunk) & (lane < (spot + 1) * chunk)
            for k, values in enumerate(approx + details):
                done = (jnp.where(even_l, values, -values) + lane_swap(values)) * root_half
                for j in range(blocks):
                    moved = lane_roll(done, spot * chunk - j * chunk)
                    if spot:
                        moved = jnp.where(inside, moved, c_send[j, tile, k])
                    c_send[j, tile, k] = moved

    for c in range(C):
        for x in range(X):
            for t in near:
                own = v_at(c, x, t)
                total = f_at(c, x, t) + jnp.where(lane == 0, 0.0, lane_roll(own, 1))
                total = total + jnp.where(lane == Z - 1, 0.0, lane_roll(own, -1))
                for other in range(max(x - 1, 0), min(x + 2, X)):
                    if other != x:
                        total = total + v_at(c, other, t)
                for other, shift, inner in ((t + 1, -1, row < 7), (t - 1, 1, row >= 1)):
                    beyond = row_roll(v_at(c, x, other), shift) if other in near else 0.0
                    total = total + jnp.where(inner, row_roll(own, shift), beyond)
                u1_ext[c, 2 + x, tile_of(t)] = keep * own + w_ext[2 + x, tile_of(t)] * total

    settle(fine_copies(), a_recv_sem.at[0])

    for sides, copy in step_copies():
        pl.when(all_exist(sides, False))(copy.start)
    for j in range(blocks):
        pl.when(me["gx"] != j)(c_copy(j, me["gx"]).start)

    for number in range(5 * C + 2):
        for side in range(2):
            depth = depth_of(number)
            ref, at = x_line(number, Y + depth if side else rows_ext - 1 - depth)
            ref[at, :] = y_recv[side, number]
    for high_x in range(2):
        for high_y in range(2):
            xs = [X + d if high_x else -1 - d for d in range(2)]
            ys = [Y + d if high_y else rows_ext - 1 - d for d in range(2)]
            source = xy_recv.at[2 * high_x + high_y]
            for c in range(C):
                for i, (x, y) in enumerate(((xs[0], ys[0]), (xs[1], ys[0]), (xs[0], ys[1]))):
                    v_ext[c, 3 + x, y : y + 1] = source[3 * c + i : 3 * c + i + 1]
                f_ext[c, 2 + xs[0], ys[0] : ys[0] + 1] = source[3 * C + c : 3 * C + c + 1]
            r_ext[2 + xs[0], ys[0] : ys[0] + 1] = source[4 * C : 4 * C + 1]
    for side in range(2):
        for i in range(4):
            z_recv[side, i, Y : Y + 2] = yz_recv[side, 1, 2 * i : 2 * i + 2]
            z_recv[side, i, Y + 6 : Y + 8] = yz_recv[side, 0, 2 * i : 2 * i + 2]

    def weight_of(reaction):
        return jnp.where(reaction < 0.1 * far, damping / (6.0 + reaction), 0.0)

    for x in range(-2, X + 2):
        outside = max(-x, x - X + 1)
        for t in ring:
            if (outside > 0 and t < tiles_y) or (t == tiles_y and outside < 2):
                w_ext[2 + x, tile_of(t)] = weight_of(r_ext[2 + x, tile_of(t)])

    mixed = {}
    for i in range(4):
        for t in ring:
            mixed[i, t] = jnp.where(place < 4, z_recv[1, i, tile_of(t)], z_recv[0, i, tile_of(t)])
    beyond = {}
    for side in range(2):
        for i in range(2):
            for t in near:
                beyond[side, i, t] = jnp.where(
                    place < 4, xz_recv[1, side, i, tile_of(t)], xz_recv[0, side, i, tile_of(t)]
                )
        ends = [
            jnp.where(place < 4, corner_recv[1, side, high], corner_recv[0, side, high]) for high in range(2)
        ]
        beyond[side, 0, tiles_y] = jnp.where(row < 4, ends[1], ends[0])

    def edge_field(number, t):
        i, half = divmod(number, 2)
        value = lane_roll(mixed[i, t], 64 * half)
        if t < tiles_y or number < 4:
            shift = (64, 0, 32, -32)[number % 4]
            low, high = (lane_roll(beyond[side, i // 2, t], shift) for side in range(2))
            value = jnp.where(group < 4, low, jnp.where(group >= 12, high, value))
        return value

    edge_v = {(c, t): edge_field(c, t) for c in range(C) for t in ring}
    edge_f = {(c, t): edge_field(4 + c, t) for c in range(C) for t in ring}
    edge_w = {t: weight_of(edge_field(7, t)) for t in ring}

    def around_rows(get, t, tiles, by):
        after, before = (t + 1) % tiles, (t - 1) % tiles
        own = get(t)
        above = jnp.where(row < 8 - by, row_roll(own, -by), row_roll(get(after), -by))
        below = jnp.where(row >= by, row_roll(own, by), row_roll(get(before), by))
        return below, above

    def rows_beside(at, t):
        get = lambda t: at(tile_of(t))
        if t < tiles_y:
            above = at(pl.ds(t * 8 + 1, 8))
        else:
            above = jnp.where(row < 7, row_roll(get(t), -1), row_roll(get(0), -1))
        if t > 0:
            below = at(pl.ds(t * 8 - 1, 8))
        else:
            below = jnp.where(row >= 1, row_roll(get(t), 1), row_roll(get(tiles_y), 1))
        return below, above

    def main_total(get, edge, c, x, t, along_z=None):
        below, above = rows_beside(lambda rows: get(c, x, rows), t)
        get = lambda c, x, t, get=get: get(c, x, tile_of(t))
        total = (get(c, x - 1, t) + get(c, x + 1, t)) + (below + above)
        beside_z = lane_roll(edge[c, t], -(8 * (x + 4) + 4))
        if along_z is not None:
            return total + (along_z + jnp.where((lane == 0) | (lane == Z - 1), beside_z, 0.0))
        own = get(c, x, t)
        total = total + jnp.where(lane == 0, beside_z, lane_roll(own, 1))
        return total + jnp.where(lane == Z - 1, beside_z, lane_roll(own, -1))

    def edge_total(get, edge, c, xs, t):
        own = edge[c, t]
        line = own
        for x in xs:
            line = jnp.where(group == x + 4, lane_roll(get(c, x, t), 8 * (x + 4) + 4), line)
        below, above = around_rows(lambda t: edge[c, t], t, tiles_y + 1, 1)
        total = (lane_roll(own, 8) + lane_roll(own, -8)) + (below + above)
        total = total + jnp.where(place == 4, line, lane_roll(own, 1))
        return total + jnp.where(place == 3, line, lane_roll(own, -1))

    u1_at = lambda c, x, t: u1_ext[c, 2 + x, tile_of(t)]
    u2_at = lambda c, x, t: u2_ext[c, 1 + x, tile_of(t)]
    v_rows = lambda c, x, rows: v_ext[c, 3 + x, rows]
    u1_rows = lambda c, x, rows: u1_ext[c, 2 + x, rows]
    u2_rows = lambda c, x, rows: u2_ext[c, 1 + x, rows]
    w_at = lambda x, t: w_ext[2 + x, tile_of(t)]

    edge_1, edge_2 = {}, {}
    for c in range(C):
        for t in ring:
            total = edge_total(v_at, edge_v, c, range(-1, X + 1), t)
            edge_1[c, t] = keep * edge_v[c, t] + edge_w[t] * (edge_f[c, t] + total)
        chosen = [
            (x, t)
            for x in range(-2, X + 2)
            for t in (near if x in (-2, X + 1) else [tiles_y] if 0 <= x < X else ring)
        ]
        along_z = dict(zip(chosen, lane_sums([v_at(c, x, t) for x, t in chosen], band_ref)))
        for x in range(-2, X + 2):
            if 0 <= x < X:
                for t in near:
                    beside_z = lane_roll(edge_v[c, t], -(8 * (x + 4) + 4))
                    total = jnp.where((lane == 0) | (lane == Z - 1), beside_z, 0.0)
                    if t == 0:
                        total = total + jnp.where(row == 0, row_roll(v_at(c, x, tiles_y), 1), 0.0)
                    if t == tiles_y - 1:
                        total = total + jnp.where(row == 7, row_roll(v_at(c, x, tiles_y), -1), 0.0)
                    if x in (0, X - 1):
                        total = total + v_at(c, -1 if x == 0 else X, t)
                    u1_ext[c, 2 + x, tile_of(t)] = u1_at(c, x, t) + w_at(x, t) * total
            for t in near if x in (-2, X + 1) else [tiles_y] if 0 <= x < X else ring:
                total = main_total(v_rows, edge_v, c, x, t, along_z[x, t])
                u1_ext[c, 2 + x, tile_of(t)] = keep * v_at(c, x, t) + w_at(x, t) * (f_at(c, x, t) + total)
    for c in range(C):
        for t in near:
            total = edge_total(u1_at, edge_1, c, range(X), t)
            edge_2[c, t] = keep * edge_1[c, t] + edge_w[t] * (edge_f[c, t] + total)
        chosen = [(x, t) for x in range(-1, X + 1) for t in (near if x in (-1, X) else ring)]
        along_z = dict(zip(chosen, lane_sums([u1_at(c, x, t) for x, t in chosen], band_ref)))
        for x in range(-1, X + 1):
            for t in near if x in (-1, X) else ring:
                total = main_total(u1_rows, edge_1, c, x, t, along_z[x, t])
                u2_ext[c, 1 + x, tile_of(t)] = keep * u1_at(c, x, t) + w_at(x, t) * (f_at(c, x, t) + total)
    sums = []
    for c in range(C):
        chosen = [(x, t) for x in range(X) for t in near]
        along_z = dict(zip(chosen, lane_sums([u2_at(c, x, t) for x, t in chosen], band_ref)))
        sums.append([
            [main_total(u2_rows, edge_2, c, x, t, along_z[x, t]) + f_at(c, x, t) for t in near] for x in range(X)
        ])

    halves = [
        pooled_halves([
            [sums[c][x][t] - (6.0 + r_ext[2 + x, tile_of(t)]) * u2_at(c, x, t) for t in near] for x in range(X)
        ])
        for c in range(C)
    ]
    for t in near:
        total = jnp.zeros((8, Z), f32)
        for c in range(C):
            own, other = halves[c][t]
            here = (lane >= 16 * c) & (lane < 16 * c + 16)
            total = jnp.where(here, lane_take(own, from_far) + lane_take(other, from_far_pair), total)
        zs_coarse[tile_of(t)] = jnp.where(lane < 64, weight_edges[t] * (0.125 * total), step_edges[t])
        for c in range(C):
            own, other = halves[c][t]
            q_ext[1, c, tile_of(t)] = coarse_weight[t] * (0.125 * (own + lane_swap(other)))
    for sides, copy in coarse_copies():
        pl.when(all_exist(sides, False))(copy.start)

    for c in range(C):
        for x in range(X):
            for t in near:
                base_ref[c, x, tile_of(t)] = keep * u2_at(c, x, t) + w_at(x, t) * sums[c][x][t]

    for j in range(blocks):
        @pl.when(me["gx"] == j)
        def _():
            c_recv[j] = c_send[j]

    settle_parts(c_recv_sem.at[0])
    loads[-1].wait()
    finish_compressed(range(c_send.shape[1]))

    settle(step_copies(), q_recv_sem.at[1])
    settle(coarse_copies(), q_recv_sem.at[0])

    settle(fine_copies(), a_send_sem.at[0])
    settle(step_copies(), q_send_sem.at[1])
    settle(coarse_copies(), q_send_sem.at[0])
    settle_parts(c_send_sem.at[0])


def finish(base_ref, w_ext, q_ext, h_ext, pairs_ref, comp_ref, vel_hbm, comp_hbm, vel_ref, sem):
    C, X, Y, Z = base_ref.shape
    f32 = jnp.float32
    comp_copy = pltpu.make_async_copy(comp_ref, comp_hbm, sem.at[C])
    comp_copy.start()
    tiles_y = Y // 8
    near = range(tiles_y)
    tile_of = lambda t: slice(t * 8, t * 8 + 8)
    lane = lax.broadcasted_iota(jnp.int32, (8, Z), 1)
    row = lax.broadcasted_iota(jnp.int32, (8, Z), 0)
    even_l = lane % 2 == 0
    even_r = row % 2 == 0
    slot_at = lane % 16
    corner_of = ((0, 0), (0, 1), (1, 1), (1, 0))
    pair_of = lane + 1 - 2 * (lane % 2)
    lane_roll = lambda t, shift: pltpu.roll(t, shift % Z, 1) if shift % Z else t
    row_roll = lambda t, shift: pltpu.roll(t, shift % 8, 0)
    lane_swap = lambda t: jnp.take_along_axis(t, pair_of, axis=1)
    row_swap = lambda t: jnp.where(even_r, row_roll(t, -1), row_roll(t, 1))

    ring = range(tiles_y + 2)
    after = lambda t: (t + 1) % len(ring)
    before = lambda t: (t - 1) % len(ring)
    main = {(b, c, t): q_ext[b, c, tile_of(t)] for b in range(3) for c in range(C) for t in ring}
    step_main = {(b, t): q_ext[b, C, tile_of(t)] for b in range(3) for t in ring}
    edge = {
        (b, t): jnp.where(slot_at < 8, h_ext[1, b, tile_of(t)], h_ext[0, b, tile_of(t)])
        for b in range(3) for t in ring
    }
    step_edge = {key: lane_roll(value, -64) for key, value in edge.items()}
    first_main, first_edge = dict(main), dict(edge)

    def above(get, t):
        return jnp.where(row < 6, row_roll(get(t), -2), row_roll(get(after(t)), -2))

    def below(get, t):
        return jnp.where(row >= 2, row_roll(get(t), 2), row_roll(get(before(t)), 2))

    def along(get, b, t):
        low, high = get(max(b - 1, 0), t), get(min(b + 1, 2), t)
        across = jnp.where(even_l, jnp.where(even_r, high, low), get(b, t))
        return row_swap(across)

    def inject(edge, b, c, t):
        return lane_roll(edge[b, t], -(16 * c + 8))

    def left_of(main, edge, b, c, t):
        return jnp.where(lane < 2, inject(edge, b, c, t), lane_roll(main[b, c, t], 2))

    def right_of(main, edge, b, c, t):
        return jnp.where(lane >= Z - 2, inject(edge, b, c, t), lane_roll(main[b, c, t], -2))

    def coarse_sweep(main, edge, main_at, edge_at):
        new_main, new_edge = dict(main), dict(edge)
        for c in range(C):
            lanes = dict(zip(main_at, lane_sums([main[b, c, t] for b, t in main_at], pairs_ref)))
            for b, t in main_at:
                get = lambda b, t, c=c: main[b, c, t]
                row_get = lambda t, b=b, c=c: main[b, c, t]
                total = along(get, b, t) + (above(row_get, t) + below(row_get, t))
                ends = jnp.where((lane < 2) | (lane >= Z - 2), inject(edge, b, c, t), 0.0)
                total = total + (lanes[b, t] + ends)
                new_main[b, c, t] = keep * main[b, c, t] + first_main[b, c, t] + step_main[b, t] * total
        for b, t in edge_at:
            get = lambda b, t: edge[b, t]
            row_get = lambda t, b=b: edge[b, t]
            own = lane_roll(main[b, 0, t], 8)
            for c in range(1, C):
                own = jnp.where(lane < 16 * c, own, lane_roll(main[b, c, t], 16 * c + 8))
            total = along(get, b, t) + lane_swap(edge[b, t]) + (above(row_get, t) + below(row_get, t))
            total = total + jnp.where((slot_at == 8) | (slot_at == 9), own, lane_roll(edge[b, t], 2))
            total = total + jnp.where((slot_at == 6) | (slot_at == 7), own, lane_roll(edge[b, t], -2))
            new_edge[b, t] = keep * edge[b, t] + first_edge[b, t] + step_edge[b, t] * total
        return new_main, new_edge

    everywhere = [(b, t) for b in range(3) for t in ring]
    centre = [(1, t) for t in ring]
    sides_near = [(b, t) for b in (0, 2) for t in near]
    main, edge = coarse_sweep(main, edge, everywhere, everywhere)
    main, edge = coarse_sweep(main, edge, everywhere, centre + sides_near)
    main, edge = coarse_sweep(main, edge, centre + sides_near, [(1, t) for t in near])

    def spread_rows(even, odd, pa):
        if pa == 0:
            return jnp.where(even_r, even, row_roll(odd, 1))
        return jnp.where(even_r, row_roll(even, -1), odd)

    def spread_lanes(even, odd, pb):
        if pb == 0:
            return jnp.where(even_l, even, lane_roll(odd, 1))
        return jnp.where(even_l, lane_roll(even, -1), odd)

    copies = []
    for c in range(C):
        for t in near:
            at = tile_of(t)
            row_get = lambda t, c=c: main[1, c, t]
            own = main[1, c, t]
            rows_near = (below(row_get, t), above(row_get, t))
            lanes_near = (left_of(main, edge, 1, c, t), right_of(main, edge, 1, c, t))
            alone = [spread_lanes(own, own, pb) for pb in range(2)]
            spread = [spread_rows(alone[pb], alone[pb], pa) for pa, pb in corner_of]
            low, high = (spread_lanes(main[b, c, t], main[b, c, t], 0) for b in (0, 2))
            spread = [spread_rows(low, low, 1)] + spread + [spread_rows(high, high, 0)]
            based = [3.0 * own + rows_near[a] for a in range(2)]
            wide = [
                [spread_lanes(based[a] + lanes_near[0], based[a] + lanes_near[1], pb) for pb in range(2)]
                for a in range(2)
            ]
            for x in range(X):
                p = x // 2
                pa, pb = corner_of[p]
                added = spread_rows(wide[0][pb], wide[1][pb], pa) + spread[p + 2 * (x % 2)]
                vel_ref[c, x, at] = base_ref[c, x, at] + keep * spread[p + 1] + w_ext[2 + x, at] * added
        copies.append(pltpu.make_async_copy(vel_ref.at[c], vel_hbm.at[c], sem.at[c]))
        copies[-1].start()
    for copy in [comp_copy] + copies:
        copy.wait()


def on_device(counts, velocity_prev, forcing, reaction):
    C, X, Y, Z = velocity_prev.shape
    blocks = counts["gx"]
    kept = X // 2
    chunk = Z // blocks
    tiles = -(-(C * (Y // 8)) // (Z // chunk))
    matrix = jnp.asarray(finish_matrix(X, blocks, 8))
    vmem = pl.BlockSpec(memory_space=pltpu.VMEM)
    space = lambda *shape: pltpu.VMEM(shape, jnp.float32)

    compressed, *kept_arrays = pl.pallas_call(
        functools.partial(kernel, counts),
        out_shape=[
            jax.ShapeDtypeStruct((C, Y, kept * blocks, chunk), jnp.float32),
            jax.ShapeDtypeStruct((C, X, Y, Z), jnp.float32),
            jax.ShapeDtypeStruct((X + 4, Y + 8, Z), jnp.float32),
            jax.ShapeDtypeStruct((3, C + 1, Y + 16, Z), jnp.float32),
            jax.ShapeDtypeStruct((2, 3, Y + 16, Z), jnp.float32),
            jax.ShapeDtypeStruct((3 * Z, Z), jnp.bfloat16),
        ],
        in_specs=[pl.BlockSpec(memory_space=pltpu.HBM)] * 4,
        out_specs=[vmem] * 6,
        scratch_shapes=[
            space(C, X + 6, Y + 8, Z),
            space(C, X + 4, Y + 8, Z),
            space(X + 4, Y + 8, Z),
            space(*matrix.shape),
            space(C, X + 4, Y + 8, Z),
            space(C, X + 2, Y + 8, Z),
            space(2, 5 * C + 2, X, Z),
            space(2, 5 * C + 2, X, Z),
            space(4, 16, Z),
            space(4, 16, Z),
            space(4, Y, Z),
            space(2, 4, Y + 8, Z),
            space(2, 8, Z),
            space(2, 2, 8, Z),
            space(2, Y, Z),
            space(2, 2, 2, Y, Z),
            space(2, 2, 2, 8, Z),
            space(Y, Z),
            space(blocks, tiles, kept, 8, Z),
            space(blocks, tiles, kept, 8, Z),
            space(max((blocks - 1) * tiles * kept * 8, 128 * Y), Z),
            pltpu.VMEM((3 * Z, Z), jnp.bfloat16),
            pltpu.SemaphoreType.DMA((1,)),
            pltpu.SemaphoreType.DMA((1,)),
            pltpu.SemaphoreType.DMA((2,)),
            pltpu.SemaphoreType.DMA((2,)),
            pltpu.SemaphoreType.DMA((1,)),
            pltpu.SemaphoreType.DMA((1,)),
            pltpu.SemaphoreType.DMA((2 * C + 2,)),
        ],
        compiler_params=pltpu.CompilerParams(collective_id=0, has_side_effects=True, vmem_limit_bytes=40000000),
    )(*(pltpu.with_memory_space_constraint(a, pltpu.HBM) for a in (velocity_prev, forcing, reaction, matrix)))
    velocity, compressed = pl.pallas_call(
        finish,
        out_shape=(
            jax.ShapeDtypeStruct((C, X, Y, Z), jnp.float32),
            jax.ShapeDtypeStruct(compressed.shape, jnp.float32),
        ),
        in_specs=[vmem] * 6,
        out_specs=[pl.BlockSpec(memory_space=pltpu.HBM)] * 2,
        scratch_shapes=[space(C, X, Y, Z), pltpu.SemaphoreType.DMA((C + 1,))],
        compiler_params=pltpu.CompilerParams(vmem_limit_bytes=16000000),
    )(*kept_arrays, compressed)
    return velocity, jnp.swapaxes(compressed, 2, 3)


def solution(mesh):
    counts = {axis: mesh.shape[axis] for axis in ("agg", "gx", "gy")}
    placed = (P(None, "gx", "gy", "agg"), P(None, "gx", "gy", "agg"), P("gx", "gy", "agg"))
    return jax.shard_map(
        functools.partial(on_device, counts),
        mesh=mesh,
        in_specs=placed,
        out_specs=(P(None, "gx", "gy", "agg"), P(None, "gy", ("agg", "gx"), None)),
        check_vma=False,
    )
```

```python
import functools
import itertools
import math

import jax
import jax.numpy as jnp
import numpy as np
from jax import lax
from jax.experimental import pallas as pl
from jax.experimental.pallas import tpu as pltpu
from jax.sharding import PartitionSpec as P

SWEEPS = 2
COARSE_SWEEPS = 4
LX = 5
MESH = pl.DeviceIdType.MESH

damping = 0.8
keep = 1.0 - damping
root_half = 0.7071067811865476


def local_levels(cells_x):
    return min(LX, cells_x.bit_length() - 1)


def finish_matrix(cells_x, blocks, rows):
    levels = local_levels(cells_x)
    kept = cells_x // 2
    eye = np.eye(blocks * kept).reshape(blocks, kept, blocks * kept)
    width = cells_x >> levels
    approx = eye[:, :width].reshape(blocks * width, -1)
    details, at = [], width
    for level in range(levels, 1, -1):
        width = cells_x >> level
        details.append(eye[:, at : at + width].reshape(blocks * width, -1))
        at += width
    for level in range(levels, LX):
        low, high = approx[0::2], approx[1::2]
        approx, detail = (low + high) * root_half, (low - high) * root_half
        details.insert(0, detail)
    along_x = np.concatenate([approx] + details, axis=0)
    along_y = np.zeros((rows, rows))
    for row in range(0, rows, 2):
        along_y[row, row : row + 2] = root_half
        along_y[row + 1, row : row + 2] = root_half, -root_half
    return np.einsum("qk,yr->yqkr", along_x, along_y).reshape(-1, blocks * kept * rows).astype(np.float32)


def around():
    axes = ("gx", "gy", "agg")
    found = []
    for number in range(1, 27):
        turn = [(number // 3**i) % 3 for i in range(3)]
        found.append(tuple((axis, way == 1) for axis, way in zip(axes, turn) if way))
    return sorted(found, key=lambda sides: (-len(sides), sides))


def lane_sums(tiles, matrix):
    stack = jnp.concatenate(tiles, axis=0)
    high = stack.astype(jnp.bfloat16)
    rest = stack - high.astype(jnp.float32)
    middle = rest.astype(jnp.bfloat16)
    low = (rest - middle.astype(jnp.float32)).astype(jnp.bfloat16)
    done = lax.dot_general(
        jnp.concatenate([high, middle, low], axis=1), matrix[...], (((1,), (0,)), ((), ())),
        preferred_element_type=jnp.float32,
    )
    return [done[i * 8 : i * 8 + 8] for i in range(len(tiles))]


far = 1e30


def kernel(
    sizes, v_hbm, f_hbm, r_hbm, m_hbm, comp_ref, base_ref, w_ext, q_ext, h_ext, pairs_ref,
    v_ext, f_ext, r_ext, m_ref, u1_ext, u2_ext,
    y_send, y_recv, xy_send, xy_recv, z_send, z_recv, yz_send, yz_recv, xz_send, xz_recv, corner_recv,
    zs_coarse, c_send, c_recv, measure, band_ref,
    a_send_sem, a_recv_sem, q_send_sem, q_recv_sem, c_send_sem, c_recv_sem, in_sem,
):
    counts = sizes
    C, X, Y, Z = base_ref.shape
    me = {axis: lax.axis_index(axis) for axis in counts}
    blocks = counts["gx"]
    chunk = Z // blocks
    rows_ext = Y + 8
    f32 = jnp.float32

    loads = [
        pltpu.make_async_copy(src, dst, in_sem.at[i])
        for i, (src, dst) in enumerate(
            [(v_hbm.at[c], v_ext.at[c, 3 : 3 + X, :Y]) for c in range(C)]
            + [(f_hbm.at[c], f_ext.at[c, 2 : 2 + X, :Y]) for c in range(C)]
            + [(r_hbm, r_ext.at[2 : 2 + X, :Y]), (m_hbm, m_ref)]
        )
    ]
    for load in loads:
        load.start()

    def exists(axis, high):
        return me[axis] < counts[axis] - 1 if high else me[axis] > 0

    def all_exist(sides, flip):
        there = None
        for axis, high in sides:
            one = exists(axis, high != flip)
            there = one if there is None else there & one
        return there

    def beside(*sides):
        return {axis: me[axis] + (1 if high else -1) for axis, high in sides}

    barrier = pltpu.get_barrier_semaphore()
    expected = blocks - 1
    for sides in around():
        if len(sides) > 1 or sides[0][0] != "gx":
            there = all_exist(sides, False)
            expected = expected + there.astype(jnp.int32)

            @pl.when(there)
            def _():
                pl.semaphore_signal(barrier, inc=1, device_id=beside(*sides), device_id_type=MESH)

    for step in range(1, blocks):
        pl.semaphore_signal(
            barrier, inc=1, device_id={"gx": lax.rem(me["gx"] + step, blocks)}, device_id_type=MESH
        )

    lane = lax.broadcasted_iota(jnp.int32, (8, Z), 1)
    row = lax.broadcasted_iota(jnp.int32, (8, Z), 0)
    place = lane % 8
    group = lane // 8
    low_half = (lane < 32) | (lane >= 96)

    def fine_messages(sides):
        at = {axis: high for axis, high in sides}
        x, y, z = at.get("gx"), at.get("gy"), at.get("agg")
        from_x, from_y, from_z = 0 if x else 1, 0 if y else 1, 0 if z else 1
        if z is None and y is None:
            made = []
            for ref, depth, fill in ((v_ext, 3, 0.0), (f_ext, 2, 0.0), (r_ext, 2, far)):
                here = pl.ds(X if x else depth, depth)
                there = pl.ds(0 if x else depth + X, depth)
                index = (slice(None),) if ref is not r_ext else ()
                made.append((ref.at[index + (here, pl.ds(0, Y))], ref.at[index + (there, pl.ds(0, Y))], fill))
            return made
        if z is None and x is None:
            return [(y_send.at[int(y)], y_recv.at[from_y], None)]
        if z is None:
            return [(xy_send.at[2 * int(x) + int(y)], xy_recv.at[2 * from_x + from_y], None)]
        if x is None and y is None:
            return [(z_send, z_recv.at[from_z, :, pl.ds(0, Y)], None)]
        if x is None:
            return [(yz_send.at[int(y)], yz_recv.at[from_z, from_y], None)]
        if y is None:
            return [(xz_send, xz_recv.at[from_z, from_x], None)]
        return [(xz_send.at[0, pl.ds(Y - 8 if y else 0, 8)], corner_recv.at[from_z, from_x, from_y], 0.0)]

    def remote(src, dst, send_sem, recv_sem, sides):
        return pltpu.make_async_remote_copy(
            src_ref=src, dst_ref=dst, send_sem=send_sem, recv_sem=recv_sem,
            device_id=beside(*sides), device_id_type=MESH,
        )

    def fine_copies():
        return [
            (sides, remote(src, dst, a_send_sem.at[0], a_recv_sem.at[0], sides))
            for sides in around()
            for src, dst, _ in fine_messages(sides)
        ]

    def rows_of(copies):
        found = {}
        for sides, copy in copies:
            axes = tuple(axis for axis, _ in sides)
            if all(high for _, high in sides):
                found[axes] = found.get(axes, 0) + math.prod(copy.src_ref.shape[:-1])
        return found

    def settle(copies, sem):
        sizes = rows_of(copies)
        neighbours = {
            axis: exists(axis, False).astype(jnp.int32) + exists(axis, True).astype(jnp.int32) for axis in counts
        }
        options = {axis: {1: (0,), 2: (1,)}.get(count, (1, 2)) for axis, count in counts.items()}
        for numbers in itertools.product(*options.values()):
            number = dict(zip(options, numbers))
            rows = sum(size * math.prod(number[axis] for axis in axes) for axes, size in sizes.items())
            there = None
            for axis, value in number.items():
                one = neighbours[axis] == value
                there = one if there is None else there & one
            if rows:
                part = measure.at[pl.ds(0, rows)]
                pl.when(there)(pltpu.make_async_copy(part, part, sem).wait)

    def coarse_message(sides, first=0, fields=C):
        at = {axis: 1 if high else -1 for axis, high in sides}
        block = 1 - at.get("gx", 0)
        here, there = {
            0: (slice(0, Y), slice(0, Y)),
            1: (slice(Y - 8, Y), slice(Y + 8, Y + 16)),
            -1: (slice(0, 8), slice(Y, Y + 8)),
        }[at.get("gy", 0)]
        if "agg" in at:
            return zs_coarse.at[here], h_ext.at[0 if at["agg"] > 0 else 1, block, there]
        which = pl.ds(first, fields)
        return q_ext.at[1, which, here], q_ext.at[block, which, there]

    def coarse_copies():
        return [
            (sides, remote(*coarse_message(sides), q_send_sem.at[0], q_recv_sem.at[0], sides))
            for sides in around()
        ]

    def step_copies():
        return [
            (sides, remote(*coarse_message(sides, C, 1), q_send_sem.at[1], q_recv_sem.at[1], sides))
            for sides in around()
            if "agg" not in dict(sides)
        ]

    far_high = jnp.where(low_half, far, 0.0).astype(f32)
    for sides in around():
        @pl.when(jnp.logical_not(all_exist(sides, True)))
        def _():
            axes = tuple(axis for axis, _ in sides)
            for _, target, fill in fine_messages(sides):
                if fill is not None:
                    target[...] = jnp.full(target.shape, fill, f32)
                elif axes == ("gy",):
                    target[: 5 * C] = jnp.zeros((5 * C, 8, Z), f32)
                    target[5 * C :] = jnp.full((2, 8, Z), far, f32)
                elif axes == ("gx", "gy"):
                    target[0:8] = jnp.zeros((8, Z), f32)
                    target[8:16] = jnp.where(row == 4 * C - 8, far, 0.0)
                elif axes == ("agg",):
                    target[:3] = jnp.zeros((3, Y, Z), f32)
                    for t in range(Y // 8):
                        target[3, t * 8 : t * 8 + 8] = far_high
                elif axes == ("gy", "agg"):
                    target[...] = jnp.where(row >= 6, far_high, 0.0)
                else:
                    target[0] = jnp.zeros((Y, Z), f32)
                    for t in range(Y // 8):
                        target[1, t * 8 : t * 8 + 8] = jnp.where(
                            (group == 0) | (group == 1) | (group == 6) | (group == 7), far, 0.0
                        )
            for target in [coarse_message(sides)[1], coarse_message(sides, C, 1)[1]][: 1 + ("agg" not in axes)]:
                target[...] = jnp.zeros(target.shape, f32)

    tiles_y = Y // 8
    near, ring = range(tiles_y), range(tiles_y + 1)
    tile_of = lambda t: slice(t * 8, t * 8 + 8)
    even_l = lane % 2 == 0
    even_r = row % 2 == 0
    lane_roll = lambda t, shift: pltpu.roll(t, shift % Z, 1) if shift % Z else t
    row_roll = lambda t, shift: pltpu.roll(t, shift % 8, 0)
    lane_take = lambda t, source: jnp.take_along_axis(t, source, axis=1)
    v_flat = v_ext.reshape(C * (X + 6) * rows_ext, Z)
    f_flat = f_ext.reshape(C * (X + 4) * rows_ext, Z)
    r_flat = r_ext.reshape((X + 4) * rows_ext, Z)

    def x_line(number, y):
        if number < 3 * C:
            c, ref, extra = number // 3, v_flat, 3
        elif number < 5 * C:
            c, ref, extra = (number - 3 * C) // 2, f_flat, 2
        else:
            c, ref, extra = 0, r_flat, 2
        return ref, pl.ds((c * (X + 2 * extra) + extra) * rows_ext + y, X, stride=rows_ext)

    depth_of = lambda number: number % 3 if number < 3 * C else (number - 3 * C) % 2

    v_at = lambda c, x, t: v_ext[c, 3 + x, tile_of(t)]
    f_at = lambda c, x, t: f_ext[c, 2 + x, tile_of(t)]
    held = (
        (lambda x, t: v_at(0, x, t), lambda x, t: v_at(1, x, t)),
        (lambda x, t: v_at(2, x, t), None),
        (lambda x, t: f_at(0, x, t), lambda x, t: f_at(1, x, t)),
        (lambda x, t: f_at(2, x, t), lambda x, t: r_ext[2 + x, tile_of(t)]),
    )
    from_ends = jnp.where(place < 4, 3 - place, Z + 3 - place)
    needed = ((0, 1), (2,), (3, 4), (5, 6))
    across = {}
    for i, pair in enumerate(held):
        for number in needed[i]:
            loads[number].wait()
        for t in near:
            packed = jnp.zeros((8, Z), f32)
            crossed = across.get(t, packed) if i % 2 else packed
            for half, get in enumerate(pair):
                if get is not None:
                    for x in range(X):
                        ends = lane_take(get(x, t), from_ends)
                        packed = jnp.where(group == (x + 4 + 8 * half) % 16, ends, packed)
                        if x < 2 or x >= X - 2:
                            crossed = jnp.where(group == (x + 4 + 8 * half + 4 * (i % 2)) % 16, ends, crossed)
            across[t] = crossed
            z_send[i, tile_of(t)] = packed
            if i % 2:
                xz_send[i // 2, tile_of(t)] = crossed
            for side in range(2):
                if t == (tiles_y - 1 if side else 0):
                    first = 6 if side else 0
                    yz_send[side, 2 * i : 2 * i + 2] = packed[first : first + 2]
    pl.semaphore_wait(barrier, expected)
    for sides, copy in fine_copies():
        if len(sides) == 3:
            pl.when(all_exist(sides, False))(copy.start)
    for number in range(5 * C + 2):
        for side in range(2):
            depth = depth_of(number)
            ref, at = x_line(number, Y - 1 - depth if side else depth)
            y_send[side, number] = ref[at, :]
    for high_x in range(2):
        for high_y in range(2):
            xs = [X - 1 - d if high_x else d for d in range(2)]
            ys = [Y - 1 - d if high_y else d for d in range(2)]
            target = xy_send.at[2 * high_x + high_y]
            for c in range(C):
                for i, (x, y) in enumerate(((xs[0], ys[0]), (xs[1], ys[0]), (xs[0], ys[1]))):
                    target[3 * c + i : 3 * c + i + 1] = v_ext[c, 3 + x, y : y + 1]
                target[3 * C + c : 3 * C + c + 1] = f_ext[c, 2 + xs[0], ys[0] : ys[0] + 1]
            target[4 * C : 4 * C + 1] = r_ext[2 + xs[0], ys[0] : ys[0] + 1]
    for sides, copy in fine_copies():
        if len(sides) < 3:
            pl.when(all_exist(sides, False))(copy.start)

    kept = X // 2
    parts = Y // 8
    combos_per_tile = Z // chunk

    def c_copy(j, source):
        return pltpu.make_async_remote_copy(
            src_ref=c_send.at[j],
            dst_ref=c_recv.at[source],
            send_sem=c_send_sem.at[0],
            recv_sem=c_recv_sem.at[0],
            device_id={"gx": j},
            device_id_type=MESH,
        )

    def settle_parts(sem):
        rows = (blocks - 1) * math.prod(c_send.shape[1:-1])
        if rows:
            part = measure.at[pl.ds(0, rows)]
            pltpu.make_async_copy(part, part, sem).wait()

    def finish_compressed(tiles):
        coefs = blocks * kept
        for tile in tiles:
            gathered = c_recv[:, tile].reshape(coefs * 8, Z)
            done = lax.dot_general(
                m_ref[...], gathered, (((1,), (0,)), ((), ())),
                precision=lax.Precision.HIGHEST, preferred_element_type=jnp.float32,
            )
            for place in range(combos_per_tile):
                c, part = divmod(tile * combos_per_tile + place, parts)
                if c < C:
                    for y in range(8):
                        comp_ref[c, part * 8 + y] = done[
                            y * coefs : (y + 1) * coefs, place * chunk : (place + 1) * chunk
                        ]

    pair_of = lane + 1 - 2 * (lane % 2)
    lane_swap = lambda t: lane_take(t, pair_of)
    row_swap = lambda t: jnp.where(even_r, row_roll(t, -1), row_roll(t, 1))
    slot_at = lane % 16
    corner_of = ((0, 0), (0, 1), (1, 1), (1, 0))

    def pooled_halves(planes):
        pairs = [[planes[x][t] + planes[x + 1][t] for t in near] for x in range(0, X, 2)]
        out = []
        for t in near:
            t0, t1, t2, t3 = (pair[t] for pair in pairs)
            left = jnp.where(even_r, t0, t3) + row_swap(jnp.where(even_r, t3, t0))
            right = jnp.where(even_r, t1, t2) + row_swap(jnp.where(even_r, t2, t1))
            out.append((jnp.where(even_l, left, right), jnp.where(even_l, right, left)))
        return out

    def pooled(planes):
        return [own + lane_swap(other) for own, other in pooled_halves(planes)]

    from_far = jnp.where(slot_at < 8, 6, Z + 6) - slot_at + 2 * (slot_at % 2)

    from_far_pair = from_far + 1 - 2 * (from_far % 2)

    def edge_lanes(fields, t):
        packed = jnp.zeros((8, Z), f32)
        for start, field in fields:
            packed = jnp.where((lane >= start) & (lane < start + 16), lane_take(field[t], from_far), packed)
        return packed

    coarse_weight = [
        damping / ((6.0 + 0.5 * total) * 0.25)
        for total in pooled([[r_ext[2 + x, tile_of(t)] for t in near] for x in range(X)])
    ]
    coarse_step = [0.25 * weight for weight in coarse_weight]
    step_edges = [edge_lanes([(64 + 16 * c, coarse_step) for c in range(C)], t) for t in near]
    weight_edges = [edge_lanes([(16 * c, coarse_weight) for c in range(C)], t) for t in near]
    for t in near:
        q_ext[1, C, tile_of(t)] = coarse_step[t]
    for x in range(X):
        for t in near:
            w_ext[2 + x, tile_of(t)] = damping / (6.0 + r_ext[2 + x, tile_of(t)])

    source = lax.broadcasted_iota(jnp.int32, (Z, Z), 0)
    target = lax.broadcasted_iota(jnp.int32, (Z, Z), 1)
    apart = jnp.abs(source - target)
    band = jnp.where(apart == 1, 1.0, 0.0).astype(jnp.bfloat16)
    paired = (apart == 2) | ((apart == 1) & (source // 2 == target // 2))
    pairs = jnp.where(paired, 1.0, 0.0).astype(jnp.bfloat16)
    for part in range(3):
        band_ref[part * Z : part * Z + Z] = band
        pairs_ref[part * Z : part * Z + Z] = pairs

    levels = local_levels(X)
    for c in range(C):
        for t in near:
            approx, details = [v_at(c, x, t) for x in range(X)], []
            for level in range(levels):
                low, high = approx[0::2], approx[1::2]
                approx = [(a + b) * root_half for a, b in zip(low, high)]
                if level > 0:
                    details = [(a - b) * root_half for a, b in zip(low, high)] + details
            tile, spot = divmod(c * parts + t, combos_per_tile)
            inside = (lane >= spot * chunk) & (lane < (spot + 1) * chunk)
            for k, values in enumerate(approx + details):
                done = (jnp.where(even_l, values, -values) + lane_swap(values)) * root_half
                for j in range(blocks):
                    moved = lane_roll(done, spot * chunk - j * chunk)
                    if spot:
                        moved = jnp.where(inside, moved, c_send[j, tile, k])
                    c_send[j, tile, k] = moved

    for c in range(C):
        for x in range(X):
            for t in near:
                own = v_at(c, x, t)
                total = f_at(c, x, t) + jnp.where(lane == 0, 0.0, lane_roll(own, 1))
                total = total + jnp.where(lane == Z - 1, 0.0, lane_roll(own, -1))
                for other in range(max(x - 1, 0), min(x + 2, X)):
                    if other != x:
                        total = total + v_at(c, other, t)
                for other, shift, inner in ((t + 1, -1, row < 7), (t - 1, 1, row >= 1)):
                    beyond = row_roll(v_at(c, x, other), shift) if other in near else 0.0
                    total = total + jnp.where(inner, row_roll(own, shift), beyond)
                u1_ext[c, 2 + x, tile_of(t)] = keep * own + w_ext[2 + x, tile_of(t)] * total

    settle(fine_copies(), a_recv_sem.at[0])

    for sides, copy in step_copies():
        pl.when(all_exist(sides, False))(copy.start)
    for j in range(blocks):
        pl.when(me["gx"] != j)(c_copy(j, me["gx"]).start)

    for number in range(5 * C + 2):
        for side in range(2):
            depth = depth_of(number)
            ref, at = x_line(number, Y + depth if side else rows_ext - 1 - depth)
            ref[at, :] = y_recv[side, number]
    for high_x in range(2):
        for high_y in range(2):
            xs = [X + d if high_x else -1 - d for d in range(2)]
            ys = [Y + d if high_y else rows_ext - 1 - d for d in range(2)]
            source = xy_recv.at[2 * high_x + high_y]
            for c in range(C):
                for i, (x, y) in enumerate(((xs[0], ys[0]), (xs[1], ys[0]), (xs[0], ys[1]))):
                    v_ext[c, 3 + x, y : y + 1] = source[3 * c + i : 3 * c + i + 1]
                f_ext[c, 2 + xs[0], ys[0] : ys[0] + 1] = source[3 * C + c : 3 * C + c + 1]
            r_ext[2 + xs[0], ys[0] : ys[0] + 1] = source[4 * C : 4 * C + 1]
    for side in range(2):
        for i in range(4):
            z_recv[side, i, Y : Y + 2] = yz_recv[side, 1, 2 * i : 2 * i + 2]
            z_recv[side, i, Y + 6 : Y + 8] = yz_recv[side, 0, 2 * i : 2 * i + 2]

    def weight_of(reaction):
        return jnp.where(reaction < 0.1 * far, damping / (6.0 + reaction), 0.0)

    for x in range(-2, X + 2):
        outside = max(-x, x - X + 1)
        for t in ring:
            if (outside > 0 and t < tiles_y) or (t == tiles_y and outside < 2):
                w_ext[2 + x, tile_of(t)] = weight_of(r_ext[2 + x, tile_of(t)])

    mixed = {}
    for i in range(4):
        for t in ring:
            mixed[i, t] = jnp.where(place < 4, z_recv[1, i, tile_of(t)], z_recv[0, i, tile_of(t)])
    beyond = {}
    for side in range(2):
        for i in range(2):
            for t in near:
                beyond[side, i, t] = jnp.where(
                    place < 4, xz_recv[1, side, i, tile_of(t)], xz_recv[0, side, i, tile_of(t)]
                )
        ends = [
            jnp.where(place < 4, corner_recv[1, side, high], corner_recv[0, side, high]) for high in range(2)
        ]
        beyond[side, 0, tiles_y] = jnp.where(row < 4, ends[1], ends[0])

    def edge_field(number, t):
        i, half = divmod(number, 2)
        value = lane_roll(mixed[i, t], 64 * half)
        if t < tiles_y or number < 4:
            shift = (64, 0, 32, -32)[number % 4]
            low, high = (lane_roll(beyond[side, i // 2, t], shift) for side in range(2))
            value = jnp.where(group < 4, low, jnp.where(group >= 12, high, value))
        return value

    edge_v = {(c, t): edge_field(c, t) for c in range(C) for t in ring}
    edge_f = {(c, t): edge_field(4 + c, t) for c in range(C) for t in ring}
    edge_w = {t: weight_of(edge_field(7, t)) for t in ring}

    def around_rows(get, t, tiles, by):
        after, before = (t + 1) % tiles, (t - 1) % tiles
        own = get(t)
        above = jnp.where(row < 8 - by, row_roll(own, -by), row_roll(get(after), -by))
        below = jnp.where(row >= by, row_roll(own, by), row_roll(get(before), by))
        return below, above

    def rows_beside(at, t):
        get = lambda t: at(tile_of(t))
        if t < tiles_y:
            above = at(pl.ds(t * 8 + 1, 8))
        else:
            above = jnp.where(row < 7, row_roll(get(t), -1), row_roll(get(0), -1))
        if t > 0:
            below = at(pl.ds(t * 8 - 1, 8))
        else:
            below = jnp.where(row >= 1, row_roll(get(t), 1), row_roll(get(tiles_y), 1))
        return below, above

    def main_total(get, edge, c, x, t, along_z=None):
        below, above = rows_beside(lambda rows: get(c, x, rows), t)
        get = lambda c, x, t, get=get: get(c, x, tile_of(t))
        total = (get(c, x - 1, t) + get(c, x + 1, t)) + (below + above)
        beside_z = lane_roll(edge[c, t], -(8 * (x + 4) + 4))
        if along_z is not None:
            return total + (along_z + jnp.where((lane == 0) | (lane == Z - 1), beside_z, 0.0))
        own = get(c, x, t)
        total = total + jnp.where(lane == 0, beside_z, lane_roll(own, 1))
        return total + jnp.where(lane == Z - 1, beside_z, lane_roll(own, -1))

    def edge_total(get, edge, c, xs, t):
        own = edge[c, t]
        line = own
        for x in xs:
            line = jnp.where(group == x + 4, lane_roll(get(c, x, t), 8 * (x + 4) + 4), line)
        below, above = around_rows(lambda t: edge[c, t], t, tiles_y + 1, 1)
        total = (lane_roll(own, 8) + lane_roll(own, -8)) + (below + above)
        total = total + jnp.where(place == 4, line, lane_roll(own, 1))
        return total + jnp.where(place == 3, line, lane_roll(own, -1))

    u1_at = lambda c, x, t: u1_ext[c, 2 + x, tile_of(t)]
    u2_at = lambda c, x, t: u2_ext[c, 1 + x, tile_of(t)]
    v_rows = lambda c, x, rows: v_ext[c, 3 + x, rows]
    u1_rows = lambda c, x, rows: u1_ext[c, 2 + x, rows]
    u2_rows = lambda c, x, rows: u2_ext[c, 1 + x, rows]
    w_at = lambda x, t: w_ext[2 + x, tile_of(t)]

    edge_1, edge_2 = {}, {}
    for c in range(C):
        for t in ring:
            total = edge_total(v_at, edge_v, c, range(-1, X + 1), t)
            edge_1[c, t] = keep * edge_v[c, t] + edge_w[t] * (edge_f[c, t] + total)
        chosen = [
            (x, t)
            for x in range(-2, X + 2)
            for t in (near if x in (-2, X + 1) else [tiles_y] if 0 <= x < X else ring)
        ]
        along_z = dict(zip(chosen, lane_sums([v_at(c, x, t) for x, t in chosen], band_ref)))
        for x in range(-2, X + 2):
            if 0 <= x < X:
                for t in near:
                    beside_z = lane_roll(edge_v[c, t], -(8 * (x + 4) + 4))
                    total = jnp.where((lane == 0) | (lane == Z - 1), beside_z, 0.0)
                    if t == 0:
                        total = total + jnp.where(row == 0, row_roll(v_at(c, x, tiles_y), 1), 0.0)
                    if t == tiles_y - 1:
                        total = total + jnp.where(row == 7, row_roll(v_at(c, x, tiles_y), -1), 0.0)
                    if x in (0, X - 1):
                        total = total + v_at(c, -1 if x == 0 else X, t)
                    u1_ext[c, 2 + x, tile_of(t)] = u1_at(c, x, t) + w_at(x, t) * total
            for t in near if x in (-2, X + 1) else [tiles_y] if 0 <= x < X else ring:
                total = main_total(v_rows, edge_v, c, x, t, along_z[x, t])
                u1_ext[c, 2 + x, tile_of(t)] = keep * v_at(c, x, t) + w_at(x, t) * (f_at(c, x, t) + total)
    for c in range(C):
        for t in near:
            total = edge_total(u1_at, edge_1, c, range(X), t)
            edge_2[c, t] = keep * edge_1[c, t] + edge_w[t] * (edge_f[c, t] + total)
        chosen = [(x, t) for x in range(-1, X + 1) for t in (near if x in (-1, X) else ring)]
        along_z = dict(zip(chosen, lane_sums([u1_at(c, x, t) for x, t in chosen], band_ref)))
        for x in range(-1, X + 1):
            for t in near if x in (-1, X) else ring:
                total = main_total(u1_rows, edge_1, c, x, t, along_z[x, t])
                u2_ext[c, 1 + x, tile_of(t)] = keep * u1_at(c, x, t) + w_at(x, t) * (f_at(c, x, t) + total)
    sums = []
    for c in range(C):
        chosen = [(x, t) for x in range(X) for t in near]
        along_z = dict(zip(chosen, lane_sums([u2_at(c, x, t) for x, t in chosen], band_ref)))
        sums.append([
            [main_total(u2_rows, edge_2, c, x, t, along_z[x, t]) + f_at(c, x, t) for t in near] for x in range(X)
        ])

    halves = [
        pooled_halves([
            [sums[c][x][t] - (6.0 + r_ext[2 + x, tile_of(t)]) * u2_at(c, x, t) for t in near] for x in range(X)
        ])
        for c in range(C)
    ]
    for t in near:
        total = jnp.zeros((8, Z), f32)
        for c in range(C):
            own, other = halves[c][t]
            here = (lane >= 16 * c) & (lane < 16 * c + 16)
            total = jnp.where(here, lane_take(own, from_far) + lane_take(other, from_far_pair), total)
        zs_coarse[tile_of(t)] = jnp.where(lane < 64, weight_edges[t] * (0.125 * total), step_edges[t])
        for c in range(C):
            own, other = halves[c][t]
            q_ext[1, c, tile_of(t)] = coarse_weight[t] * (0.125 * (own + lane_swap(other)))
    for sides, copy in coarse_copies():
        pl.when(all_exist(sides, False))(copy.start)

    for c in range(C):
        for x in range(X):
            for t in near:
                base_ref[c, x, tile_of(t)] = keep * u2_at(c, x, t) + w_at(x, t) * sums[c][x][t]

    for j in range(blocks):
        @pl.when(me["gx"] == j)
        def _():
            c_recv[j] = c_send[j]

    settle_parts(c_recv_sem.at[0])
    loads[-1].wait()
    finish_compressed(range(c_send.shape[1]))

    settle(step_copies(), q_recv_sem.at[1])
    settle(coarse_copies(), q_recv_sem.at[0])

    settle(fine_copies(), a_send_sem.at[0])
    settle(step_copies(), q_send_sem.at[1])
    settle(coarse_copies(), q_send_sem.at[0])
    settle_parts(c_send_sem.at[0])


def finish(base_ref, w_ext, q_ext, h_ext, pairs_ref, comp_ref, vel_hbm, comp_hbm, vel_ref, sem):
    C, X, Y, Z = base_ref.shape
    f32 = jnp.float32
    comp_copy = pltpu.make_async_copy(comp_ref, comp_hbm, sem.at[C])
    comp_copy.start()
    tiles_y = Y // 8
    near = range(tiles_y)
    tile_of = lambda t: slice(t * 8, t * 8 + 8)
    lane = lax.broadcasted_iota(jnp.int32, (8, Z), 1)
    row = lax.broadcasted_iota(jnp.int32, (8, Z), 0)
    even_l = lane % 2 == 0
    even_r = row % 2 == 0
    slot_at = lane % 16
    corner_of = ((0, 0), (0, 1), (1, 1), (1, 0))
    pair_of = lane + 1 - 2 * (lane % 2)
    lane_roll = lambda t, shift: pltpu.roll(t, shift % Z, 1) if shift % Z else t
    row_roll = lambda t, shift: pltpu.roll(t, shift % 8, 0)
    lane_swap = lambda t: jnp.take_along_axis(t, pair_of, axis=1)
    row_swap = lambda t: jnp.where(even_r, row_roll(t, -1), row_roll(t, 1))

    ring = range(tiles_y + 2)
    after = lambda t: (t + 1) % len(ring)
    before = lambda t: (t - 1) % len(ring)
    main = {(b, c, t): q_ext[b, c, tile_of(t)] for b in range(3) for c in range(C) for t in ring}
    step_main = {(b, t): q_ext[b, C, tile_of(t)] for b in range(3) for t in ring}
    edge = {
        (b, t): jnp.where(slot_at < 8, h_ext[1, b, tile_of(t)], h_ext[0, b, tile_of(t)])
        for b in range(3) for t in ring
    }
    step_edge = {key: lane_roll(value, -64) for key, value in edge.items()}
    first_main, first_edge = dict(main), dict(edge)

    def above(get, t):
        return jnp.where(row < 6, row_roll(get(t), -2), row_roll(get(after(t)), -2))

    def below(get, t):
        return jnp.where(row >= 2, row_roll(get(t), 2), row_roll(get(before(t)), 2))

    def along(get, b, t):
        low, high = get(max(b - 1, 0), t), get(min(b + 1, 2), t)
        across = jnp.where(even_l, jnp.where(even_r, high, low), get(b, t))
        return row_swap(across)

    def inject(edge, b, c, t):
        return lane_roll(edge[b, t], -(16 * c + 8))

    def left_of(main, edge, b, c, t):
        return jnp.where(lane < 2, inject(edge, b, c, t), lane_roll(main[b, c, t], 2))

    def right_of(main, edge, b, c, t):
        return jnp.where(lane >= Z - 2, inject(edge, b, c, t), lane_roll(main[b, c, t], -2))

    def coarse_sweep(main, edge, main_at, edge_at):
        new_main, new_edge = dict(main), dict(edge)
        for c in range(C):
            lanes = dict(zip(main_at, lane_sums([main[b, c, t] for b, t in main_at], pairs_ref)))
            for b, t in main_at:
                get = lambda b, t, c=c: main[b, c, t]
                row_get = lambda t, b=b, c=c: main[b, c, t]
                total = along(get, b, t) + (above(row_get, t) + below(row_get, t))
                ends = jnp.where((lane < 2) | (lane >= Z - 2), inject(edge, b, c, t), 0.0)
                total = total + (lanes[b, t] + ends)
                new_main[b, c, t] = keep * main[b, c, t] + first_main[b, c, t] + step_main[b, t] * total
        for b, t in edge_at:
            get = lambda b, t: edge[b, t]
            row_get = lambda t, b=b: edge[b, t]
            own = lane_roll(main[b, 0, t], 8)
            for c in range(1, C):
                own = jnp.where(lane < 16 * c, own, lane_roll(main[b, c, t], 16 * c + 8))
            total = along(get, b, t) + lane_swap(edge[b, t]) + (above(row_get, t) + below(row_get, t))
            total = total + jnp.where((slot_at == 8) | (slot_at == 9), own, lane_roll(edge[b, t], 2))
            total = total + jnp.where((slot_at == 6) | (slot_at == 7), own, lane_roll(edge[b, t], -2))
            new_edge[b, t] = keep * edge[b, t] + first_edge[b, t] + step_edge[b, t] * total
        return new_main, new_edge

    everywhere = [(b, t) for b in range(3) for t in ring]
    centre = [(1, t) for t in ring]
    sides_near = [(b, t) for b in (0, 2) for t in near]
    main, edge = coarse_sweep(main, edge, everywhere, everywhere)
    main, edge = coarse_sweep(main, edge, everywhere, centre + sides_near)
    main, edge = coarse_sweep(main, edge, centre + sides_near, [(1, t) for t in near])

    def spread_rows(even, odd, pa):
        if pa == 0:
            return jnp.where(even_r, even, row_roll(odd, 1))
        return jnp.where(even_r, row_roll(even, -1), odd)

    def spread_lanes(even, odd, pb):
        if pb == 0:
            return jnp.where(even_l, even, lane_roll(odd, 1))
        return jnp.where(even_l, lane_roll(even, -1), odd)

    copies = []
    for c in range(C):
        for t in near:
            at = tile_of(t)
            row_get = lambda t, c=c: main[1, c, t]
            own = main[1, c, t]
            rows_near = (below(row_get, t), above(row_get, t))
            lanes_near = (left_of(main, edge, 1, c, t), right_of(main, edge, 1, c, t))
            alone = [spread_lanes(own, own, pb) for pb in range(2)]
            spread = [spread_rows(alone[pb], alone[pb], pa) for pa, pb in corner_of]
            low, high = (spread_lanes(main[b, c, t], main[b, c, t], 0) for b in (0, 2))
            spread = [spread_rows(low, low, 1)] + spread + [spread_rows(high, high, 0)]
            based = [3.0 * own + rows_near[a] for a in range(2)]
            wide = [
                [spread_lanes(based[a] + lanes_near[0], based[a] + lanes_near[1], pb) for pb in range(2)]
                for a in range(2)
            ]
            for x in range(X):
                p = x // 2
                pa, pb = corner_of[p]
                added = spread_rows(wide[0][pb], wide[1][pb], pa) + spread[p + 2 * (x % 2)]
                vel_ref[c, x, at] = base_ref[c, x, at] + keep * spread[p + 1] + w_ext[2 + x, at] * added
        copies.append(pltpu.make_async_copy(vel_ref.at[c], vel_hbm.at[c], sem.at[c]))
        copies[-1].start()
    for copy in [comp_copy] + copies:
        copy.wait()


def on_device(counts, velocity_prev, forcing, reaction):
    C, X, Y, Z = velocity_prev.shape
    blocks = counts["gx"]
    kept = X // 2
    chunk = Z // blocks
    tiles = -(-(C * (Y // 8)) // (Z // chunk))
    matrix = jnp.asarray(finish_matrix(X, blocks, 8))
    vmem = pl.BlockSpec(memory_space=pltpu.VMEM)
    space = lambda *shape: pltpu.VMEM(shape, jnp.float32)

    compressed, *kept_arrays = pl.pallas_call(
        functools.partial(kernel, counts),
        out_shape=[
            jax.ShapeDtypeStruct((C, Y, kept * blocks, chunk), jnp.float32),
            jax.ShapeDtypeStruct((C, X, Y, Z), jnp.float32),
            jax.ShapeDtypeStruct((X + 4, Y + 8, Z), jnp.float32),
            jax.ShapeDtypeStruct((3, C + 1, Y + 16, Z), jnp.float32),
            jax.ShapeDtypeStruct((2, 3, Y + 16, Z), jnp.float32),
            jax.ShapeDtypeStruct((3 * Z, Z), jnp.bfloat16),
        ],
        in_specs=[pl.BlockSpec(memory_space=pltpu.HBM)] * 4,
        out_specs=[vmem] * 6,
        scratch_shapes=[
            space(C, X + 6, Y + 8, Z),
            space(C, X + 4, Y + 8, Z),
            space(X + 4, Y + 8, Z),
            space(*matrix.shape),
            space(C, X + 4, Y + 8, Z),
            space(C, X + 2, Y + 8, Z),
            space(2, 5 * C + 2, X, Z),
            space(2, 5 * C + 2, X, Z),
            space(4, 16, Z),
            space(4, 16, Z),
            space(4, Y, Z),
            space(2, 4, Y + 8, Z),
            space(2, 8, Z),
            space(2, 2, 8, Z),
            space(2, Y, Z),
            space(2, 2, 2, Y, Z),
            space(2, 2, 2, 8, Z),
            space(Y, Z),
            space(blocks, tiles, kept, 8, Z),
            space(blocks, tiles, kept, 8, Z),
            space(max((blocks - 1) * tiles * kept * 8, 128 * Y), Z),
            pltpu.VMEM((3 * Z, Z), jnp.bfloat16),
            pltpu.SemaphoreType.DMA((1,)),
            pltpu.SemaphoreType.DMA((1,)),
            pltpu.SemaphoreType.DMA((2,)),
            pltpu.SemaphoreType.DMA((2,)),
            pltpu.SemaphoreType.DMA((1,)),
            pltpu.SemaphoreType.DMA((1,)),
            pltpu.SemaphoreType.DMA((2 * C + 2,)),
        ],
        compiler_params=pltpu.CompilerParams(collective_id=0, has_side_effects=True, vmem_limit_bytes=40000000),
    )(*(pltpu.with_memory_space_constraint(a, pltpu.HBM) for a in (velocity_prev, forcing, reaction, matrix)))
    velocity, compressed = pl.pallas_call(
        finish,
        out_shape=(
            jax.ShapeDtypeStruct((C, X, Y, Z), jnp.float32),
            jax.ShapeDtypeStruct(compressed.shape, jnp.float32),
        ),
        in_specs=[vmem] * 6,
        out_specs=[pl.BlockSpec(memory_space=pltpu.HBM)] * 2,
        scratch_shapes=[space(C, X, Y, Z), pltpu.SemaphoreType.DMA((C + 1,))],
        compiler_params=pltpu.CompilerParams(vmem_limit_bytes=16000000),
    )(*kept_arrays, compressed)
    return velocity, jnp.swapaxes(compressed, 2, 3)


def solution(mesh):
    counts = {axis: mesh.shape[axis] for axis in ("agg", "gx", "gy")}
    placed = (P(None, "gx", "gy", "agg"), P(None, "gx", "gy", "agg"), P("gx", "gy", "agg"))
    return jax.shard_map(
        functools.partial(on_device, counts),
        mesh=mesh,
        in_specs=placed,
        out_specs=(P(None, "gx", "gy", "agg"), P(None, "gy", ("agg", "gx"), None)),
        check_vma=False,
    )
```
